32 devices in a mesh: graph: 32 (over z, y, x, core).
Axes of the slice: x: 2, y: 2, z: 4, core: 2. Of those that a mesh axis runs over, the one named last changes fastest.
Arguments:
- feats: bfloat16 [131072, 128], P('graph')
- w_one: float32 [128, 256], replicated
- w_two: float32 [256, 172], replicated
- send_idx: int32 [1024, 64], P('graph')
- send_count: int32 [1024], P('graph')
- edge_src: int32 [131072, 6], P('graph')
- edge_wt: float32 [131072, 6], P('graph')
- labels: int32 [131072], P('graph')
- label_mask: int32 [131072], P('graph')
Outputs:
- output 1: float32 [], replicated
- output 2: float32 [128, 256], replicated
- output 3: float32 [256, 172], replicated
All inputs are finite; a program needn't handle non-finite values.
Results may differ from the reference program's by a relative error of at most 0.0012.
Values are sent between devices in bfloat16 or wider.
A program may use at most 1 GiB of HBM per device.

```python
import jax
import jax.numpy as jnp
from jax import lax

GRAPH_DEVS = 32
ROWS_DEV = 4096
HALO_ROWS = 64
IN_DEG = 6
FEAT_IN = 128
FEAT_HID = 256
CLASSES = 172

TOTAL_ROWS = GRAPH_DEVS * ROWS_DEV
EXT_ROWS = ROWS_DEV + GRAPH_DEVS * HALO_ROWS


def draw_structure(rng_key):
    rng_keys = jax.random.split(rng_key, 7)
    dev_ids = jnp.arange(GRAPH_DEVS)
    skew_a = jax.random.randint(rng_keys[0], (GRAPH_DEVS, GRAPH_DEVS), 0, HALO_ROWS)
    skew_b = jax.random.randint(rng_keys[1], (GRAPH_DEVS, GRAPH_DEVS), 0, HALO_ROWS)
    counts = 1 + (skew_a * skew_b) // HALO_ROWS
    full_list = dev_ids[None, :] == (dev_ids[:, None] + 1) % GRAPH_DEVS
    counts = jnp.where(full_list, HALO_ROWS, counts)
    send_idx = jax.random.randint(rng_keys[2], (GRAPH_DEVS * GRAPH_DEVS, HALO_ROWS), 0, ROWS_DEV)
    edge_shape = (GRAPH_DEVS, ROWS_DEV, IN_DEG)
    is_cut = jax.random.randint(rng_keys[3], edge_shape, 0, 4) == 0
    local_src = jax.random.randint(rng_keys[4], edge_shape, 0, ROWS_DEV)
    peer_dev = (dev_ids[:, None, None] + jax.random.randint(rng_keys[5], edge_shape, 1, GRAPH_DEVS)) % GRAPH_DEVS
    peer_count = counts[peer_dev, dev_ids[:, None, None]]
    slot_pos = jax.random.randint(rng_keys[6], edge_shape, 0, 1048576) % peer_count
    halo_src = ROWS_DEV + peer_dev * HALO_ROWS + slot_pos
    edge_src = jnp.where(is_cut, halo_src, local_src).reshape(TOTAL_ROWS, IN_DEG)
    return send_idx, counts.reshape(GRAPH_DEVS * GRAPH_DEVS), edge_src, is_cut.reshape(TOTAL_ROWS, IN_DEG)


def setup_inputs(seed: int = 0) -> dict:
    rng_keys = jax.random.split(jax.random.key(seed), 7)
    feats = jax.random.normal(rng_keys[0], (TOTAL_ROWS, FEAT_IN), jnp.float32).astype(jnp.bfloat16)
    w_one = jax.random.normal(rng_keys[1], (FEAT_IN, FEAT_HID), jnp.float32) * FEAT_IN ** -0.5
    w_two = jax.random.normal(rng_keys[2], (FEAT_HID, CLASSES), jnp.float32) * FEAT_HID ** -0.5
    send_idx, send_count, edge_src, is_cut = draw_structure(rng_keys[3])
    raw_wt = jax.random.uniform(rng_keys[4], (TOTAL_ROWS, IN_DEG), jnp.float32, 0.5, 1.5) * jnp.where(is_cut, 0.5, 1.0)
    edge_wt = raw_wt / jnp.sqrt(jnp.sum(raw_wt * raw_wt, axis=1, keepdims=True))
    labels = jax.random.randint(rng_keys[5], (TOTAL_ROWS,), 0, CLASSES)
    label_mask = jax.random.randint(rng_keys[6], (TOTAL_ROWS,), 0, 2)
    return {"feats": feats, "w_one": w_one, "w_two": w_two, "send_idx": send_idx, "send_count": send_count, "edge_src": edge_src, "edge_wt": edge_wt, "labels": labels, "label_mask": label_mask}


def reference(feats, w_one, w_two, send_idx, send_count, edge_src, edge_wt, labels, label_mask):
    dev_ids = jnp.arange(GRAPH_DEVS)
    send_lists = send_idx.reshape(GRAPH_DEVS, GRAPH_DEVS, HALO_ROWS) + (dev_ids * ROWS_DEV)[:, None, None]
    is_valid = (jnp.arange(HALO_ROWS)[None, None, :] < send_count.reshape(GRAPH_DEVS, GRAPH_DEVS)[:, :, None]).astype(jnp.float32)
    halo_ids = jnp.transpose(send_lists, (1, 0, 2)).reshape(GRAPH_DEVS, GRAPH_DEVS * HALO_ROWS)
    halo_ok = jnp.transpose(is_valid, (1, 0, 2)).reshape(GRAPH_DEVS, GRAPH_DEVS * HALO_ROWS)
    src_dev = edge_src.reshape(GRAPH_DEVS, ROWS_DEV, IN_DEG)
    wt_dev = edge_wt.reshape(GRAPH_DEVS, ROWS_DEV, IN_DEG)

    def aggregate(h_flat):
        feat_width = h_flat.shape[1]

        def one_dev(per_dev):
            own_rows, src_ids, edge_w, ids_here, ok_here = per_dev
            halo_vals = h_flat[ids_here].astype(jnp.float32) * ok_here[:, None]
            ext_rows = jnp.concatenate([own_rows.astype(jnp.float32), halo_vals], axis=0)
            return jnp.sum(ext_rows[src_ids] * edge_w[:, :, None], axis=1)

        blocks = h_flat.reshape(GRAPH_DEVS, ROWS_DEV, feat_width)
        return lax.map(one_dev, (blocks, src_dev, wt_dev, halo_ids, halo_ok)).reshape(TOTAL_ROWS, feat_width)

    def scatter_back(d_z):
        feat_width = d_z.shape[1]

        def one_dev(per_dev):
            src_ids, edge_w, dz_rows = per_dev
            contrib = (edge_w[:, :, None] * dz_rows[:, None, :]).reshape(ROWS_DEV * IN_DEG, feat_width)
            return jax.ops.segment_sum(contrib, src_ids.reshape(ROWS_DEV * IN_DEG), num_segments=EXT_ROWS)

        ext_grad = lax.map(one_dev, (src_dev, wt_dev, d_z.reshape(GRAPH_DEVS, ROWS_DEV, feat_width)))
        own_grad = ext_grad[:, :ROWS_DEV].reshape(TOTAL_ROWS, feat_width)
        halo_grad = ext_grad[:, ROWS_DEV:] * halo_ok[:, :, None]
        back_sum = jax.ops.segment_sum(halo_grad.reshape(GRAPH_DEVS * GRAPH_DEVS * HALO_ROWS, feat_width), halo_ids.reshape(GRAPH_DEVS * GRAPH_DEVS * HALO_ROWS), num_segments=TOTAL_ROWS)
        return own_grad + back_sum

    w_one_b = w_one.astype(jnp.bfloat16)
    w_two_b = w_two.astype(jnp.bfloat16)
    z_one = aggregate(feats).astype(jnp.bfloat16)
    h_one = jnp.maximum(jnp.dot(z_one, w_one_b, preferred_element_type=jnp.float32), 0.0).astype(jnp.bfloat16)
    z_two = aggregate(h_one).astype(jnp.bfloat16)
    logits = jnp.dot(z_two, w_two_b, preferred_element_type=jnp.float32)
    mask_f = label_mask.astype(jnp.float32)
    label_total = jnp.sum(mask_f)
    log_prob = jax.nn.log_softmax(logits, axis=-1)
    onehot = (labels[:, None] == jnp.arange(CLASSES)[None, :]).astype(jnp.float32)
    loss_val = -jnp.sum(mask_f[:, None] * onehot * log_prob) / label_total
    d_logits = ((jnp.exp(log_prob) - onehot) * (mask_f / label_total)[:, None]).astype(jnp.bfloat16)
    grad_two = jnp.dot(z_two.T, d_logits, preferred_element_type=jnp.float32)
    d_z2 = jnp.dot(d_logits, w_two_b.T, preferred_element_type=jnp.float32)
    d_h1 = scatter_back(d_z2)
    d_y1 = jnp.where(h_one > 0, d_h1, 0.0).astype(jnp.bfloat16)
    grad_one = jnp.dot(z_one.T, d_y1, preferred_element_type=jnp.float32)
    return (loss_val, grad_one, grad_two)
```

```python
import functools

import jax
import jax.numpy as jnp
from jax import lax
from jax.experimental import pallas as pl
from jax.experimental.pallas import tpu as pltpu
from jax.sharding import PartitionSpec as P

LANES = 128
F32, BF16 = jnp.float32, jnp.bfloat16
VMEM = pl.BlockSpec(memory_space=pltpu.VMEM)
SMEM = pl.BlockSpec(memory_space=pltpu.SMEM)
PAD = 8


def params(limit_mib):
    return pltpu.CompilerParams(vmem_limit_bytes=limit_mib * 2**20)


def row_masks():
    sub = lax.broadcasted_iota(jnp.int32, (8, LANES), 0)
    return [sub == r for r in range(8)]


def dot(a, b, dims):
    return lax.dot_general(a, b, (dims, ((), ())), preferred_element_type=F32)


def fill_weights(wt_ref, wts_ref):
    def body(j, _):
        s = pl.ds(pl.multiple_of(j * LANES, LANES), LANES)
        wts_ref[s, :] = wt_ref[:, s].T
        return 0
    lax.fori_loop(0, wt_ref.shape[1] // LANES, body, 0)


def pick_rows(tables, ids, masks):
    outs = []
    for tbl in tables:
        v = None
        for r in range(8):
            win = tbl[pl.ds(ids[r] + (PAD - r), 8), :]
            v = win if v is None else jnp.where(masks[r], win, v)
        outs.append(v)
    return outs


def gather_sum(src_ref, wts_ref, tables, masks, g, rows, in_deg):
    per = LANES // rows
    blk = src_ref.at[g // per, :, pl.ds((g % per) * rows, rows)]
    out = []
    for h in range(rows // 8):
        w8 = wts_ref[pl.ds(pl.multiple_of(g * rows, rows) + 8 * h, 8), :]
        acc = None
        for k in range(in_deg):
            wk = jnp.broadcast_to(w8[:, k:k + 1], (8, LANES))
            vs = pick_rows(tables, [blk[k, 8 * h + r] for r in range(8)], masks)
            vs = [v * wk for v in vs]
            acc = vs if acc is None else [a + v for a, v in zip(acc, vs)]
        out.append(jnp.concatenate(acc, 1))
    return jnp.concatenate(out, 0)


def send_rows(list_ref, tbl, out_ref, masks):
    def body(g, _):
        blk = list_ref.at[pl.ds(pl.multiple_of(g * 16, 16), 16)]
        parts = [pick_rows([tbl], [blk[8 * h + r] for r in range(8)], masks)[0] for h in range(2)]
        out_ref[pl.ds(pl.multiple_of(g * 16, 16), 16), :] = jnp.concatenate(parts, 0).astype(BF16)
        return 0
    lax.fori_loop(0, out_ref.shape[0] // 16, body, 0)


def chunked(total, chunk, fn):
    def body(i, _):
        fn(pl.multiple_of(i * chunk, chunk))
        return 0
    lax.fori_loop(0, total // chunk, body, 0)


def pick_kernel(list_ref, own_ref, out_ref, tbl):
    rows = own_ref.shape[0]
    chunked(rows, 256, lambda o: tbl.__setitem__((pl.ds(o + PAD, 256), slice(None)), own_ref[pl.ds(o, 256), :].astype(F32)))
    send_rows(list_ref, tbl, out_ref, row_masks())


def layer_one_kernel(in_deg, src_ref, list_ref, wt_ref, own_ref, halo_ref, z_ref, out_ref, tbl, wts, ztbl):
    rows, halo = own_ref.shape[0], halo_ref.shape[0]
    masks = row_masks()
    fill_weights(wt_ref, wts)

    def load_own(o):
        tbl[pl.ds(o + PAD, 256), :] = own_ref[pl.ds(o, 256), :].astype(F32)

    def load_halo(o):
        tbl[pl.ds(o + (PAD + rows), 256), :] = halo_ref[pl.ds(o, 256), :].astype(F32)
    chunked(rows, 256, load_own)
    chunked(halo, 256, load_halo)

    def body(g, _):
        z = gather_sum(src_ref, wts, [tbl], masks, g, 32, in_deg).astype(BF16)
        z_ref[pl.ds(pl.multiple_of(g * 32, 32), 32), :] = z
        ztbl[pl.ds(pl.multiple_of(g * 32, 32) + PAD, 32), :] = z.astype(F32)
        return 0
    lax.fori_loop(0, rows // 32, body, 0)
    send_rows(list_ref, ztbl, out_ref, masks)


def hidden(z, w1):
    return jnp.maximum(dot(z, w1, ((1,), (0,))), 0.0).astype(BF16)


def layer_two_kernel(in_deg, classes, src_ref, total_ref, wt_ref, z_own_ref, z_halo_ref, w1_ref, w2t_ref, lab_ref, mask_ref,
                     g2_ref, gw2t_ref, loss_ref, tlo, thi, wts, z2):
    rows, halo = z_own_ref.shape[0], z_halo_ref.shape[0]
    masks = row_masks()
    fill_weights(wt_ref, wts)
    w1 = w1_ref[...].astype(BF16)

    def load(ref, base):
        def fn(o):
            h = hidden(ref[pl.ds(o, 256), :], w1).astype(F32)
            tlo[pl.ds(o + (PAD + base), 256), :] = h[:, :LANES]
            thi[pl.ds(o + (PAD + base), 256), :] = h[:, LANES:]
        return fn
    chunked(rows, 256, load(z_own_ref, 0))
    chunked(halo, 256, load(z_halo_ref, rows))

    def body(g, _):
        z2[pl.ds(pl.multiple_of(g * 16, 16), 16), :] = gather_sum(src_ref, wts, [tlo, thi], masks, g, 16, in_deg).astype(BF16)
        return 0
    lax.fori_loop(0, rows // 16, body, 0)

    total = total_ref[0]
    w2t = w2t_ref[...].astype(BF16)
    pad_cls = w2t.shape[0]
    gw2t_ref[...] = jnp.zeros_like(gw2t_ref)
    loss_ref[...] = jnp.zeros_like(loss_ref)
    cls = lax.broadcasted_iota(jnp.int32, (pad_cls, 256), 0)

    def chunk(i, _):
        o = pl.multiple_of(i * 256, 256)
        zc = z2[pl.ds(o, 256), :]
        logits = dot(w2t, zc, ((1,), (1,)))
        live = cls < classes
        lab = lab_ref[pl.ds(i, 1), :]
        mf = mask_ref[pl.ds(i, 1), :].astype(F32)
        top = jnp.max(jnp.where(live, logits, -jnp.inf), axis=0, keepdims=True)
        shifted = logits - top
        ex = jnp.where(live, jnp.exp(shifted), 0.0)
        logp = shifted - jnp.log(jnp.sum(ex, axis=0, keepdims=True))
        hot = (cls == lab).astype(F32)
        loss_ref[...] += jnp.sum(mf * hot * logp, axis=0, keepdims=True)
        prob = jnp.where(live, jnp.exp(logp), 0.0)
        g2t = ((prob - hot) * (mf / total)).astype(BF16)
        gw2t_ref[...] += dot(g2t, zc, ((1,), (0,)))
        g2 = jnp.concatenate([g2t.astype(F32), jnp.zeros((2 * LANES - pad_cls, 256), F32)], 0).T
        g2_ref[pl.ds(o, 256), :] = g2.astype(BF16)
        return 0
    lax.fori_loop(0, rows // 256, chunk, 0)


def scatter_kernel(in_deg, src_ref, wt_ref, g2_ref, own_ref, halo_ref, wts, *bufs):
    rows, halo = own_ref.shape[1], halo_ref.shape[0]
    masks = row_masks()
    fill_weights(wt_ref, wts)

    def zero(i, _):
        for b in bufs:
            for t in range(2):
                b[t, pl.ds(pl.multiple_of(i * 80, 16), 80), :] = jnp.zeros((80, LANES), F32)
        return 0
    lax.fori_loop(0, bufs[0].shape[1] // 80, zero, 0)

    def body(g, _):
        blk = src_ref.at[g // 8, :, pl.ds((g % 8) * 16, 16)]
        gg = g2_ref[pl.ds(pl.multiple_of(g * 16, 16), 16), :].astype(F32)
        for h in range(2):
            w8 = wts[pl.ds(pl.multiple_of(g * 16, 16) + 8 * h, 8), :]
            gs = [gg[8 * h:8 * h + 8, t * LANES:(t + 1) * LANES] for t in range(2)]
            terms = []
            for k in range(in_deg):
                wk = jnp.broadcast_to(w8[:, k:k + 1], (8, LANES))
                terms.append([wk * x for x in gs])
            for r in range(8):
                for k in range(in_deg):
                    start = blk[k, 8 * h + r] + (PAD - r)
                    for t in range(2):
                        win = bufs[k].at[t, pl.ds(start, 8), :]
                        pltpu.store(win, win[...] + terms[k][t], mask=masks[r])
        return 0
    lax.fori_loop(0, rows // 16, body, 0)

    def total(t, o, n):
        s = pl.ds(o + PAD, n)
        a = bufs[0][t, s, :]
        for b in bufs[1:]:
            a = a + b[t, s, :]
        return a

    def red_own(o):
        for t in range(2):
            own_ref[t, pl.ds(o, 64), :] = total(t, o, 64)
    chunked(rows, 64, red_own)

    def red_halo(q, _):
        o = pl.multiple_of(rows + q * 64, 64)
        d = pl.multiple_of(q * 96, 32)
        halo_ref[pl.ds(d, 64), :] = total(0, o, 64)
        a, b = total(1, o, 32), total(1, o + 32, 32)
        halo_ref[pl.ds(d + 64, 32), :] = a + pltpu.roll(b, 64, 1)
        return 0
    lax.fori_loop(0, halo // 96, red_halo, 0)


def combine_kernel(list_ref, own_ref, back_ref, z_ref, w1_ref, w2t_ref, gw1_ref, *sc):
    bufs, w2p = sc[:-1], sc[-1]
    nb = len(bufs)
    rows = own_ref.shape[1]
    masks = row_masks()

    def init(o):
        for t in range(2):
            bufs[0][t, pl.ds(o + PAD, 256), :] = own_ref[t, pl.ds(o, 256), :]
            for b in bufs[1:]:
                b[t, pl.ds(o + PAD, 256), :] = jnp.zeros((256, LANES), F32)
    chunked(rows, 256, init)
    low = lax.broadcasted_iota(jnp.int32, (8, LANES), 1) < 64

    def body(q, _):
        for half in range(2):
            for h in range(4):
                blk = list_ref.at[pl.ds(pl.multiple_of(q * 64, 64) + half * 32 + h * 8, 8)]
                d = pl.multiple_of(q * 96, 32)
                lo = back_ref[pl.ds(d + half * 32 + h * 8, 8), :]
                hi = back_ref[pl.ds(d + 64 + h * 8, 8), :]
                hi = jnp.where(low, hi if half == 0 else pltpu.roll(hi, 64, 1), 0.0)
                for r in range(8):
                    b = bufs[r % nb]
                    start = blk[r] + (PAD - r)
                    for t, x in ((0, lo), (1, hi)):
                        win = b.at[t, pl.ds(start, 8), :]
                        pltpu.store(win, win[...] + x, mask=masks[r])
        return 0
    lax.fori_loop(0, back_ref.shape[0] // 96, body, 0)

    w1 = w1_ref[...].astype(BF16)
    w2p[...] = jnp.zeros_like(w2p)
    w2p[pl.ds(0, w2t_ref.shape[0]), :] = w2t_ref[...].astype(BF16)
    gw1_ref[...] = jnp.zeros_like(gw1_ref)

    def finish(o):
        z = z_ref[pl.ds(o, 256), :]
        h = hidden(z, w1)
        halves = []
        for t in range(2):
            a = bufs[0][t, pl.ds(o + PAD, 256), :]
            for b in bufs[1:]:
                a = a + b[t, pl.ds(o + PAD, 256), :]
            halves.append(a)
        x = jnp.concatenate(halves, 1)
        x1 = x.astype(BF16)
        rest = x - x1.astype(F32)
        x2 = rest.astype(BF16)
        x3 = (rest - x2.astype(F32)).astype(BF16)
        w2 = w2p[...]
        dh = dot(x3, w2, ((1,), (0,))) + dot(x2, w2, ((1,), (0,))) + dot(x1, w2, ((1,), (0,)))
        g1 = jnp.where(h.astype(F32) > 0, dh, 0.0).astype(BF16)
        gw1_ref[...] += dot(z, g1, ((0,), (0,)))
    chunked(rows, 256, finish)


def solution(mesh):
    dev_count = mesh.shape["graph"]

    def device_step(feats, w_one, w_two, send_idx, send_count, edge_src, edge_wt, labels, label_mask):
        rows, feat_in = feats.shape
        hid, classes = w_two.shape
        halo_rows = send_idx.shape[1]
        in_deg = edge_src.shape[1]
        halo = dev_count * halo_rows
        ext = rows + halo + 2 * PAD
        blocks = rows // LANES
        pad_cls = -(-classes // 16) * 16
        list_ids = send_idx.reshape(halo)
        src = edge_src.T.reshape(in_deg, blocks, LANES).transpose(1, 0, 2)
        wt = jnp.pad(edge_wt.T, ((0, 8 - in_deg), (0, 0)))
        w2t = jnp.pad(w_two.T, ((0, pad_cls - classes), (0, 0)))
        total = lax.psum(jnp.sum(label_mask.astype(F32)), "graph")

        def exchange(x, n):
            return lax.all_to_all(x.reshape(dev_count, n, x.shape[1]), "graph", 0, 0, tiled=True).reshape(x.shape)

        out0 = pl.pallas_call(
            pick_kernel, out_shape=jax.ShapeDtypeStruct((halo, feat_in), BF16), in_specs=[SMEM, VMEM], out_specs=VMEM,
            scratch_shapes=[pltpu.VMEM((rows + 2 * PAD, feat_in), F32)], compiler_params=params(16), name="pick",
        )(list_ids, feats)
        halo0 = exchange(out0, halo_rows)
        z1, out1 = pl.pallas_call(
            functools.partial(layer_one_kernel, in_deg),
            out_shape=[jax.ShapeDtypeStruct((rows, feat_in), BF16), jax.ShapeDtypeStruct((halo, feat_in), BF16)],
            in_specs=[SMEM, SMEM, VMEM, VMEM, VMEM], out_specs=[VMEM, VMEM],
            scratch_shapes=[pltpu.VMEM((ext, feat_in), F32), pltpu.VMEM((rows, 8), F32), pltpu.VMEM((rows + 2 * PAD, feat_in), F32)],
            compiler_params=params(32), name="layer_one",
        )(src, list_ids, wt, feats, halo0)
        zh = exchange(out1, halo_rows)
        g2, gw2t, loss_part = pl.pallas_call(
            functools.partial(layer_two_kernel, in_deg, classes),
            out_shape=[jax.ShapeDtypeStruct((rows, 2 * LANES), BF16), jax.ShapeDtypeStruct((pad_cls, hid), F32), jax.ShapeDtypeStruct((1, 256), F32)],
            in_specs=[SMEM, SMEM, VMEM, VMEM, VMEM, VMEM, VMEM, VMEM, VMEM], out_specs=[VMEM, VMEM, VMEM],
            scratch_shapes=[pltpu.VMEM((ext, LANES), F32), pltpu.VMEM((ext, LANES), F32), pltpu.VMEM((rows, 8), F32), pltpu.VMEM((rows, hid), BF16)],
            compiler_params=params(40), name="layer_two",
        )(src, total.reshape(1), wt, z1, zh, w_one, w2t, labels.reshape(rows // 256, 256), label_mask.reshape(rows // 256, 256))
        own, halo_g = pl.pallas_call(
            functools.partial(scatter_kernel, in_deg),
            out_shape=[jax.ShapeDtypeStruct((2, rows, LANES), F32), jax.ShapeDtypeStruct((halo * 3 // 2, LANES), F32)],
            in_specs=[SMEM, VMEM, VMEM], out_specs=[VMEM, VMEM],
            scratch_shapes=[pltpu.VMEM((rows, 8), F32)] + [pltpu.VMEM((2, ext, LANES), F32)] * in_deg,
            compiler_params=params(60), name="scatter",
        )(src, wt, g2)
        back = exchange(halo_g, halo_rows * 3 // 2)
        gw1 = pl.pallas_call(
            combine_kernel, out_shape=jax.ShapeDtypeStruct((feat_in, hid), F32),
            in_specs=[SMEM, VMEM, VMEM, VMEM, VMEM, VMEM], out_specs=VMEM,
            scratch_shapes=[pltpu.VMEM((2, rows + 2 * PAD, LANES), F32)] * 4 + [pltpu.VMEM((2 * LANES, hid), BF16)],
            compiler_params=params(48), name="combine",
        )(list_ids, own, back, z1, w_one, w2t)
        loss, gw1, gw2t = lax.psum((jnp.sum(loss_part), gw1, gw2t), "graph")
        return -loss / total, gw1, gw2t[:classes].T

    row_spec = P("graph", None)
    vec_spec = P("graph")
    return jax.shard_map(device_step, mesh=mesh, in_specs=(row_spec, P(), P(), row_spec, vec_spec, row_spec, row_spec, vec_spec, vec_spec), out_specs=(P(), P(), P()), check_vma=False)
```

```python
import functools

import jax
import jax.numpy as jnp
from jax import lax
from jax.experimental import pallas as pl
from jax.experimental.pallas import tpu as pltpu
from jax.sharding import PartitionSpec as P

LANES = 128
F32, BF16 = jnp.float32, jnp.bfloat16
VMEM = pl.BlockSpec(memory_space=pltpu.VMEM)
SMEM = pl.BlockSpec(memory_space=pltpu.SMEM)
MESH = pl.DeviceIdType.MESH


def params(limit_mib):
    return pltpu.CompilerParams(vmem_limit_bytes=limit_mib * 2**20)


def row_masks():
    sub = lax.broadcasted_iota(jnp.int32, (8, LANES), 0)
    return [sub == r for r in range(8)]


def dot(a, b, dims):
    return lax.dot_general(a, b, (dims, ((), ())), preferred_element_type=F32)


def fill_weights(wt_ref, wts_ref):
    def body(j, _):
        s = pl.ds(pl.multiple_of(j * LANES, LANES), LANES)
        wts_ref[s, :] = wt_ref[:, s].T
        return 0
    lax.fori_loop(0, wt_ref.shape[1] // LANES, body, 0)


def pick_rows(tbl, parts, ids, masks):
    outs = []
    for t in range(parts):
        v = None
        for r in range(8):
            row = jnp.broadcast_to(tbl[t, pl.ds(ids[r], 1), :], (8, LANES))
            v = row if v is None else jnp.where(masks[r], row, v)
        outs.append(v)
    return outs


def gather_sum(src_ref, wts_ref, tbl, parts, masks, g, rows, in_deg):
    per = LANES // rows
    blk = src_ref.at[g // per, :, pl.ds((g % per) * rows, rows)]
    out = []
    for h in range(rows // 8):
        w8 = wts_ref[pl.ds(pl.multiple_of(g * rows, rows) + 8 * h, 8), :]
        acc = None
        for k in range(in_deg):
            wk = jnp.broadcast_to(w8[:, k:k + 1], (8, LANES))
            vs = pick_rows(tbl, parts, [blk[k, 8 * h + r] for r in range(8)], masks)
            vs = [v * wk for v in vs]
            acc = vs if acc is None else [a + v for a, v in zip(acc, vs)]
        out.append(jnp.concatenate(acc, 1))
    return jnp.concatenate(out, 0)


def send_rows(list_ref, tbl, out_ref, masks):
    blocks, size = out_ref.shape[:2]
    per = size // 16

    def body(g, _):
        blk = list_ref.at[pl.ds(pl.multiple_of(g * 16, 16), 16)]
        parts = [pick_rows(tbl, 1, [blk[8 * h + r] for r in range(8)], masks)[0] for h in range(2)]
        out_ref[g // per, pl.ds(pl.multiple_of(g % per * 16, 16), 16), :] = jnp.concatenate(parts, 0).astype(BF16)
        return 0
    lax.fori_loop(0, blocks * per, body, 0)


def chunked(total, chunk, fn):
    def body(i, _):
        fn(pl.multiple_of(i * chunk, chunk))
        return 0
    lax.fori_loop(0, total // chunk, body, 0)


def enter(n, me):
    barrier = pltpu.get_barrier_semaphore()
    for i in range(1, n):
        pl.semaphore_signal(barrier, inc=1, device_id=((me + i) % n,), device_id_type=MESH)
    return lambda: pl.semaphore_wait(barrier, n - 1)


def all_to_all(n, me, src, dst, send_sem, recv_sem):
    plane = 8 if n % 8 == 0 else n
    steps = sorted(range(n // plane), key=lambda z: -min(z, n // plane - z))
    copies = []
    for dr in range(plane):
        for dz in steps:
            if dr or dz:
                copies.append((dz, dr))
    copies.sort(key=lambda c: -min(c[0], n // plane - c[0]))
    made = []
    for dz, dr in copies:
        peer = ((me // plane + dz) % (n // plane)) * plane + (me % plane + dr) % plane
        i = dz * plane + dr
        made.append(pltpu.make_async_remote_copy(
            src_ref=src.at[peer], dst_ref=dst.at[me], send_sem=send_sem.at[i], recv_sem=recv_sem.at[i],
            device_id=(peer,), device_id_type=MESH))
    for c in made:
        c.start()
    return made


def first_kernel(n, list_ref, own_ref, mask_ref, halo_ref, total_ref, tbl, out, cnt, cnts, sems):
    me = lax.axis_index("graph")
    ready = enter(n, me)
    rows = own_ref.shape[0]
    mine = jnp.sum(mask_ref[...].astype(F32), axis=0, keepdims=True)
    for p in range(n):
        cnt[p] = mine

    def load_own(o):
        tbl[0, pl.ds(o, 256), :] = own_ref[pl.ds(o, 256), :].astype(F32)
    chunked(rows, 256, load_own)
    send_rows(list_ref, tbl, out, row_masks())
    ready()
    small = all_to_all(n, me, cnt, cnts, sems.at[0], sems.at[1])
    big = all_to_all(n, me, out, halo_ref, sems.at[2], sems.at[3])
    halo_ref[pl.ds(me, 1)] = out[pl.ds(me, 1)]
    cnts[pl.ds(me, 1)] = cnt[pl.ds(me, 1)]
    for c in small:
        c.wait()
    total_ref[0] = jnp.sum(jnp.sum(cnts[...], axis=0))
    for c in big:
        c.wait()


def exchange_kernel(n, x_ref, o_ref, sems):
    me = lax.axis_index("graph")
    enter(n, me)()
    copies = all_to_all(n, me, x_ref, o_ref, sems.at[0], sems.at[1])
    o_ref[pl.ds(me, 1)] = x_ref[pl.ds(me, 1)]
    for c in copies:
        c.wait()


def reduce_kernel(n, classes, gw1_ref, gw2t_ref, loss_ref, total_ref, o1_ref, o2_ref, ol_ref, full, pair, acc, ring, half, sems):
    chips = n // 2
    me = lax.axis_index("graph")
    chip, core = me // 2, me % 2
    ready = enter(n, me)
    full[...] = jnp.zeros_like(full)

    def tiles(rows):
        return [(i, t) for i in range(rows // 8) for t in range(2)]
    where_ = {}
    at = 0
    for name, ref, rows in (("a", gw1_ref, gw1_ref.shape[0]), ("b", gw2t_ref, gw2t_ref.shape[0])):
        for i, t in tiles(rows):
            where_[name, i, t] = (at // (3 * chips), at // 3 % chips, at % 3)
            full[where_[name, i, t]] = ref[8 * i:8 * i + 8, t * LANES:(t + 1) * LANES]
            at += 1
    last = (at // (3 * chips), at // 3 % chips, at % 3)
    full[last[0], last[1], last[2], 0:1] = loss_ref[:, :LANES] + loss_ref[:, LANES:]
    ready()
    partner = me + 1 - 2 * core
    swap = pltpu.make_async_remote_copy(src_ref=full.at[1 - core], dst_ref=pair, send_sem=sems.at[0, 0], recv_sem=sems.at[1, 0],
                                        device_id=(partner,), device_id_type=MESH)
    swap.start()
    swap.wait()
    acc[...] = pair[...] + full[core]

    def others(src_of, dst, s):
        made = []
        for i in sorted(range(1, chips), key=lambda i: -min(i // 4, chips // 4 - i // 4)):
            other = (chip + i) % chips
            made.append(pltpu.make_async_remote_copy(
                src_ref=src_of(other), dst_ref=dst, send_sem=sems.at[s, i], recv_sem=sems.at[s + 1, i],
                device_id=(2 * other + core,), device_id_type=MESH))
        for c in made:
            c.start()
        return made
    first = others(lambda other: acc.at[other], ring.at[chip], 2)
    ring[pl.ds(chip, 1)] = acc[pl.ds(chip, 1)]
    for c in first:
        c.wait()
    half[pl.ds(core, 1), pl.ds(chip, 1)] = jnp.sum(ring[...], axis=0)[None, None]
    second = others(lambda other: half.at[core, chip], half.at[core, chip], 4)
    for c in second:
        c.wait()
    back = pltpu.make_async_remote_copy(src_ref=half.at[core], dst_ref=half.at[core], send_sem=sems.at[0, 1], recv_sem=sems.at[1, 1],
                                        device_id=(partner,), device_id_type=MESH)
    back.start()
    back.wait()
    for name, ref, rows in (("a", o1_ref, o1_ref.shape[0]), ("b", o2_ref, gw2t_ref.shape[0])):
        for i, t in tiles(rows):
            n_rows = min(8, ref.shape[0] - 8 * i)
            ref[8 * i:8 * i + n_rows, t * LANES:(t + 1) * LANES] = half[where_[name, i, t]][:n_rows]
    ol_ref[0] = -jnp.sum(half[last]) / total_ref[0]


def layer_one_kernel(in_deg, src_ref, list_ref, wt_ref, own_ref, halo_ref, z_ref, out_ref, tbl, wts, ztbl):
    rows, halo = own_ref.shape[0], halo_ref.shape[0]
    masks = row_masks()
    fill_weights(wt_ref, wts)

    def load_own(o):
        tbl[0, pl.ds(o, 256), :] = own_ref[pl.ds(o, 256), :].astype(F32)

    def load_halo(o):
        tbl[0, pl.ds(o + rows, 256), :] = halo_ref[pl.ds(o, 256), :].astype(F32)
    chunked(rows, 256, load_own)
    chunked(halo, 256, load_halo)

    def body(g, _):
        z = gather_sum(src_ref, wts, tbl, 1, masks, g, 32, in_deg).astype(BF16)
        z_ref[pl.ds(pl.multiple_of(g * 32, 32), 32), :] = z
        ztbl[0, pl.ds(pl.multiple_of(g * 32, 32), 32), :] = z.astype(F32)
        return 0
    lax.fori_loop(0, rows // 32, body, 0)
    send_rows(list_ref, ztbl, out_ref, masks)


def hidden(z, w1):
    return jnp.maximum(dot(z, w1, ((1,), (0,))), 0.0).astype(BF16)


def layer_two_kernel(in_deg, classes, src_ref, total_ref, wt_ref, z_own_ref, z_halo_ref, w1_ref, w2t_ref, lab_ref, mask_ref,
                     g2_ref, gw2t_ref, loss_ref, tbl, wts, z2):
    rows, halo = z_own_ref.shape[0], z_halo_ref.shape[0]
    masks = row_masks()
    fill_weights(wt_ref, wts)
    w1 = w1_ref[...].astype(BF16)

    def load(ref, base):
        def fn(o):
            h = hidden(ref[pl.ds(o, 256), :], w1).astype(F32)
            tbl[0, pl.ds(o + base, 256), :] = h[:, :LANES]
            tbl[1, pl.ds(o + base, 256), :] = h[:, LANES:]
        return fn
    chunked(rows, 256, load(z_own_ref, 0))
    chunked(halo, 256, load(z_halo_ref, rows))

    def body(g, _):
        z2[pl.ds(pl.multiple_of(g * 16, 16), 16), :] = gather_sum(src_ref, wts, tbl, 2, masks, g, 16, in_deg).astype(BF16)
        return 0
    lax.fori_loop(0, rows // 16, body, 0)

    total = total_ref[0]
    w2t = w2t_ref[...].astype(BF16)
    pad_cls = w2t.shape[0]
    gw2t_ref[...] = jnp.zeros_like(gw2t_ref)
    loss_ref[...] = jnp.zeros_like(loss_ref)
    cls = lax.broadcasted_iota(jnp.int32, (pad_cls, 256), 0)

    def chunk(i, _):
        o = pl.multiple_of(i * 256, 256)
        zc = z2[pl.ds(o, 256), :]
        logits = dot(w2t, zc, ((1,), (1,)))
        live = cls < classes
        lab = lab_ref[pl.ds(i, 1), :]
        mf = mask_ref[pl.ds(i, 1), :].astype(F32)
        top = jnp.max(jnp.where(live, logits, -jnp.inf), axis=0, keepdims=True)
        shifted = logits - top
        ex = jnp.where(live, jnp.exp(shifted), 0.0)
        logp = shifted - jnp.log(jnp.sum(ex, axis=0, keepdims=True))
        hot = (cls == lab).astype(F32)
        loss_ref[...] += jnp.sum(mf * hot * logp, axis=0, keepdims=True)
        prob = jnp.where(live, jnp.exp(logp), 0.0)
        g2t = ((prob - hot) * (mf / total)).astype(BF16)
        gw2t_ref[...] += dot(g2t, zc, ((1,), (0,)))
        g2 = jnp.concatenate([g2t.astype(F32), jnp.zeros((2 * LANES - pad_cls, 256), F32)], 0).T
        g2_ref[pl.ds(o, 256), :] = g2.astype(BF16)
        return 0
    lax.fori_loop(0, rows // 256, chunk, 0)


def scatter_kernel(in_deg, src_ref, wt_ref, g2_ref, own_ref, halo_ref, wts, *bufs):
    rows, nodes = own_ref.shape[1], halo_ref.shape[0]
    fill_weights(wt_ref, wts)

    def zero(i, _):
        for b in bufs:
            for t in range(2):
                b[t, pl.ds(pl.multiple_of(i * 64, 64), 64), :] = jnp.zeros((64, LANES), F32)
        return 0
    lax.fori_loop(0, bufs[0].shape[1] // 64, zero, 0)

    def body(g, _):
        blk = src_ref.at[g // 8, :, pl.ds((g % 8) * 16, 16)]
        gg = g2_ref[pl.ds(pl.multiple_of(g * 16, 16), 16), :].astype(F32)
        for h in range(2):
            w8 = wts[pl.ds(pl.multiple_of(g * 16, 16) + 8 * h, 8), :]
            gs = [gg[8 * h:8 * h + 8, t * LANES:(t + 1) * LANES] for t in range(2)]
            terms = []
            for k in range(in_deg):
                wk = jnp.broadcast_to(w8[:, k:k + 1], (8, LANES))
                terms.append([wk * x for x in gs])
            for r in range(8):
                for k in range(in_deg):
                    i = blk[k, 8 * h + r]
                    for t in range(2):
                        row = jnp.broadcast_to(bufs[k][t, pl.ds(i, 1), :], (8, LANES)) + terms[k][t]
                        bufs[k][t, pl.ds(i, 1), :] = row[r:r + 1, :]
        return 0
    lax.fori_loop(0, rows // 16, body, 0)

    def total(t, o, n):
        s = pl.ds(o, n)
        a = bufs[0][t, s, :]
        for b in bufs[1:]:
            a = a + b[t, s, :]
        return a

    def red_own(o):
        for t in range(2):
            own_ref[t, pl.ds(o, 64), :] = total(t, o, 64)
    chunked(rows, 64, red_own)

    def red_halo(q, _):
        o = pl.multiple_of(rows + q * 64, 64)
        halo_ref[q, pl.ds(0, 64), :] = total(0, o, 64)
        a, b = total(1, o, 32), total(1, o + 32, 32)
        halo_ref[q, pl.ds(64, 32), :] = a + pltpu.roll(b, 64, 1)
        return 0
    lax.fori_loop(0, nodes, red_halo, 0)


def combine_kernel(list_ref, own_ref, back_ref, z_ref, w1_ref, w2t_ref, gw1_ref, *sc):
    bufs, w2p = sc[:-1], sc[-1]
    nb = len(bufs)
    rows = own_ref.shape[1]

    def init(o):
        for t in range(2):
            bufs[0][t, pl.ds(o, 256), :] = own_ref[t, pl.ds(o, 256), :]
            for b in bufs[1:]:
                b[t, pl.ds(o, 256), :] = jnp.zeros((256, LANES), F32)
    chunked(rows, 256, init)
    low = lax.broadcasted_iota(jnp.int32, (8, LANES), 1) < 64

    def body(q, _):
        for half in range(2):
            for h in range(4):
                blk = list_ref.at[pl.ds(pl.multiple_of(q * 64, 64) + half * 32 + h * 8, 8)]
                lo = back_ref[q, pl.ds(half * 32 + h * 8, 8), :]
                hi = back_ref[q, pl.ds(64 + h * 8, 8), :]
                hi = jnp.where(low, hi if half == 0 else pltpu.roll(hi, 64, 1), 0.0)
                for r in range(8):
                    b = bufs[r % nb]
                    i = blk[r]
                    for t, x in ((0, lo), (1, hi)):
                        row = jnp.broadcast_to(b[t, pl.ds(i, 1), :], (8, LANES)) + x
                        b[t, pl.ds(i, 1), :] = row[r:r + 1, :]
        return 0
    lax.fori_loop(0, back_ref.shape[0], body, 0)

    w1 = w1_ref[...].astype(BF16)
    w2p[...] = jnp.zeros_like(w2p)
    w2p[pl.ds(0, w2t_ref.shape[0]), :] = w2t_ref[...].astype(BF16)
    gw1_ref[...] = jnp.zeros_like(gw1_ref)

    def finish(o):
        z = z_ref[pl.ds(o, 256), :]
        h = hidden(z, w1)
        halves = []
        for t in range(2):
            a = bufs[0][t, pl.ds(o, 256), :]
            for b in bufs[1:]:
                a = a + b[t, pl.ds(o, 256), :]
            halves.append(a)
        x = jnp.concatenate(halves, 1)
        x1 = x.astype(BF16)
        rest = x - x1.astype(F32)
        x2 = rest.astype(BF16)
        x3 = (rest - x2.astype(F32)).astype(BF16)
        w2 = w2p[...]
        dh = dot(x3, w2, ((1,), (0,))) + dot(x2, w2, ((1,), (0,))) + dot(x1, w2, ((1,), (0,)))
        g1 = jnp.where(h.astype(F32) > 0, dh, 0.0).astype(BF16)
        gw1_ref[...] += dot(z, g1, ((0,), (0,)))
    chunked(rows, 256, finish)


def solution(mesh):
    dev_count = mesh.shape["graph"]

    def device_step(feats, w_one, w_two, send_idx, send_count, edge_src, edge_wt, labels, label_mask):
        rows, feat_in = feats.shape
        hid, classes = w_two.shape
        halo_rows = send_idx.shape[1]
        in_deg = edge_src.shape[1]
        halo = dev_count * halo_rows
        ext = rows + halo
        blocks = rows // LANES
        pad_cls = -(-classes // 16) * 16
        list_ids = send_idx.reshape(halo)
        src = edge_src.T.reshape(in_deg, blocks, LANES).transpose(1, 0, 2)
        wt = jnp.pad(edge_wt.T, ((0, 8 - in_deg), (0, 0)))
        w2t = jnp.pad(w_two.T, ((0, pad_cls - classes), (0, 0)))

        def comm(limit_mib, cid):
            return pltpu.CompilerParams(vmem_limit_bytes=limit_mib * 2**20,
                                        collective_id=cid, has_side_effects=True)

        def exchange(x, cid):
            return pl.pallas_call(
                functools.partial(exchange_kernel, dev_count), out_shape=jax.ShapeDtypeStruct(x.shape, x.dtype),
                in_specs=[VMEM], out_specs=VMEM, scratch_shapes=[pltpu.SemaphoreType.DMA((2, dev_count))],
                compiler_params=comm(8, cid), name="exchange",
            )(x)

        halo0, total = pl.pallas_call(
            functools.partial(first_kernel, dev_count),
            out_shape=[jax.ShapeDtypeStruct((dev_count, halo_rows, feat_in), BF16), jax.ShapeDtypeStruct((1,), F32)],
            in_specs=[SMEM, VMEM, VMEM], out_specs=[VMEM, SMEM],
            scratch_shapes=[pltpu.VMEM((1, rows, feat_in), F32), pltpu.VMEM((dev_count, halo_rows, feat_in), BF16),
                            pltpu.VMEM((dev_count, 1, LANES), F32), pltpu.VMEM((dev_count, 1, LANES), F32),
                            pltpu.SemaphoreType.DMA((4, dev_count))],
            compiler_params=comm(16, 0), name="first",
        )(list_ids, feats, label_mask.reshape(blocks, LANES))
        z1, out1 = pl.pallas_call(
            functools.partial(layer_one_kernel, in_deg),
            out_shape=[jax.ShapeDtypeStruct((rows, feat_in), BF16), jax.ShapeDtypeStruct((dev_count, halo_rows, feat_in), BF16)],
            in_specs=[SMEM, SMEM, VMEM, VMEM, VMEM], out_specs=[VMEM, VMEM],
            scratch_shapes=[pltpu.VMEM((1, ext, feat_in), F32), pltpu.VMEM((rows, 8), F32), pltpu.VMEM((1, rows, feat_in), F32)],
            compiler_params=params(16), name="layer_one",
        )(src, list_ids, wt, feats, halo0.reshape(halo, feat_in))
        zh = exchange(out1, 1).reshape(halo, feat_in)
        g2, gw2t, loss_part = pl.pallas_call(
            functools.partial(layer_two_kernel, in_deg, classes),
            out_shape=[jax.ShapeDtypeStruct((rows, 2 * LANES), BF16), jax.ShapeDtypeStruct((pad_cls, hid), F32), jax.ShapeDtypeStruct((1, 256), F32)],
            in_specs=[SMEM, SMEM, VMEM, VMEM, VMEM, VMEM, VMEM, VMEM, VMEM], out_specs=[VMEM, VMEM, VMEM],
            scratch_shapes=[pltpu.VMEM((2, ext, LANES), F32), pltpu.VMEM((rows, 8), F32), pltpu.VMEM((rows, hid), BF16)],
            compiler_params=params(24), name="layer_two",
        )(src, total, wt, z1, zh, w_one, w2t, labels.reshape(rows // 256, 256), label_mask.reshape(rows // 256, 256))
        own, halo_g = pl.pallas_call(
            functools.partial(scatter_kernel, in_deg),
            out_shape=[jax.ShapeDtypeStruct((2, rows, LANES), F32), jax.ShapeDtypeStruct((dev_count, halo_rows * 3 // 2, LANES), F32)],
            in_specs=[SMEM, VMEM, VMEM], out_specs=[VMEM, VMEM],
            scratch_shapes=[pltpu.VMEM((rows, 8), F32)] + [pltpu.VMEM((2, ext, LANES), F32)] * in_deg,
            compiler_params=params(50), name="scatter",
        )(src, wt, g2)
        back = exchange(halo_g, 2)
        gw1 = pl.pallas_call(
            combine_kernel, out_shape=jax.ShapeDtypeStruct((feat_in, hid), F32),
            in_specs=[SMEM, VMEM, VMEM, VMEM, VMEM, VMEM], out_specs=VMEM,
            scratch_shapes=[pltpu.VMEM((2, rows, LANES), F32)] * 4 + [pltpu.VMEM((2 * LANES, hid), BF16)],
            compiler_params=params(30), name="combine",
        )(list_ids, own, back, z1, w_one, w2t)
        chips = dev_count // 2
        gw1, gw2t, loss = pl.pallas_call(
            functools.partial(reduce_kernel, dev_count, classes),
            out_shape=[jax.ShapeDtypeStruct((feat_in, hid), F32), jax.ShapeDtypeStruct((classes, hid), F32), jax.ShapeDtypeStruct((1,), F32)],
            in_specs=[VMEM, VMEM, VMEM, SMEM], out_specs=[VMEM, VMEM, SMEM],
            scratch_shapes=[pltpu.VMEM((2, chips, 3, 8, LANES), F32), pltpu.VMEM((chips, 3, 8, LANES), F32), pltpu.VMEM((chips, 3, 8, LANES), F32),
                            pltpu.VMEM((chips, 3, 8, LANES), F32), pltpu.VMEM((2, chips, 3, 8, LANES), F32), pltpu.SemaphoreType.DMA((6, dev_count))],
            compiler_params=comm(8, 3), name="reduce",
        )(gw1, gw2t, loss_part, total)
        return loss[0], gw1, gw2t.T

    row_spec = P("graph", None)
    vec_spec = P("graph")
    return jax.shard_map(device_step, mesh=mesh, in_specs=(row_spec, P(), P(), row_spec, vec_spec, row_spec, row_spec, vec_spec, vec_spec), out_specs=(P(), P(), P()), check_vma=False)
```

```python
import functools

import jax
import jax.numpy as jnp
from jax import lax
from jax.experimental import pallas as pl
from jax.experimental.pallas import tpu as pltpu
from jax.sharding import PartitionSpec as P

LANES = 128
F32, BF16 = jnp.float32, jnp.bfloat16
VMEM = pl.BlockSpec(memory_space=pltpu.VMEM)
SMEM = pl.BlockSpec(memory_space=pltpu.SMEM)
MESH = pl.DeviceIdType.MESH


def params(limit_mib):
    return pltpu.CompilerParams(vmem_limit_bytes=limit_mib * 2**20)


def row_masks():
    sub = lax.broadcasted_iota(jnp.int32, (8, LANES), 0)
    return [sub == r for r in range(8)]


def dot(a, b, dims):
    return lax.dot_general(a, b, (dims, ((), ())), preferred_element_type=F32)


def fill_weights(wt_ref, wts_ref):
    def body(j, _):
        s = pl.ds(pl.multiple_of(j * LANES, LANES), LANES)
        wts_ref[s, :] = wt_ref[:, s].T
        return 0
    lax.fori_loop(0, wt_ref.shape[1] // LANES, body, 0)


def pick_rows(tbl, parts, ids, masks):
    outs = []
    for t in range(parts):
        v = None
        for r in range(8):
            row = jnp.broadcast_to(tbl[t, pl.ds(ids[r], 1), :], (8, LANES))
            v = row if v is None else jnp.where(masks[r], row, v)
        outs.append(v)
    return outs


def gather_sum(src_ref, wts_ref, tbl, parts, masks, g, rows, in_deg):
    per = LANES // rows
    blk = src_ref.at[g // per, :, pl.ds((g % per) * rows, rows)]
    out = []
    for h in range(rows // 8):
        w8 = wts_ref[pl.ds(pl.multiple_of(g * rows, rows) + 8 * h, 8), :]
        acc = None
        for k in range(in_deg):
            wk = jnp.broadcast_to(w8[:, k:k + 1], (8, LANES))
            vs = pick_rows(tbl, parts, [blk[k, 8 * h + r] for r in range(8)], masks)
            vs = [v * wk for v in vs]
            acc = vs if acc is None else [a + v for a, v in zip(acc, vs)]
        out.append(jnp.concatenate(acc, 1))
    return jnp.concatenate(out, 0)


def send_rows(list_ref, tbl, out_ref, masks):
    blocks, size = out_ref.shape[:2]
    per = size // 16

    def body(g, _):
        blk = list_ref.at[pl.ds(pl.multiple_of(g * 16, 16), 16)]
        parts = [pick_rows(tbl, 1, [blk[8 * h + r] for r in range(8)], masks)[0] for h in range(2)]
        out_ref[g // per, pl.ds(pl.multiple_of(g % per * 16, 16), 16), :] = jnp.concatenate(parts, 0).astype(BF16)
        return 0
    lax.fori_loop(0, blocks * per, body, 0)


def chunked(total, chunk, fn):
    def body(i, _):
        fn(pl.multiple_of(i * chunk, chunk))
        return 0
    lax.fori_loop(0, total // chunk, body, 0)


def enter(n, me):
    barrier = pltpu.get_barrier_semaphore()
    for i in range(1, n):
        pl.semaphore_signal(barrier, inc=1, device_id=((me + i) % n,), device_id_type=MESH)
    return lambda: pl.semaphore_wait(barrier, n - 1)


def all_to_all(n, me, src, dst, send_sem, recv_sem):
    plane = 8 if n % 8 == 0 else n
    steps = sorted(range(n // plane), key=lambda z: -min(z, n // plane - z))
    copies = []
    for dr in range(plane):
        for dz in steps:
            if dr or dz:
                copies.append((dz, dr))
    copies.sort(key=lambda c: -min(c[0], n // plane - c[0]))
    made = []
    for dz, dr in copies:
        peer = ((me // plane + dz) % (n // plane)) * plane + (me % plane + dr) % plane
        i = dz * plane + dr
        made.append(pltpu.make_async_remote_copy(
            src_ref=src.at[peer], dst_ref=dst.at[me], send_sem=send_sem.at[i], recv_sem=recv_sem.at[i],
            device_id=(peer,), device_id_type=MESH))
    for c in made:
        c.start()
    return made


def first_kernel(n, list_ref, own_ref, mask_ref, halo_ref, total_ref, tbl, out, cnt, cnts, sems):
    me = lax.axis_index("graph")
    ready = enter(n, me)
    rows = own_ref.shape[0]
    mine = jnp.sum(mask_ref[...].astype(F32), axis=0, keepdims=True)
    for p in range(n):
        cnt[p] = mine

    def load_own(o):
        tbl[0, pl.ds(o, 256), :] = own_ref[pl.ds(o, 256), :].astype(F32)
    chunked(rows, 256, load_own)
    send_rows(list_ref, tbl, out, row_masks())
    ready()
    small = all_to_all(n, me, cnt, cnts, sems.at[0], sems.at[1])
    big = all_to_all(n, me, out, halo_ref, sems.at[2], sems.at[3])
    halo_ref[pl.ds(me, 1)] = out[pl.ds(me, 1)]
    cnts[pl.ds(me, 1)] = cnt[pl.ds(me, 1)]
    for c in small:
        c.wait()
    total_ref[0] = jnp.sum(jnp.sum(cnts[...], axis=0))
    for c in big:
        c.wait()


def exchange_kernel(n, x_ref, o_ref, sems):
    me = lax.axis_index("graph")
    enter(n, me)()
    copies = all_to_all(n, me, x_ref, o_ref, sems.at[0], sems.at[1])
    o_ref[pl.ds(me, 1)] = x_ref[pl.ds(me, 1)]
    for c in copies:
        c.wait()


def reduce_kernel(n, classes, gw1_ref, gw2t_ref, loss_ref, total_ref, o1_ref, o2_ref, ol_ref, full, pair, acc, ring, half, sems):
    chips = n // 2
    me = lax.axis_index("graph")
    chip, core = me // 2, me % 2
    ready = enter(n, me)
    full[...] = jnp.zeros_like(full)

    def tiles(rows):
        return [(i, t) for i in range(rows // 8) for t in range(2)]
    where_ = {}
    at = 0
    for name, ref, rows in (("a", gw1_ref, gw1_ref.shape[0]), ("b", gw2t_ref, gw2t_ref.shape[0])):
        for i, t in tiles(rows):
            where_[name, i, t] = (at // (3 * chips), at // 3 % chips, at % 3)
            full[where_[name, i, t]] = ref[8 * i:8 * i + 8, t * LANES:(t + 1) * LANES]
            at += 1
    last = (at // (3 * chips), at // 3 % chips, at % 3)
    full[last[0], last[1], last[2], 0:1] = loss_ref[:, :LANES] + loss_ref[:, LANES:]
    ready()
    partner = me + 1 - 2 * core
    swap = pltpu.make_async_remote_copy(src_ref=full.at[1 - core], dst_ref=pair, send_sem=sems.at[0, 0], recv_sem=sems.at[1, 0],
                                        device_id=(partner,), device_id_type=MESH)
    swap.start()
    swap.wait()
    acc[...] = pair[...] + full[core]

    def others(src_of, dst, s):
        made = []
        for i in sorted(range(1, chips), key=lambda i: -min(i // 4, chips // 4 - i // 4)):
            other = (chip + i) % chips
            made.append(pltpu.make_async_remote_copy(
                src_ref=src_of(other), dst_ref=dst, send_sem=sems.at[s, i], recv_sem=sems.at[s + 1, i],
                device_id=(2 * other + core,), device_id_type=MESH))
        for c in made:
            c.start()
        return made
    first = others(lambda other: acc.at[other], ring.at[chip], 2)
    ring[pl.ds(chip, 1)] = acc[pl.ds(chip, 1)]
    for c in first:
        c.wait()
    half[pl.ds(core, 1), pl.ds(chip, 1)] = jnp.sum(ring[...], axis=0)[None, None]
    second = others(lambda other: half.at[core, chip], half.at[core, chip], 4)
    for c in second:
        c.wait()
    back = pltpu.make_async_remote_copy(src_ref=half.at[core], dst_ref=half.at[core], send_sem=sems.at[0, 1], recv_sem=sems.at[1, 1],
                                        device_id=(partner,), device_id_type=MESH)
    back.start()
    back.wait()
    for name, ref, rows in (("a", o1_ref, o1_ref.shape[0]), ("b", o2_ref, gw2t_ref.shape[0])):
        for i, t in tiles(rows):
            n_rows = min(8, ref.shape[0] - 8 * i)
            ref[8 * i:8 * i + n_rows, t * LANES:(t + 1) * LANES] = half[where_[name, i, t]][:n_rows]
    ol_ref[0] = -jnp.sum(half[last]) / total_ref[0]


def layer_one_kernel(in_deg, src_ref, list_ref, wt_ref, own_ref, halo_ref, z_ref, out_ref, tbl, wts, ztbl):
    rows, halo = own_ref.shape[0], halo_ref.shape[0]
    masks = row_masks()
    fill_weights(wt_ref, wts)

    def load_own(o):
        tbl[0, pl.ds(o, 256), :] = own_ref[pl.ds(o, 256), :].astype(F32)

    def load_halo(o):
        tbl[0, pl.ds(o + rows, 256), :] = halo_ref[pl.ds(o, 256), :].astype(F32)
    chunked(rows, 256, load_own)
    chunked(halo, 256, load_halo)

    def body(g, _):
        z = gather_sum(src_ref, wts, tbl, 1, masks, g, 32, in_deg).astype(BF16)
        z_ref[pl.ds(pl.multiple_of(g * 32, 32), 32), :] = z
        ztbl[0, pl.ds(pl.multiple_of(g * 32, 32), 32), :] = z.astype(F32)
        return 0
    lax.fori_loop(0, rows // 32, body, 0)
    send_rows(list_ref, ztbl, out_ref, masks)


def hidden(z, w1):
    return jnp.maximum(dot(z, w1, ((1,), (0,))), 0.0).astype(BF16)


def layer_two_kernel(in_deg, classes, src_ref, total_ref, wt_ref, z_own_ref, z_halo_ref, w1_ref, w2t_ref, lab_ref, mask_ref,
                     g2_ref, gw2t_ref, loss_ref, tbl, wts, z2):
    rows, halo = z_own_ref.shape[0], z_halo_ref.shape[0]
    masks = row_masks()
    fill_weights(wt_ref, wts)
    w1 = w1_ref[...].astype(BF16)

    def load(ref, base):
        def fn(o):
            h = hidden(ref[pl.ds(o, 256), :], w1).astype(F32)
            tbl[0, pl.ds(o + base, 256), :] = h[:, :LANES]
            tbl[1, pl.ds(o + base, 256), :] = h[:, LANES:]
        return fn
    chunked(rows, 256, load(z_own_ref, 0))
    chunked(halo, 256, load(z_halo_ref, rows))

    def body(g, _):
        z2[pl.ds(pl.multiple_of(g * 16, 16), 16), :] = gather_sum(src_ref, wts, tbl, 2, masks, g, 16, in_deg).astype(BF16)
        return 0
    lax.fori_loop(0, rows // 16, body, 0)

    total = total_ref[0]
    w2t = w2t_ref[...].astype(BF16)
    pad_cls = w2t.shape[0]
    gw2t_ref[...] = jnp.zeros_like(gw2t_ref)
    loss_ref[...] = jnp.zeros_like(loss_ref)
    cls = lax.broadcasted_iota(jnp.int32, (pad_cls, 256), 0)

    def chunk(i, _):
        o = pl.multiple_of(i * 256, 256)
        zc = z2[pl.ds(o, 256), :]
        logits = dot(w2t, zc, ((1,), (1,)))
        live = cls < classes
        lab = lab_ref[pl.ds(i, 1), :]
        mf = mask_ref[pl.ds(i, 1), :].astype(F32)
        top = jnp.max(jnp.where(live, logits, -jnp.inf), axis=0, keepdims=True)
        shifted = logits - top
        ex = jnp.where(live, jnp.exp(shifted), 0.0)
        logp = shifted - jnp.log(jnp.sum(ex, axis=0, keepdims=True))
        hot = (cls == lab).astype(F32)
        loss_ref[...] += jnp.sum(mf * hot * logp, axis=0, keepdims=True)
        prob = jnp.where(live, jnp.exp(logp), 0.0)
        g2t = ((prob - hot) * (mf / total)).astype(BF16)
        gw2t_ref[...] += dot(g2t, zc, ((1,), (0,)))
        g2 = jnp.concatenate([g2t.astype(F32), jnp.zeros((2 * LANES - pad_cls, 256), F32)], 0).T
        g2_ref[pl.ds(o, 256), :] = g2.astype(BF16)
        return 0
    lax.fori_loop(0, rows // 256, chunk, 0)


def scatter_kernel(in_deg, src_ref, wt_ref, g2_ref, own_ref, halo_ref, wts, *bufs):
    rows, nodes = own_ref.shape[1], halo_ref.shape[0]
    fill_weights(wt_ref, wts)

    def zero(i, _):
        for b in bufs:
            for t in range(2):
                b[t, pl.ds(pl.multiple_of(i * 64, 64), 64), :] = jnp.zeros((64, LANES), F32)
        return 0
    lax.fori_loop(0, bufs[0].shape[1] // 64, zero, 0)

    def body(g, _):
        blk = src_ref.at[g // 8, :, pl.ds((g % 8) * 16, 16)]
        gg = g2_ref[pl.ds(pl.multiple_of(g * 16, 16), 16), :].astype(F32)
        for h in range(2):
            w8 = wts[pl.ds(pl.multiple_of(g * 16, 16) + 8 * h, 8), :]
            gs = [gg[8 * h:8 * h + 8, t * LANES:(t + 1) * LANES] for t in range(2)]
            terms = []
            for k in range(in_deg):
                wk = jnp.broadcast_to(w8[:, k:k + 1], (8, LANES))
                terms.append([wk * x for x in gs])
            for r in range(8):
                for k in range(in_deg):
                    i = blk[k, 8 * h + r]
                    for t in range(2):
                        row = jnp.broadcast_to(bufs[k][t, pl.ds(i, 1), :], (8, LANES)) + terms[k][t]
                        bufs[k][t, pl.ds(i, 1), :] = row[r:r + 1, :]
        return 0
    lax.fori_loop(0, rows // 16, body, 0)

    def total(t, o, n):
        s = pl.ds(o, n)
        a = bufs[0][t, s, :]
        for b in bufs[1:]:
            a = a + b[t, s, :]
        return a

    def red_own(o):
        for t in range(2):
            own_ref[t, pl.ds(o, 64), :] = total(t, o, 64)
    chunked(rows, 64, red_own)

    def red_halo(q, _):
        o = pl.multiple_of(rows + q * 64, 64)
        halo_ref[q, pl.ds(0, 64), :] = total(0, o, 64)
        a, b = total(1, o, 32), total(1, o + 32, 32)
        halo_ref[q, pl.ds(64, 32), :] = a + pltpu.roll(b, 64, 1)
        return 0
    lax.fori_loop(0, nodes, red_halo, 0)


def combine_kernel(list_ref, own_ref, back_ref, z_ref, w1_ref, w2t_ref, gw1_ref, *sc):
    bufs, w2p = sc[:-1], sc[-1]
    nb = len(bufs)
    rows = own_ref.shape[1]

    def init(o):
        for t in range(2):
            bufs[0][t, pl.ds(o, 256), :] = own_ref[t, pl.ds(o, 256), :]
            for b in bufs[1:]:
                b[t, pl.ds(o, 256), :] = jnp.zeros((256, LANES), F32)
    chunked(rows, 256, init)
    low = lax.broadcasted_iota(jnp.int32, (8, LANES), 1) < 64

    def body(q, _):
        for half in range(2):
            for h in range(4):
                blk = list_ref.at[pl.ds(pl.multiple_of(q * 64, 64) + half * 32 + h * 8, 8)]
                lo = back_ref[q, pl.ds(half * 32 + h * 8, 8), :]
                hi = back_ref[q, pl.ds(64 + h * 8, 8), :]
                hi = jnp.where(low, hi if half == 0 else pltpu.roll(hi, 64, 1), 0.0)
                for r in range(8):
                    b = bufs[r % nb]
                    i = blk[r]
                    for t, x in ((0, lo), (1, hi)):
                        row = jnp.broadcast_to(b[t, pl.ds(i, 1), :], (8, LANES)) + x
                        b[t, pl.ds(i, 1), :] = row[r:r + 1, :]
        return 0
    lax.fori_loop(0, back_ref.shape[0], body, 0)

    w1 = w1_ref[...].astype(BF16)
    w2p[...] = jnp.zeros_like(w2p)
    w2p[pl.ds(0, w2t_ref.shape[0]), :] = w2t_ref[...].astype(BF16)
    gw1_ref[...] = jnp.zeros_like(gw1_ref)

    def finish(o):
        z = z_ref[pl.ds(o, 256), :]
        h = hidden(z, w1)
        halves = []
        for t in range(2):
            a = bufs[0][t, pl.ds(o, 256), :]
            for b in bufs[1:]:
                a = a + b[t, pl.ds(o, 256), :]
            halves.append(a)
        x = jnp.concatenate(halves, 1)
        x1 = x.astype(BF16)
        rest = x - x1.astype(F32)
        x2 = rest.astype(BF16)
        x3 = (rest - x2.astype(F32)).astype(BF16)
        w2 = w2p[...]
        dh = dot(x3, w2, ((1,), (0,))) + dot(x2, w2, ((1,), (0,))) + dot(x1, w2, ((1,), (0,)))
        g1 = jnp.where(h.astype(F32) > 0, dh, 0.0).astype(BF16)
        gw1_ref[...] += dot(z, g1, ((0,), (0,)))
    chunked(rows, 256, finish)


def solution(mesh):
    dev_count = mesh.shape["graph"]

    def device_step(feats, w_one, w_two, send_idx, send_count, edge_src, edge_wt, labels, label_mask):
        rows, feat_in = feats.shape
        hid, classes = w_two.shape
        halo_rows = send_idx.shape[1]
        in_deg = edge_src.shape[1]
        halo = dev_count * halo_rows
        ext = rows + halo + 16
        blocks = rows // LANES
        pad_cls = -(-classes // 16) * 16
        list_ids = send_idx.reshape(halo)
        src = edge_src.T.reshape(in_deg, blocks, LANES).transpose(1, 0, 2)
        wt = jnp.pad(edge_wt.T, ((0, 8 - in_deg), (0, 0)))
        w2t = jnp.pad(w_two.T, ((0, pad_cls - classes), (0, 0)))

        def comm(limit_mib, cid):
            return pltpu.CompilerParams(vmem_limit_bytes=limit_mib * 2**20,
                                        collective_id=cid, has_side_effects=True)

        def exchange(x, cid):
            return pl.pallas_call(
                functools.partial(exchange_kernel, dev_count), out_shape=jax.ShapeDtypeStruct(x.shape, x.dtype),
                in_specs=[VMEM], out_specs=VMEM, scratch_shapes=[pltpu.SemaphoreType.DMA((2, dev_count))],
                compiler_params=comm(8, cid), name="exchange",
            )(x)

        halo0, total = pl.pallas_call(
            functools.partial(first_kernel, dev_count),
            out_shape=[jax.ShapeDtypeStruct((dev_count, halo_rows, feat_in), BF16), jax.ShapeDtypeStruct((1,), F32)],
            in_specs=[SMEM, VMEM, VMEM], out_specs=[VMEM, SMEM],
            scratch_shapes=[pltpu.VMEM((1, rows, feat_in), F32), pltpu.VMEM((dev_count, halo_rows, feat_in), BF16),
                            pltpu.VMEM((dev_count, 1, LANES), F32), pltpu.VMEM((dev_count, 1, LANES), F32),
                            pltpu.SemaphoreType.DMA((4, dev_count))],
            compiler_params=comm(16, 0), name="first",
        )(list_ids, feats, label_mask.reshape(blocks, LANES))
        z1, out1 = pl.pallas_call(
            functools.partial(layer_one_kernel, in_deg),
            out_shape=[jax.ShapeDtypeStruct((rows, feat_in), BF16), jax.ShapeDtypeStruct((dev_count, halo_rows, feat_in), BF16)],
            in_specs=[SMEM, SMEM, VMEM, VMEM, VMEM], out_specs=[VMEM, VMEM],
            scratch_shapes=[pltpu.VMEM((1, ext, feat_in), F32), pltpu.VMEM((rows, 8), F32), pltpu.VMEM((1, rows, feat_in), F32)],
            compiler_params=params(16), name="layer_one",
        )(src, list_ids, wt, feats, halo0.reshape(halo, feat_in))
        zh = exchange(out1, 1).reshape(halo, feat_in)
        g2, gw2t, loss_part = pl.pallas_call(
            functools.partial(layer_two_kernel, in_deg, classes),
            out_shape=[jax.ShapeDtypeStruct((rows, 2 * LANES), BF16), jax.ShapeDtypeStruct((pad_cls, hid), F32), jax.ShapeDtypeStruct((1, 256), F32)],
            in_specs=[SMEM, SMEM, VMEM, VMEM, VMEM, VMEM, VMEM, VMEM, VMEM], out_specs=[VMEM, VMEM, VMEM],
            scratch_shapes=[pltpu.VMEM((2, ext, LANES), F32), pltpu.VMEM((rows, 8), F32), pltpu.VMEM((rows, hid), BF16)],
            compiler_params=params(24), name="layer_two",
        )(src, total, wt, z1, zh, w_one, w2t, labels.reshape(rows // 256, 256), label_mask.reshape(rows // 256, 256))
        own, halo_g = pl.pallas_call(
            functools.partial(scatter_kernel, in_deg),
            out_shape=[jax.ShapeDtypeStruct((2, rows, LANES), F32), jax.ShapeDtypeStruct((dev_count, halo_rows * 3 // 2, LANES), F32)],
            in_specs=[SMEM, VMEM, VMEM], out_specs=[VMEM, VMEM],
            scratch_shapes=[pltpu.VMEM((rows, 8), F32)] + [pltpu.VMEM((2, ext, LANES), F32)] * in_deg,
            compiler_params=params(50), name="scatter",
        )(src, wt, g2)
        back = exchange(halo_g, 2)
        gw1 = pl.pallas_call(
            combine_kernel, out_shape=jax.ShapeDtypeStruct((feat_in, hid), F32),
            in_specs=[SMEM, VMEM, VMEM, VMEM, VMEM, VMEM], out_specs=VMEM,
            scratch_shapes=[pltpu.VMEM((2, rows + 16, LANES), F32)] * 4 + [pltpu.VMEM((2 * LANES, hid), BF16)],
            compiler_params=params(30), name="combine",
        )(list_ids, own, back, z1, w_one, w2t)
        chips = dev_count // 2
        gw1, gw2t, loss = pl.pallas_call(
            functools.partial(reduce_kernel, dev_count, classes),
            out_shape=[jax.ShapeDtypeStruct((feat_in, hid), F32), jax.ShapeDtypeStruct((classes, hid), F32), jax.ShapeDtypeStruct((1,), F32)],
            in_specs=[VMEM, VMEM, VMEM, SMEM], out_specs=[VMEM, VMEM, SMEM],
            scratch_shapes=[pltpu.VMEM((2, chips, 3, 8, LANES), F32), pltpu.VMEM((chips, 3, 8, LANES), F32), pltpu.VMEM((chips, 3, 8, LANES), F32),
                            pltpu.VMEM((chips, 3, 8, LANES), F32), pltpu.VMEM((2, chips, 3, 8, LANES), F32), pltpu.SemaphoreType.DMA((6, dev_count))],
            compiler_params=comm(8, 3), name="reduce",
        )(gw1, gw2t, loss_part, total)
        return loss[0], gw1, gw2t.T

    row_spec = P("graph", None)
    vec_spec = P("graph")
    return jax.shard_map(device_step, mesh=mesh, in_specs=(row_spec, P(), P(), row_spec, vec_spec, row_spec, row_spec, vec_spec, vec_spec), out_specs=(P(), P(), P()), check_vma=False)
```

```python
import functools

import jax
import jax.numpy as jnp
from jax import lax
from jax.experimental import pallas as pl
from jax.experimental.pallas import tpu as pltpu
from jax.sharding import PartitionSpec as P

LANES = 128
F32, BF16 = jnp.float32, jnp.bfloat16
VMEM = pl.BlockSpec(memory_space=pltpu.VMEM)
SMEM = pl.BlockSpec(memory_space=pltpu.SMEM)
ANY = pl.BlockSpec(memory_space=pl.ANY)
MESH = pl.DeviceIdType.MESH


def params(limit_mib):
    return pltpu.CompilerParams(vmem_limit_bytes=limit_mib * 2**20)


def row_masks():
    sub = lax.broadcasted_iota(jnp.int32, (8, LANES), 0)
    return [sub == r for r in range(8)]


def dot(a, b, dims):
    return lax.dot_general(a, b, (dims, ((), ())), preferred_element_type=F32)


def fill_weights(wt_ref, wts_ref):
    deg = wt_ref.shape[0]

    def body(j, _):
        s = pl.ds(pl.multiple_of(j * LANES, LANES), LANES)
        wts_ref[s, :] = jnp.concatenate([wt_ref[:, s], jnp.zeros((8 - deg, LANES), F32)], 0).T
        return 0
    lax.fori_loop(0, wt_ref.shape[1] // LANES, body, 0)


def load_edges(src_any, src_ref, sem):
    copy = pltpu.make_async_copy(src_any, src_ref, sem)
    copy.start()
    return copy


def pick_rows(tbl, parts, ids, masks):
    outs = []
    for t in range(parts):
        v = None
        for r in range(8):
            row = jnp.broadcast_to(tbl[t, pl.ds(ids[r], 1), :], (8, LANES))
            v = row if v is None else jnp.where(masks[r], row, v)
        outs.append(v)
    return outs


def gather_sum(src_ref, wts_ref, tbl, parts, masks, g, rows, in_deg):
    per = LANES // rows
    blk = src_ref.at[g // per, :, pl.ds((g % per) * rows, rows)]
    out = []
    for h in range(rows // 8):
        w8 = wts_ref[pl.ds(pl.multiple_of(g * rows, rows) + 8 * h, 8), :]
        acc = None
        for k in range(in_deg):
            wk = jnp.broadcast_to(w8[:, k:k + 1], (8, LANES))
            vs = pick_rows(tbl, parts, [blk[k, 8 * h + r] for r in range(8)], masks)
            vs = [v * wk for v in vs]
            acc = vs if acc is None else [a + v for a, v in zip(acc, vs)]
        out.append(jnp.concatenate(acc, 1))
    return jnp.concatenate(out, 0)


def send_rows(list_ref, tbl, out_ref, masks):
    blocks, size = out_ref.shape[:2]
    per = size // 16

    def body(g, _):
        blk = list_ref.at[g // per, pl.ds(pl.multiple_of(g % per * 16, 16), 16)]
        parts = [pick_rows(tbl, 1, [blk[8 * h + r] for r in range(8)], masks)[0] for h in range(2)]
        out_ref[g // per, pl.ds(pl.multiple_of(g % per * 16, 16), 16), :] = jnp.concatenate(parts, 0).astype(BF16)
        return 0
    lax.fori_loop(0, blocks * per, body, 0)


def chunked(total, chunk, fn):
    def body(i, _):
        fn(pl.multiple_of(i * chunk, chunk))
        return 0
    lax.fori_loop(0, total // chunk, body, 0)


def enter(n, me):
    barrier = pltpu.get_barrier_semaphore()
    for i in range(1, n):
        pl.semaphore_signal(barrier, inc=1, device_id=((me + i) % n,), device_id_type=MESH)
    return lambda: pl.semaphore_wait(barrier, n - 1)


def all_to_all(n, me, src, dst, send_sem, recv_sem):
    plane = 8 if n % 8 == 0 else n
    steps = sorted(range(n // plane), key=lambda z: -min(z, n // plane - z))
    copies = []
    for dr in range(plane):
        for dz in steps:
            if dr or dz:
                copies.append((dz, dr))
    copies.sort(key=lambda c: -min(c[0], n // plane - c[0]))
    made = []
    for dz, dr in copies:
        peer = ((me // plane + dz) % (n // plane)) * plane + (me % plane + dr) % plane
        i = dz * plane + dr
        made.append(pltpu.make_async_remote_copy(
            src_ref=src.at[peer], dst_ref=dst.at[me], send_sem=send_sem.at[i], recv_sem=recv_sem.at[i],
            device_id=(peer,), device_id_type=MESH))
    for c in made:
        c.start()
    return made


def first_kernel(n, list_ref, own_ref, mask_ref, halo_ref, total_ref, tbl, out, cnt, cnts, sems):
    me = lax.axis_index("graph")
    ready = enter(n, me)
    rows = own_ref.shape[0]
    mine = jnp.sum(mask_ref[...].astype(F32), axis=0, keepdims=True)
    for p in range(n):
        cnt[p] = mine

    def load_own(o):
        tbl[0, pl.ds(o, 256), :] = own_ref[pl.ds(o, 256), :].astype(F32)
    chunked(rows, 256, load_own)
    send_rows(list_ref, tbl, out, row_masks())
    ready()
    small = all_to_all(n, me, cnt, cnts, sems.at[0], sems.at[1])
    big = all_to_all(n, me, out, halo_ref, sems.at[2], sems.at[3])
    halo_ref[pl.ds(me, 1)] = out[pl.ds(me, 1)]
    cnts[pl.ds(me, 1)] = cnt[pl.ds(me, 1)]
    for c in small:
        c.wait()
    total_ref[0] = jnp.sum(jnp.sum(cnts[...], axis=0))
    for c in big:
        c.wait()


def exchange_kernel(n, x_ref, o_ref, sems):
    me = lax.axis_index("graph")
    enter(n, me)()
    copies = all_to_all(n, me, x_ref, o_ref, sems.at[0], sems.at[1])
    o_ref[pl.ds(me, 1)] = x_ref[pl.ds(me, 1)]
    for c in copies:
        c.wait()


def reduce_kernel(n, classes, gw1_ref, gw2t_ref, loss_ref, total_ref, o1_ref, o2_ref, ol_ref, full, pair, acc, ring, half, sems):
    chips = n // 2
    me = lax.axis_index("graph")
    chip, core = me // 2, me % 2
    ready = enter(n, me)
    full[...] = jnp.zeros_like(full)

    def tiles(rows):
        return [(i, t) for i in range(rows // 8) for t in range(2)]
    where_ = {}
    at = 0
    for name, ref, rows in (("a", gw1_ref, gw1_ref.shape[0]), ("b", gw2t_ref, gw2t_ref.shape[0])):
        for i, t in tiles(rows):
            where_[name, i, t] = (at // (3 * chips), at // 3 % chips, at % 3)
            full[where_[name, i, t]] = ref[8 * i:8 * i + 8, t * LANES:(t + 1) * LANES]
            at += 1
    last = (at // (3 * chips), at // 3 % chips, at % 3)
    full[last[0], last[1], last[2], 0:1] = loss_ref[:, :LANES] + loss_ref[:, LANES:]
    ready()
    partner = me + 1 - 2 * core
    swap = pltpu.make_async_remote_copy(src_ref=full.at[1 - core], dst_ref=pair, send_sem=sems.at[0, 0], recv_sem=sems.at[1, 0],
                                        device_id=(partner,), device_id_type=MESH)
    swap.start()
    swap.wait()
    acc[...] = pair[...] + full[core]

    def others(src_of, dst, s):
        made = []
        for i in sorted(range(1, chips), key=lambda i: -min(i // 4, chips // 4 - i // 4)):
            other = (chip + i) % chips
            made.append(pltpu.make_async_remote_copy(
                src_ref=src_of(other), dst_ref=dst, send_sem=sems.at[s, i], recv_sem=sems.at[s + 1, i],
                device_id=(2 * other + core,), device_id_type=MESH))
        for c in made:
            c.start()
        return made
    first = others(lambda other: acc.at[other], ring.at[chip], 2)
    ring[pl.ds(chip, 1)] = acc[pl.ds(chip, 1)]
    for c in first:
        c.wait()
    half[pl.ds(core, 1), pl.ds(chip, 1)] = jnp.sum(ring[...], axis=0)[None, None]
    second = others(lambda other: half.at[core, chip], half.at[core, chip], 4)
    for c in second:
        c.wait()
    back = pltpu.make_async_remote_copy(src_ref=half.at[core], dst_ref=half.at[core], send_sem=sems.at[0, 1], recv_sem=sems.at[1, 1],
                                        device_id=(partner,), device_id_type=MESH)
    back.start()
    back.wait()
    for name, ref, rows in (("a", o1_ref, o1_ref.shape[0]), ("b", o2_ref, gw2t_ref.shape[0])):
        for i, t in tiles(rows):
            n_rows = min(8, ref.shape[0] - 8 * i)
            ref[8 * i:8 * i + n_rows, t * LANES:(t + 1) * LANES] = half[where_[name, i, t]][:n_rows]
    ol_ref[0] = -jnp.sum(half[last]) / total_ref[0]


def layer_one_kernel(in_deg, src_any, list_ref, wt_ref, own_ref, halo_ref, z_ref, out_ref, tbl, wts, ztbl, src_ref, sem):
    edges = load_edges(src_any, src_ref, sem)
    rows, halo = own_ref.shape[0], halo_ref.shape[0]
    masks = row_masks()
    fill_weights(wt_ref, wts)

    def load_own(o):
        tbl[0, pl.ds(o, 256), :] = own_ref[pl.ds(o, 256), :].astype(F32)

    def load_halo(o):
        tbl[0, pl.ds(o + rows, 256), :] = halo_ref[pl.ds(o, 256), :].astype(F32)
    chunked(rows, 256, load_own)
    chunked(halo, 256, load_halo)
    edges.wait()

    def body(g, _):
        z = gather_sum(src_ref, wts, tbl, 1, masks, g, 32, in_deg).astype(BF16)
        z_ref[pl.ds(pl.multiple_of(g * 32, 32), 32), :] = z
        ztbl[0, pl.ds(pl.multiple_of(g * 32, 32), 32), :] = z.astype(F32)
        return 0
    lax.fori_loop(0, rows // 32, body, 0)
    send_rows(list_ref, ztbl, out_ref, masks)


def hidden(z, w1):
    return jnp.maximum(dot(z, w1, ((1,), (0,))), 0.0).astype(BF16)


def layer_two_kernel(in_deg, src_any, total_ref, wt_ref, z_own_ref, z_halo_ref, w1_ref, w2t_ref, lab_ref, mask_ref,
                     g2_ref, gw2t_ref, loss_ref, tbl, wts, z2, w2s, src_ref, sem):
    edges = load_edges(src_any, src_ref, sem)
    classes = w2t_ref.shape[0]
    rows, halo = z_own_ref.shape[0], z_halo_ref.shape[0]
    masks = row_masks()
    fill_weights(wt_ref, wts)
    w1 = w1_ref[...].astype(BF16)

    def load(ref, base):
        def fn(o):
            h = hidden(ref[pl.ds(o, 256), :], w1).astype(F32)
            tbl[0, pl.ds(o + base, 256), :] = h[:, :LANES]
            tbl[1, pl.ds(o + base, 256), :] = h[:, LANES:]
        return fn
    chunked(rows, 256, load(z_own_ref, 0))
    chunked(halo, 256, load(z_halo_ref, rows))
    edges.wait()

    def body(g, _):
        z2[pl.ds(pl.multiple_of(g * 32, 32), 32), :] = gather_sum(src_ref, wts, tbl, 2, masks, g, 32, in_deg).astype(BF16)
        return 0
    lax.fori_loop(0, rows // 32, body, 0)

    total = total_ref[0]
    w2s[...] = jnp.zeros_like(w2s)
    w2s[pl.ds(0, classes), :] = w2t_ref[...].astype(BF16)
    w2t = w2s[...]
    pad_cls = w2t.shape[0]
    gw2t_ref[...] = jnp.zeros_like(gw2t_ref)
    loss_ref[...] = jnp.zeros_like(loss_ref)
    cls = lax.broadcasted_iota(jnp.int32, (pad_cls, 256), 0)

    def chunk(i, _):
        o = pl.multiple_of(i * 256, 256)
        zc = z2[pl.ds(o, 256), :]
        logits = dot(w2t, zc, ((1,), (1,)))
        live = cls < classes
        lab = jnp.concatenate([lab_ref[pl.ds(2 * i + t, 1), :] for t in range(2)], 1)
        mf = jnp.concatenate([mask_ref[pl.ds(2 * i + t, 1), :] for t in range(2)], 1).astype(F32)
        top = jnp.max(jnp.where(live, logits, -jnp.inf), axis=0, keepdims=True)
        shifted = logits - top
        ex = jnp.where(live, jnp.exp(shifted), 0.0)
        logp = shifted - jnp.log(jnp.sum(ex, axis=0, keepdims=True))
        hot = (cls == lab).astype(F32)
        loss_ref[...] += jnp.sum(mf * hot * logp, axis=0, keepdims=True)
        prob = jnp.where(live, jnp.exp(logp), 0.0)
        g2t = ((prob - hot) * (mf / total)).astype(BF16)
        gw2t_ref[...] += dot(g2t, zc, ((1,), (0,)))
        g2 = jnp.concatenate([g2t.astype(F32), jnp.zeros((2 * LANES - pad_cls, 256), F32)], 0).T
        g2_ref[pl.ds(o, 256), :] = g2.astype(BF16)
        return 0
    lax.fori_loop(0, rows // 256, chunk, 0)


def scatter_kernel(in_deg, src_any, wt_ref, g2_ref, own_ref, halo_ref, src_ref, sem, wts, *bufs):
    edges = load_edges(src_any, src_ref, sem)
    rows, nodes = own_ref.shape[1], halo_ref.shape[0]
    fill_weights(wt_ref, wts)

    def zero(i, _):
        for b in bufs:
            for t in range(2):
                b[t, pl.ds(pl.multiple_of(i * 64, 64), 64), :] = jnp.zeros((64, LANES), F32)
        return 0
    lax.fori_loop(0, bufs[0].shape[1] // 64, zero, 0)
    edges.wait()

    def body(g, _):
        blk = src_ref.at[g // 4, :, pl.ds((g % 4) * 32, 32)]
        gg = g2_ref[pl.ds(pl.multiple_of(g * 32, 32), 32), :].astype(F32)
        for h in range(4):
            w8 = wts[pl.ds(pl.multiple_of(g * 32, 32) + 8 * h, 8), :]
            gs = [gg[8 * h:8 * h + 8, t * LANES:(t + 1) * LANES] for t in range(2)]
            terms = []
            for k in range(in_deg):
                wk = jnp.broadcast_to(w8[:, k:k + 1], (8, LANES))
                terms.append([wk * x for x in gs])
            for r in range(8):
                for k in range(in_deg):
                    i = blk[k, 8 * h + r]
                    for t in range(2):
                        row = jnp.broadcast_to(bufs[k][t, pl.ds(i, 1), :], (8, LANES)) + terms[k][t]
                        bufs[k][t, pl.ds(i, 1), :] = row[r:r + 1, :]
        return 0
    lax.fori_loop(0, rows // 32, body, 0)

    def total(t, o, n):
        s = pl.ds(o, n)
        a = bufs[0][t, s, :]
        for b in bufs[1:]:
            a = a + b[t, s, :]
        return a

    def red_own(o):
        for t in range(2):
            own_ref[t, pl.ds(o, 64), :] = total(t, o, 64)
    chunked(rows, 64, red_own)

    def red_halo(q, _):
        o = pl.multiple_of(rows + q * 64, 64)
        halo_ref[q, pl.ds(0, 64), :] = total(0, o, 64)
        a, b = total(1, o, 32), total(1, o + 32, 32)
        halo_ref[q, pl.ds(64, 32), :] = a + pltpu.roll(b, 64, 1)
        return 0
    lax.fori_loop(0, nodes, red_halo, 0)


def combine_kernel(list_ref, own_ref, back_ref, z_ref, w1_ref, w2t_ref, gw1_ref, *sc):
    bufs, w2p = sc[:-1], sc[-1]
    nb = len(bufs)
    rows = own_ref.shape[1]

    def init(o):
        for t in range(2):
            bufs[0][t, pl.ds(o, 256), :] = own_ref[t, pl.ds(o, 256), :]
            for b in bufs[1:]:
                b[t, pl.ds(o, 256), :] = jnp.zeros((256, LANES), F32)
    chunked(rows, 256, init)
    low = lax.broadcasted_iota(jnp.int32, (8, LANES), 1) < 64

    def body(q, _):
        for half in range(2):
            for h in range(4):
                blk = list_ref.at[q, pl.ds(half * 32 + h * 8, 8)]
                lo = back_ref[q, pl.ds(half * 32 + h * 8, 8), :]
                hi = back_ref[q, pl.ds(64 + h * 8, 8), :]
                hi = jnp.where(low, hi if half == 0 else pltpu.roll(hi, 64, 1), 0.0)
                for r in range(8):
                    b = bufs[r % nb]
                    i = blk[r]
                    for t, x in ((0, lo), (1, hi)):
                        row = jnp.broadcast_to(b[t, pl.ds(i, 1), :], (8, LANES)) + x
                        b[t, pl.ds(i, 1), :] = row[r:r + 1, :]
        return 0
    lax.fori_loop(0, back_ref.shape[0], body, 0)

    w1 = w1_ref[...].astype(BF16)
    w2p[...] = jnp.zeros_like(w2p)
    w2p[pl.ds(0, w2t_ref.shape[0]), :] = w2t_ref[...].astype(BF16)
    gw1_ref[...] = jnp.zeros_like(gw1_ref)

    def finish(o):
        z = z_ref[pl.ds(o, 256), :]
        h = hidden(z, w1)
        halves = []
        for t in range(2):
            a = bufs[0][t, pl.ds(o, 256), :]
            for b in bufs[1:]:
                a = a + b[t, pl.ds(o, 256), :]
            halves.append(a)
        x = jnp.concatenate(halves, 1)
        x1 = x.astype(BF16)
        rest = x - x1.astype(F32)
        x2 = rest.astype(BF16)
        x3 = (rest - x2.astype(F32)).astype(BF16)
        w2 = w2p[...]
        dh = dot(x3, w2, ((1,), (0,))) + dot(x2, w2, ((1,), (0,))) + dot(x1, w2, ((1,), (0,)))
        g1 = jnp.where(h.astype(F32) > 0, dh, 0.0).astype(BF16)
        gw1_ref[...] += dot(z, g1, ((0,), (0,)))
    chunked(rows, 256, finish)


def solution(mesh):
    dev_count = mesh.shape["graph"]

    def device_step(feats, w_one, w_two, send_idx, send_count, edge_src, edge_wt, labels, label_mask):
        rows, feat_in = feats.shape
        hid, classes = w_two.shape
        halo_rows = send_idx.shape[1]
        in_deg = edge_src.shape[1]
        halo = dev_count * halo_rows
        ext = rows + halo + 16
        blocks = rows // LANES
        pad_cls = -(-classes // 16) * 16
        src = edge_src.T.reshape(in_deg, blocks, LANES).transpose(1, 0, 2)
        wt, w2t = edge_wt.T, w_two.T
        edge_ids = pltpu.SMEM((blocks, in_deg, LANES), jnp.int32)

        def comm(limit_mib, cid):
            return pltpu.CompilerParams(vmem_limit_bytes=limit_mib * 2**20,
                                        collective_id=cid, has_side_effects=True)

        def exchange(x, cid):
            return pl.pallas_call(
                functools.partial(exchange_kernel, dev_count), out_shape=jax.ShapeDtypeStruct(x.shape, x.dtype),
                in_specs=[VMEM], out_specs=VMEM, scratch_shapes=[pltpu.SemaphoreType.DMA((2, dev_count))],
                compiler_params=comm(8, cid), name="exchange",
            )(x)

        halo0, total = pl.pallas_call(
            functools.partial(first_kernel, dev_count),
            out_shape=[jax.ShapeDtypeStruct((dev_count, halo_rows, feat_in), BF16), jax.ShapeDtypeStruct((1,), F32)],
            in_specs=[SMEM, VMEM, VMEM], out_specs=[VMEM, SMEM],
            scratch_shapes=[pltpu.VMEM((1, rows, feat_in), F32), pltpu.VMEM((dev_count, halo_rows, feat_in), BF16),
                            pltpu.VMEM((dev_count, 1, LANES), F32), pltpu.VMEM((dev_count, 1, LANES), F32),
                            pltpu.SemaphoreType.DMA((4, dev_count))],
            compiler_params=comm(16, 0), name="first",
        )(send_idx, feats, label_mask.reshape(blocks, LANES))
        z1, out1 = pl.pallas_call(
            functools.partial(layer_one_kernel, in_deg),
            out_shape=[jax.ShapeDtypeStruct((rows, feat_in), BF16), jax.ShapeDtypeStruct((dev_count, halo_rows, feat_in), BF16)],
            in_specs=[ANY, SMEM, VMEM, VMEM, VMEM], out_specs=[VMEM, VMEM],
            scratch_shapes=[pltpu.VMEM((1, ext, feat_in), F32), pltpu.VMEM((rows, 8), F32), pltpu.VMEM((1, rows, feat_in), F32), edge_ids, pltpu.SemaphoreType.DMA],
            compiler_params=params(16), name="layer_one",
        )(src, send_idx, wt, feats, halo0.reshape(halo, feat_in))
        zh = exchange(out1, 1).reshape(halo, feat_in)
        g2, gw2t, loss_part = pl.pallas_call(
            functools.partial(layer_two_kernel, in_deg),
            out_shape=[jax.ShapeDtypeStruct((rows, 2 * LANES), BF16), jax.ShapeDtypeStruct((pad_cls, hid), F32), jax.ShapeDtypeStruct((1, 256), F32)],
            in_specs=[ANY, SMEM, VMEM, VMEM, VMEM, VMEM, VMEM, VMEM, VMEM], out_specs=[VMEM, VMEM, VMEM],
            scratch_shapes=[pltpu.VMEM((2, ext, LANES), F32), pltpu.VMEM((rows, 8), F32), pltpu.VMEM((rows, hid), BF16),
                            pltpu.VMEM((pad_cls, hid), BF16), edge_ids, pltpu.SemaphoreType.DMA],
            compiler_params=params(24), name="layer_two",
        )(src, total, wt, z1, zh, w_one, w2t, labels.reshape(blocks, LANES), label_mask.reshape(blocks, LANES))
        own, halo_g = pl.pallas_call(
            functools.partial(scatter_kernel, in_deg),
            out_shape=[jax.ShapeDtypeStruct((2, rows, LANES), F32), jax.ShapeDtypeStruct((dev_count, halo_rows * 3 // 2, LANES), F32)],
            in_specs=[ANY, VMEM, VMEM], out_specs=[VMEM, VMEM],
            scratch_shapes=[edge_ids, pltpu.SemaphoreType.DMA, pltpu.VMEM((rows, 8), F32)] + [pltpu.VMEM((2, ext, LANES), F32)] * in_deg,
            compiler_params=params(50), name="scatter",
        )(src, wt, g2)
        back = exchange(halo_g, 2)
        gw1 = pl.pallas_call(
            combine_kernel, out_shape=jax.ShapeDtypeStruct((feat_in, hid), F32),
            in_specs=[SMEM, VMEM, VMEM, VMEM, VMEM, VMEM], out_specs=VMEM,
            scratch_shapes=[pltpu.VMEM((2, rows + 16, LANES), F32)] * 4 + [pltpu.VMEM((2 * LANES, hid), BF16)],
            compiler_params=params(30), name="combine",
        )(send_idx, own, back, z1, w_one, w2t)
        chips = dev_count // 2
        gw1, gw2t, loss = pl.pallas_call(
            functools.partial(reduce_kernel, dev_count, classes),
            out_shape=[jax.ShapeDtypeStruct((feat_in, hid), F32), jax.ShapeDtypeStruct((classes, hid), F32), jax.ShapeDtypeStruct((1,), F32)],
            in_specs=[VMEM, VMEM, VMEM, SMEM], out_specs=[VMEM, VMEM, SMEM],
            scratch_shapes=[pltpu.VMEM((2, chips, 3, 8, LANES), F32), pltpu.VMEM((chips, 3, 8, LANES), F32), pltpu.VMEM((chips, 3, 8, LANES), F32),
                            pltpu.VMEM((chips, 3, 8, LANES), F32), pltpu.VMEM((2, chips, 3, 8, LANES), F32), pltpu.SemaphoreType.DMA((6, dev_count))],
            compiler_params=comm(8, 3), name="reduce",
        )(gw1, gw2t, loss_part, total)
        return loss[0], gw1, gw2t.T

    row_spec = P("graph", None)
    vec_spec = P("graph")
    return jax.shard_map(device_step, mesh=mesh, in_specs=(row_spec, P(), P(), row_spec, vec_spec, row_spec, row_spec, vec_spec, vec_spec), out_specs=(P(), P(), P()), check_vma=False)
```

```python
import functools

import jax
import jax.numpy as jnp
from jax import lax
from jax.experimental import pallas as pl
from jax.experimental.pallas import tpu as pltpu
from jax.sharding import PartitionSpec as P

LANES = 128
F32, BF16 = jnp.float32, jnp.bfloat16
VMEM = pl.BlockSpec(memory_space=pltpu.VMEM)
SMEM = pl.BlockSpec(memory_space=pltpu.SMEM)
ANY = pl.BlockSpec(memory_space=pl.ANY)
MESH = pl.DeviceIdType.MESH


def params(limit_mib):
    return pltpu.CompilerParams(vmem_limit_bytes=limit_mib * 2**20)


def row_masks():
    sub = lax.broadcasted_iota(jnp.int32, (8, LANES), 0)
    return [sub == r for r in range(8)]


def dot(a, b, dims):
    return lax.dot_general(a, b, (dims, ((), ())), preferred_element_type=F32)


def fill_weights(wt_ref, wts_ref):
    deg = wt_ref.shape[0]

    def body(j, _):
        s = pl.ds(pl.multiple_of(j * LANES, LANES), LANES)
        wts_ref[s, :] = jnp.concatenate([wt_ref[:, s], jnp.zeros((8 - deg, LANES), F32)], 0).T
        return 0
    lax.fori_loop(0, wt_ref.shape[1] // LANES, body, 0)


RING = 4


def each_block(src_any, ring, sem, fn):
    blocks = src_any.shape[0]

    def copy(j, b):
        return pltpu.make_async_copy(src_any.at[j], ring[b], sem.at[b])

    def start():
        for b in range(RING):
            copy(b, b).start()

    def run():
        def body(i, _):
            for b in range(RING):
                j = i * RING + b
                copy(j, b).wait()
                fn(j, ring[b])

                @pl.when(j + RING < blocks)
                def _():
                    copy(j + RING, b).start()
            return 0
        lax.fori_loop(0, blocks // RING, body, 0)
    return start, run


def pick_rows(tbl, parts, ids, masks):
    outs = []
    for t in range(parts):
        v = None
        for r in range(8):
            row = jnp.broadcast_to(tbl[t, pl.ds(ids[r], 1), :], (8, LANES))
            v = row if v is None else jnp.where(masks[r], row, v)
        outs.append(v)
    return outs


def gather_sum(ids, wts_ref, tbl, parts, masks, j, store):
    for c in range(LANES // 32):
        out = []
        at = pl.multiple_of(j * LANES, LANES) + 32 * c
        for h in range(4):
            w8 = wts_ref[pl.ds(at + 8 * h, 8), :]
            acc = None
            for k in range(ids.shape[0]):
                wk = jnp.broadcast_to(w8[:, k:k + 1], (8, LANES))
                vs = pick_rows(tbl, parts, [ids[k, 32 * c + 8 * h + r] for r in range(8)], masks)
                vs = [v * wk for v in vs]
                acc = vs if acc is None else [a + v for a, v in zip(acc, vs)]
            out.append(jnp.concatenate(acc, 1))
        store(at, jnp.concatenate(out, 0))


def send_rows(list_ref, tbl, out_ref, masks):
    blocks, size = out_ref.shape[:2]

    def body(q, _):
        for g in range(size // 32):
            blk = list_ref.at[q, pl.ds(32 * g, 32)]
            parts = [pick_rows(tbl, 1, [blk[8 * h + r] for r in range(8)], masks)[0] for h in range(4)]
            out_ref[q, pl.ds(32 * g, 32), :] = jnp.concatenate(parts, 0).astype(BF16)
        return 0
    lax.fori_loop(0, blocks, body, 0)


def chunked(total, chunk, fn):
    def body(i, _):
        fn(pl.multiple_of(i * chunk, chunk))
        return 0
    lax.fori_loop(0, total // chunk, body, 0)


def enter(n, me):
    barrier = pltpu.get_barrier_semaphore()
    for i in range(1, n):
        pl.semaphore_signal(barrier, inc=1, device_id=((me + i) % n,), device_id_type=MESH)
    return lambda: pl.semaphore_wait(barrier, n - 1)


def all_to_all(n, me, src, dst, send_sem, recv_sem):
    plane = 8 if n % 8 == 0 else n
    steps = sorted(range(n // plane), key=lambda z: -min(z, n // plane - z))
    copies = []
    for dr in range(plane):
        for dz in steps:
            if dr or dz:
                copies.append((dz, dr))
    copies.sort(key=lambda c: -min(c[0], n // plane - c[0]))
    made = []
    for dz, dr in copies:
        peer = ((me // plane + dz) % (n // plane)) * plane + (me % plane + dr) % plane
        i = dz * plane + dr
        made.append(pltpu.make_async_remote_copy(
            src_ref=src.at[peer], dst_ref=dst.at[me], send_sem=send_sem.at[i], recv_sem=recv_sem.at[i],
            device_id=(peer,), device_id_type=MESH))
    for c in made:
        c.start()
    return made


def first_kernel(n, list_ref, own_ref, mask_ref, halo_ref, total_ref, tbl, out, cnt, cnts, sems):
    me = lax.axis_index("graph")
    ready = enter(n, me)
    rows = own_ref.shape[0]
    mine = jnp.sum(mask_ref[...].astype(F32), axis=0, keepdims=True)
    for p in range(n):
        cnt[p] = mine

    def load_own(o):
        tbl[0, pl.ds(o, 256), :] = own_ref[pl.ds(o, 256), :].astype(F32)
    chunked(rows, 256, load_own)
    send_rows(list_ref, tbl, out, row_masks())
    ready()
    small = all_to_all(n, me, cnt, cnts, sems.at[0], sems.at[1])
    big = all_to_all(n, me, out, halo_ref, sems.at[2], sems.at[3])
    halo_ref[pl.ds(me, 1)] = out[pl.ds(me, 1)]
    cnts[pl.ds(me, 1)] = cnt[pl.ds(me, 1)]
    for c in small:
        c.wait()
    total_ref[0] = jnp.sum(jnp.sum(cnts[...], axis=0))
    for c in big:
        c.wait()


def exchange_kernel(n, x_ref, o_ref, sems):
    me = lax.axis_index("graph")
    enter(n, me)()
    copies = all_to_all(n, me, x_ref, o_ref, sems.at[0], sems.at[1])
    o_ref[pl.ds(me, 1)] = x_ref[pl.ds(me, 1)]
    for c in copies:
        c.wait()


def reduce_kernel(n, classes, gw1_ref, gw2t_ref, loss_ref, total_ref, o1_ref, o2_ref, ol_ref, full, pair, acc, ring, half, sems):
    chips = n // 2
    me = lax.axis_index("graph")
    chip, core = me // 2, me % 2
    ready = enter(n, me)
    full[...] = jnp.zeros_like(full)

    def tiles(rows):
        return [(i, t) for i in range(rows // 8) for t in range(2)]
    where_ = {}
    at = 0
    for name, ref, rows in (("a", gw1_ref, gw1_ref.shape[0]), ("b", gw2t_ref, gw2t_ref.shape[0])):
        for i, t in tiles(rows):
            where_[name, i, t] = (at // (3 * chips), at // 3 % chips, at % 3)
            full[where_[name, i, t]] = ref[8 * i:8 * i + 8, t * LANES:(t + 1) * LANES]
            at += 1
    last = (at // (3 * chips), at // 3 % chips, at % 3)
    full[last[0], last[1], last[2], 0:1] = loss_ref[:, :LANES] + loss_ref[:, LANES:]
    ready()
    partner = me + 1 - 2 * core
    swap = pltpu.make_async_remote_copy(src_ref=full.at[1 - core], dst_ref=pair, send_sem=sems.at[0, 0], recv_sem=sems.at[1, 0],
                                        device_id=(partner,), device_id_type=MESH)
    swap.start()
    swap.wait()
    acc[...] = pair[...] + full[core]

    def others(src_of, dst, s):
        made = []
        for i in sorted(range(1, chips), key=lambda i: -min(i // 4, chips // 4 - i // 4)):
            other = (chip + i) % chips
            made.append(pltpu.make_async_remote_copy(
                src_ref=src_of(other), dst_ref=dst, send_sem=sems.at[s, i], recv_sem=sems.at[s + 1, i],
                device_id=(2 * other + core,), device_id_type=MESH))
        for c in made:
            c.start()
        return made
    first = others(lambda other: acc.at[other], ring.at[chip], 2)
    ring[pl.ds(chip, 1)] = acc[pl.ds(chip, 1)]
    for c in first:
        c.wait()
    half[pl.ds(core, 1), pl.ds(chip, 1)] = jnp.sum(ring[...], axis=0)[None, None]
    second = others(lambda other: half.at[core, chip], half.at[core, chip], 4)
    for c in second:
        c.wait()
    back = pltpu.make_async_remote_copy(src_ref=half.at[core], dst_ref=half.at[core], send_sem=sems.at[0, 1], recv_sem=sems.at[1, 1],
                                        device_id=(partner,), device_id_type=MESH)
    back.start()
    back.wait()
    for name, ref, rows in (("a", o1_ref, o1_ref.shape[0]), ("b", o2_ref, gw2t_ref.shape[0])):
        for i, t in tiles(rows):
            n_rows = min(8, ref.shape[0] - 8 * i)
            ref[8 * i:8 * i + n_rows, t * LANES:(t + 1) * LANES] = half[where_[name, i, t]][:n_rows]
    ol_ref[0] = -jnp.sum(half[last]) / total_ref[0]


def layer_one_kernel(src_any, list_ref, wt_ref, own_ref, halo_ref, z_ref, out_ref, tbl, wts, ztbl, sem, *ring):
    def block(j, ids):
        def store(at, z):
            zb = z.astype(BF16)
            z_ref[pl.ds(at, 32), :] = zb
            ztbl[0, pl.ds(at, 32), :] = zb.astype(F32)
        gather_sum(ids, wts, tbl, 1, masks, j, store)
    start, run = each_block(src_any, ring, sem, block)
    start()
    rows, halo = own_ref.shape[0], halo_ref.shape[0]
    masks = row_masks()
    fill_weights(wt_ref, wts)

    def load_own(o):
        tbl[0, pl.ds(o, 256), :] = own_ref[pl.ds(o, 256), :].astype(F32)

    def load_halo(o):
        tbl[0, pl.ds(o + rows, 256), :] = halo_ref[pl.ds(o, 256), :].astype(F32)
    chunked(rows, 256, load_own)
    chunked(halo, 256, load_halo)
    run()
    send_rows(list_ref, ztbl, out_ref, masks)


def hidden(z, w1):
    return jnp.maximum(dot(z, w1, ((1,), (0,))), 0.0).astype(BF16)


def layer_two_kernel(src_any, total_ref, wt_ref, z_own_ref, z_halo_ref, w1_ref, w2t_ref, lab_ref, mask_ref,
                     g2_ref, gw2t_ref, loss_ref, tbl, wts, z2, w2s, sem, *ring):
    def block(j, ids):
        def store(at, z):
            z2[pl.ds(at, 32), :] = z.astype(BF16)
        gather_sum(ids, wts, tbl, 2, masks, j, store)
    start, run = each_block(src_any, ring, sem, block)
    start()
    classes = w2t_ref.shape[0]
    rows, halo = z_own_ref.shape[0], z_halo_ref.shape[0]
    masks = row_masks()
    fill_weights(wt_ref, wts)
    w1 = w1_ref[...].astype(BF16)

    def load(ref, base):
        def fn(o):
            h = hidden(ref[pl.ds(o, 256), :], w1).astype(F32)
            tbl[0, pl.ds(o + base, 256), :] = h[:, :LANES]
            tbl[1, pl.ds(o + base, 256), :] = h[:, LANES:]
        return fn
    chunked(rows, 256, load(z_own_ref, 0))
    chunked(halo, 256, load(z_halo_ref, rows))
    run()

    total = total_ref[0]
    w2s[...] = jnp.zeros_like(w2s)
    w2s[pl.ds(0, classes), :] = w2t_ref[...].astype(BF16)
    w2t = w2s[...]
    pad_cls = w2t.shape[0]
    gw2t_ref[...] = jnp.zeros_like(gw2t_ref)
    loss_ref[...] = jnp.zeros_like(loss_ref)
    cls = lax.broadcasted_iota(jnp.int32, (pad_cls, 256), 0)

    def chunk(i, _):
        o = pl.multiple_of(i * 256, 256)
        zc = z2[pl.ds(o, 256), :]
        logits = dot(w2t, zc, ((1,), (1,)))
        live = cls < classes
        lab = jnp.concatenate([lab_ref[pl.ds(2 * i + t, 1), :] for t in range(2)], 1)
        mf = jnp.concatenate([mask_ref[pl.ds(2 * i + t, 1), :] for t in range(2)], 1).astype(F32)
        top = jnp.max(jnp.where(live, logits, -jnp.inf), axis=0, keepdims=True)
        shifted = logits - top
        ex = jnp.where(live, jnp.exp(shifted), 0.0)
        norm = jnp.sum(ex, axis=0, keepdims=True)
        logp = shifted - jnp.log(norm)
        hot = cls == lab
        loss_ref[...] += mf * jnp.sum(jnp.where(hot, logp, 0.0), axis=0, keepdims=True)
        g2t = ((ex * (1.0 / norm) - hot.astype(F32)) * (mf / total)).astype(BF16)
        gw2t_ref[...] += dot(g2t, zc, ((1,), (0,)))
        g2 = jnp.concatenate([g2t.astype(F32), jnp.zeros((2 * LANES - pad_cls, 256), F32)], 0).T
        g2_ref[pl.ds(o, 256), :] = g2.astype(BF16)
        return 0
    lax.fori_loop(0, rows // 256, chunk, 0)


PACKED = 88


def in_span(at, rows, width):
    lane = lax.broadcasted_iota(jnp.int32, (rows, LANES), 1)
    return (lane >= at) & (lane < at + width)


def scatter_kernel(in_deg, src_any, wt_ref, g2_ref, own_ref, halo_ref, sem, wts, *more):
    bufs, ring = more[:in_deg], more[in_deg:]

    def block(j, ids):
        for c in range(LANES // 32):
            at = pl.multiple_of(j * LANES, LANES) + 32 * c
            gg = g2_ref[pl.ds(at, 32), :].astype(F32)
            for h in range(4):
                w8 = wts[pl.ds(at + 8 * h, 8), :]
                gs = [gg[8 * h:8 * h + 8, t * LANES:(t + 1) * LANES] for t in range(2)]
                terms = []
                for k in range(in_deg):
                    wk = jnp.broadcast_to(w8[:, k:k + 1], (8, LANES))
                    terms.append([wk * x for x in gs])
                for r in range(8):
                    for k in range(in_deg):
                        i = ids[k, 32 * c + 8 * h + r]
                        for t in range(2):
                            row = jnp.broadcast_to(bufs[k][t, pl.ds(i, 1), :], (8, LANES)) + terms[k][t]
                            bufs[k][t, pl.ds(i, 1), :] = row[r:r + 1, :]
    start, run = each_block(src_any, ring, sem, block)
    start()
    rows, nodes = own_ref.shape[1], halo_ref.shape[0]
    fill_weights(wt_ref, wts)

    def zero(i, _):
        for b in bufs:
            for t in range(2):
                b[t, pl.ds(pl.multiple_of(i * 64, 64), 64), :] = jnp.zeros((64, LANES), F32)
        return 0
    lax.fori_loop(0, bufs[0].shape[1] // 64, zero, 0)
    run()

    def total(t, o, n):
        s = pl.ds(o, n)
        a = bufs[0][t, s, :]
        for b in bufs[1:]:
            a = a + b[t, s, :]
        return a

    def red_own(o):
        for t in range(2):
            own_ref[t, pl.ds(o, 64), :] = total(t, o, 64)
    chunked(rows, 64, red_own)

    def red_halo(q, _):
        o = pl.multiple_of(rows + q * 64, 64)
        halo_ref[q, pl.ds(0, 64), :] = total(0, o, 64)
        hi = total(1, o, 64)
        packed = hi[:16]
        for g in range(1, 4):
            packed = jnp.where(in_span(32 * g, 16, 32), pltpu.roll(hi[16 * g:16 * g + 16], 32 * g, 1), packed)
        halo_ref[q, pl.ds(64, 16), :] = packed
        packed = pltpu.roll(hi[:8], LANES - 32, 1)
        for g in range(1, 8):
            packed = jnp.where(in_span(16 * g, 8, 16), pltpu.roll(hi[8 * g:8 * g + 8], (16 * g - 32) % LANES, 1), packed)
        halo_ref[q, pl.ds(80, 8), :] = packed
        return 0
    lax.fori_loop(0, nodes, red_halo, 0)


def combine_kernel(list_ref, own_ref, back_ref, z_ref, w1_ref, w2t_ref, gw1_ref, *sc):
    bufs, w2p = sc[:-1], sc[-1]
    nb = len(bufs)
    rows = own_ref.shape[1]

    def init(o):
        for t in range(2):
            bufs[0][t, pl.ds(o, 256), :] = own_ref[t, pl.ds(o, 256), :]
            for b in bufs[1:]:
                b[t, pl.ds(o, 256), :] = jnp.zeros((256, LANES), F32)
    chunked(rows, 256, init)
    first, second = in_span(0, 8, 32), in_span(32, 8, 16)

    def body(q, _):
        last = back_ref[q, pl.ds(80, 8), :]
        for g in range(8):
            lo = back_ref[q, pl.ds(8 * g, 8), :]
            mid = back_ref[q, pl.ds(64 + 8 * (g % 2), 8), :]
            mid = mid if g < 2 else pltpu.roll(mid, LANES - 32 * (g // 2), 1)
            tail = pltpu.roll(last, (32 - 16 * g) % LANES, 1) if g != 2 else last
            hi = jnp.where(first, mid, jnp.where(second, tail, 0.0))
            for r in range(8):
                b = bufs[r % nb]
                i = list_ref[q, 8 * g + r]
                for t, x in ((0, lo), (1, hi)):
                    row = jnp.broadcast_to(b[t, pl.ds(i, 1), :], (8, LANES)) + x
                    b[t, pl.ds(i, 1), :] = row[r:r + 1, :]
        return 0
    lax.fori_loop(0, back_ref.shape[0], body, 0)

    w1 = w1_ref[...].astype(BF16)
    w2p[...] = jnp.zeros_like(w2p)
    w2p[pl.ds(0, w2t_ref.shape[0]), :] = w2t_ref[...].astype(BF16)
    gw1_ref[...] = jnp.zeros_like(gw1_ref)

    def finish(o):
        z = z_ref[pl.ds(o, 256), :]
        h = hidden(z, w1)
        halves = []
        for t in range(2):
            a = bufs[0][t, pl.ds(o, 256), :]
            for b in bufs[1:]:
                a = a + b[t, pl.ds(o, 256), :]
            halves.append(a)
        x = jnp.concatenate(halves, 1)
        x1 = x.astype(BF16)
        rest = x - x1.astype(F32)
        x2 = rest.astype(BF16)
        x3 = (rest - x2.astype(F32)).astype(BF16)
        w2 = w2p[...]
        dh = dot(x3, w2, ((1,), (0,))) + dot(x2, w2, ((1,), (0,))) + dot(x1, w2, ((1,), (0,)))
        g1 = jnp.where(h.astype(F32) > 0, dh, 0.0).astype(BF16)
        gw1_ref[...] += dot(z, g1, ((0,), (0,)))
    chunked(rows, 256, finish)


def solution(mesh):
    dev_count = mesh.shape["graph"]

    def device_step(feats, w_one, w_two, send_idx, send_count, edge_src, edge_wt, labels, label_mask):
        rows, feat_in = feats.shape
        hid, classes = w_two.shape
        halo_rows = send_idx.shape[1]
        in_deg = edge_src.shape[1]
        halo = dev_count * halo_rows
        ext = rows + halo + 16
        blocks = rows // LANES
        pad_cls = -(-classes // 16) * 16
        src = edge_src.T.reshape(in_deg, blocks, LANES).transpose(1, 0, 2)
        wt, w2t = edge_wt.T, w_two.T
        edge_ids = [pltpu.SMEM((in_deg, LANES), jnp.int32)] * RING
        edge_sem = pltpu.SemaphoreType.DMA((RING,))

        def comm(limit_mib, cid):
            return pltpu.CompilerParams(vmem_limit_bytes=limit_mib * 2**20,
                                        collective_id=cid, has_side_effects=True)

        def exchange(x, cid):
            return pl.pallas_call(
                functools.partial(exchange_kernel, dev_count), out_shape=jax.ShapeDtypeStruct(x.shape, x.dtype),
                in_specs=[VMEM], out_specs=VMEM, scratch_shapes=[pltpu.SemaphoreType.DMA((2, dev_count))],
                compiler_params=comm(8, cid), name="exchange",
            )(x)

        halo0, total = pl.pallas_call(
            functools.partial(first_kernel, dev_count),
            out_shape=[jax.ShapeDtypeStruct((dev_count, halo_rows, feat_in), BF16), jax.ShapeDtypeStruct((1,), F32)],
            in_specs=[SMEM, VMEM, VMEM], out_specs=[VMEM, SMEM],
            scratch_shapes=[pltpu.VMEM((1, rows, feat_in), F32), pltpu.VMEM((dev_count, halo_rows, feat_in), BF16),
                            pltpu.VMEM((dev_count, 1, LANES), F32), pltpu.VMEM((dev_count, 1, LANES), F32),
                            pltpu.SemaphoreType.DMA((4, dev_count))],
            compiler_params=comm(16, 0), name="first",
        )(send_idx, feats, label_mask.reshape(blocks, LANES))
        z1, out1 = pl.pallas_call(
            layer_one_kernel,
            out_shape=[jax.ShapeDtypeStruct((rows, feat_in), BF16), jax.ShapeDtypeStruct((dev_count, halo_rows, feat_in), BF16)],
            in_specs=[ANY, SMEM, VMEM, VMEM, VMEM], out_specs=[VMEM, VMEM],
            scratch_shapes=[pltpu.VMEM((1, ext, feat_in), F32), pltpu.VMEM((rows, 8), F32), pltpu.VMEM((1, rows, feat_in), F32), edge_sem] + edge_ids,
            compiler_params=params(16), name="layer_one",
        )(src, send_idx, wt, feats, halo0.reshape(halo, feat_in))
        zh = exchange(out1, 1).reshape(halo, feat_in)
        g2, gw2t, loss_part = pl.pallas_call(
            layer_two_kernel,
            out_shape=[jax.ShapeDtypeStruct((rows, 2 * LANES), BF16), jax.ShapeDtypeStruct((pad_cls, hid), F32), jax.ShapeDtypeStruct((1, 256), F32)],
            in_specs=[ANY, SMEM, VMEM, VMEM, VMEM, VMEM, VMEM, VMEM, VMEM], out_specs=[VMEM, VMEM, VMEM],
            scratch_shapes=[pltpu.VMEM((2, ext, LANES), F32), pltpu.VMEM((rows, 8), F32), pltpu.VMEM((rows, hid), BF16),
                            pltpu.VMEM((pad_cls, hid), BF16), edge_sem] + edge_ids,
            compiler_params=params(24), name="layer_two",
        )(src, total, wt, z1, zh, w_one, w2t, labels.reshape(blocks, LANES), label_mask.reshape(blocks, LANES))
        own, halo_g = pl.pallas_call(
            functools.partial(scatter_kernel, in_deg),
            out_shape=[jax.ShapeDtypeStruct((2, rows, LANES), F32), jax.ShapeDtypeStruct((dev_count, PACKED, LANES), F32)],
            in_specs=[ANY, VMEM, VMEM], out_specs=[VMEM, VMEM],
            scratch_shapes=[edge_sem, pltpu.VMEM((rows, 8), F32)] + [pltpu.VMEM((2, ext, LANES), F32)] * in_deg + edge_ids,
            compiler_params=params(41), name="scatter",
        )(src, wt, g2)
        back = exchange(halo_g, 2)
        gw1 = pl.pallas_call(
            combine_kernel, out_shape=jax.ShapeDtypeStruct((feat_in, hid), F32),
            in_specs=[SMEM, VMEM, VMEM, VMEM, VMEM, VMEM], out_specs=VMEM,
            scratch_shapes=[pltpu.VMEM((2, rows + 16, LANES), F32)] * 4 + [pltpu.VMEM((2 * LANES, hid), BF16)],
            compiler_params=params(30), name="combine",
        )(send_idx, own, back, z1, w_one, w2t)
        chips = dev_count // 2
        gw1, gw2t, loss = pl.pallas_call(
            functools.partial(reduce_kernel, dev_count, classes),
            out_shape=[jax.ShapeDtypeStruct((feat_in, hid), F32), jax.ShapeDtypeStruct((classes, hid), F32), jax.ShapeDtypeStruct((1,), F32)],
            in_specs=[VMEM, VMEM, VMEM, SMEM], out_specs=[VMEM, VMEM, SMEM],
            scratch_shapes=[pltpu.VMEM((2, chips, 3, 8, LANES), F32), pltpu.VMEM((chips, 3, 8, LANES), F32), pltpu.VMEM((chips, 3, 8, LANES), F32),
                            pltpu.VMEM((chips, 3, 8, LANES), F32), pltpu.VMEM((2, chips, 3, 8, LANES), F32), pltpu.SemaphoreType.DMA((6, dev_count))],
            compiler_params=comm(8, 3), name="reduce",
        )(gw1, gw2t, loss_part, total)
        return loss[0], gw1, gw2t.T

    row_spec = P("graph", None)
    vec_spec = P("graph")
    return jax.shard_map(device_step, mesh=mesh, in_specs=(row_spec, P(), P(), row_spec, vec_spec, row_spec, row_spec, vec_spec, vec_spec), out_specs=(P(), P(), P()), check_vma=False)
```

```python
import functools

import jax
import jax.numpy as jnp
from jax import lax
from jax.experimental import pallas as pl
from jax.experimental.pallas import tpu as pltpu
from jax.sharding import PartitionSpec as P

LANES = 128
F32, BF16 = jnp.float32, jnp.bfloat16
VMEM = pl.BlockSpec(memory_space=pltpu.VMEM)
SMEM = pl.BlockSpec(memory_space=pltpu.SMEM)
ANY = pl.BlockSpec(memory_space=pl.ANY)
MESH = pl.DeviceIdType.MESH


def params(limit_mib):
    return pltpu.CompilerParams(vmem_limit_bytes=limit_mib * 2**20)


def row_masks():
    sub = lax.broadcasted_iota(jnp.int32, (8, LANES), 0)
    return [sub == r for r in range(8)]


def dot(a, b, dims):
    return lax.dot_general(a, b, (dims, ((), ())), preferred_element_type=F32)


SUMS = 6
RING = 4


def each_block(src_any, wt_ref, ring, wts, sem, fn):
    blocks = src_any.shape[0]
    deg = wt_ref.shape[0]

    def copy(j, b):
        return pltpu.make_async_copy(src_any.at[j], ring[b], sem.at[b])

    def turn(j, b):
        cols = wt_ref[:, pl.ds(pl.multiple_of(j * LANES, LANES), LANES)]
        wts[b] = jnp.concatenate([cols, jnp.zeros((8 - deg, LANES), F32)], 0).T

    def start():
        for b in range(RING):
            copy(b, b).start()
        turn(0, 0)

    def run():
        def body(i, _):
            for b in range(RING):
                j = i * RING + b
                copy(j, b).wait()
                turn(jnp.minimum(j + 1, blocks - 1), (b + 1) % RING)
                fn(j, ring[b], wts.at[b])

                @pl.when(j + RING < blocks)
                def _():
                    copy(j + RING, b).start()
            return 0
        lax.fori_loop(0, blocks // RING, body, 0)
    return start, run


def pick_rows(tbl, parts, ids, masks):
    outs = []
    for t in range(parts):
        v = None
        for r in range(8):
            row = jnp.broadcast_to(tbl[t, pl.ds(ids[r], 1), :], (8, LANES))
            v = row if v is None else jnp.where(masks[r], row, v)
        outs.append(v)
    return outs


def gather_sum(ids, w_ref, tbl, parts, masks, j, store):
    for c in range(LANES // 32):
        out = []
        at = pl.multiple_of(j * LANES, LANES) + 32 * c
        for h in range(4):
            w8 = w_ref[32 * c + 8 * h:32 * c + 8 * h + 8, :]
            acc = None
            for k in range(ids.shape[0]):
                wk = jnp.broadcast_to(w8[:, k:k + 1], (8, LANES))
                vs = pick_rows(tbl, parts, [ids[k, 32 * c + 8 * h + r] for r in range(8)], masks)
                vs = [v * wk for v in vs]
                acc = vs if acc is None else [a + v for a, v in zip(acc, vs)]
            out.append(jnp.concatenate(acc, 1))
        store(at, jnp.concatenate(out, 0))


def send_rows(list_ref, tbl, out_ref, masks):
    blocks, size = out_ref.shape[:2]

    def body(q, _):
        for g in range(size // 32):
            blk = list_ref.at[q, pl.ds(32 * g, 32)]
            parts = [pick_rows(tbl, 1, [blk[8 * h + r] for r in range(8)], masks)[0] for h in range(4)]
            out_ref[q, pl.ds(32 * g, 32), :] = jnp.concatenate(parts, 0).astype(BF16)
        return 0
    lax.fori_loop(0, blocks, body, 0)


def chunked(total, chunk, fn):
    def body(i, _):
        fn(pl.multiple_of(i * chunk, chunk))
        return 0
    lax.fori_loop(0, total // chunk, body, 0)


def enter(n, me):
    barrier = pltpu.get_barrier_semaphore()
    for i in range(1, n):
        pl.semaphore_signal(barrier, inc=1, device_id=((me + i) % n,), device_id_type=MESH)
    return lambda: pl.semaphore_wait(barrier, n - 1)


def all_to_all(n, me, src, dst, send_sem, recv_sem):
    plane = 8 if n % 8 == 0 else n
    steps = sorted(range(n // plane), key=lambda z: -min(z, n // plane - z))
    copies = []
    for dr in range(plane):
        for dz in steps:
            if dr or dz:
                copies.append((dz, dr))
    copies.sort(key=lambda c: -min(c[0], n // plane - c[0]))
    made = []
    for dz, dr in copies:
        peer = ((me // plane + dz) % (n // plane)) * plane + (me % plane + dr) % plane
        i = dz * plane + dr
        made.append(pltpu.make_async_remote_copy(
            src_ref=src.at[peer], dst_ref=dst.at[me], send_sem=send_sem.at[i], recv_sem=recv_sem.at[i],
            device_id=(peer,), device_id_type=MESH))
    for c in made:
        c.start()
    return made


def first_kernel(n, list_ref, own_ref, mask_ref, halo_ref, total_ref, tbl, out, cnt, cnts, sems):
    me = lax.axis_index("graph")
    ready = enter(n, me)
    rows = own_ref.shape[0]
    mine = jnp.sum(mask_ref[...].astype(F32), axis=0, keepdims=True)
    for p in range(n):
        cnt[p] = mine

    def load_own(o):
        tbl[0, pl.ds(o, 256), :] = own_ref[pl.ds(o, 256), :].astype(F32)
    chunked(rows, 256, load_own)
    send_rows(list_ref, tbl, out, row_masks())
    ready()
    small = all_to_all(n, me, cnt, cnts, sems.at[0], sems.at[1])
    big = all_to_all(n, me, out, halo_ref, sems.at[2], sems.at[3])
    halo_ref[pl.ds(me, 1)] = out[pl.ds(me, 1)]
    cnts[pl.ds(me, 1)] = cnt[pl.ds(me, 1)]
    for c in small:
        c.wait()
    total_ref[0] = jnp.sum(jnp.sum(cnts[...], axis=0))
    for c in big:
        c.wait()


def exchange_kernel(n, x_ref, o_ref, sems):
    me = lax.axis_index("graph")
    enter(n, me)()
    copies = all_to_all(n, me, x_ref, o_ref, sems.at[0], sems.at[1])
    o_ref[pl.ds(me, 1)] = x_ref[pl.ds(me, 1)]
    for c in copies:
        c.wait()


def reduce_kernel(n, classes, gw1_ref, gw2t_ref, loss_ref, total_ref, o1_ref, o2_ref, ol_ref, full, pair, acc, ring, half, sems):
    chips = n // 2
    me = lax.axis_index("graph")
    chip, core = me // 2, me % 2
    ready = enter(n, me)
    full[...] = jnp.zeros_like(full)

    def tiles(rows):
        return [(i, t) for i in range(rows // 8) for t in range(2)]
    where_ = {}
    at = 0
    for name, ref, rows in (("a", gw1_ref, gw1_ref.shape[0]), ("b", gw2t_ref, gw2t_ref.shape[0])):
        for i, t in tiles(rows):
            where_[name, i, t] = (at // (3 * chips), at // 3 % chips, at % 3)
            full[where_[name, i, t]] = ref[8 * i:8 * i + 8, t * LANES:(t + 1) * LANES]
            at += 1
    last = (at // (3 * chips), at // 3 % chips, at % 3)
    full[last[0], last[1], last[2], 0:1] = loss_ref[:, :LANES] + loss_ref[:, LANES:]
    ready()
    partner = me + 1 - 2 * core
    swap = pltpu.make_async_remote_copy(src_ref=full.at[1 - core], dst_ref=pair, send_sem=sems.at[0, 0], recv_sem=sems.at[1, 0],
                                        device_id=(partner,), device_id_type=MESH)
    swap.start()
    swap.wait()
    acc[...] = pair[...] + full[core]

    def others(src_of, dst, s):
        made = []
        for i in sorted(range(1, chips), key=lambda i: -min(i // 4, chips // 4 - i // 4)):
            other = (chip + i) % chips
            made.append(pltpu.make_async_remote_copy(
                src_ref=src_of(other), dst_ref=dst, send_sem=sems.at[s, i], recv_sem=sems.at[s + 1, i],
                device_id=(2 * other + core,), device_id_type=MESH))
        for c in made:
            c.start()
        return made
    first = others(lambda other: acc.at[other], ring.at[chip], 2)
    ring[pl.ds(chip, 1)] = acc[pl.ds(chip, 1)]
    for c in first:
        c.wait()
    half[pl.ds(core, 1), pl.ds(chip, 1)] = jnp.sum(ring[...], axis=0)[None, None]
    second = others(lambda other: half.at[core, chip], half.at[core, chip], 4)
    for c in second:
        c.wait()
    back = pltpu.make_async_remote_copy(src_ref=half.at[core], dst_ref=half.at[core], send_sem=sems.at[0, 1], recv_sem=sems.at[1, 1],
                                        device_id=(partner,), device_id_type=MESH)
    back.start()
    back.wait()
    for name, ref, rows in (("a", o1_ref, o1_ref.shape[0]), ("b", o2_ref, gw2t_ref.shape[0])):
        for i, t in tiles(rows):
            n_rows = min(8, ref.shape[0] - 8 * i)
            ref[8 * i:8 * i + n_rows, t * LANES:(t + 1) * LANES] = half[where_[name, i, t]][:n_rows]
    ol_ref[0] = -jnp.sum(half[last]) / total_ref[0]


def layer_one_kernel(src_any, list_ref, wt_ref, own_ref, halo_ref, z_ref, out_ref, tbl, wts, ztbl, sem, *ring):
    def block(j, ids, w_ref):
        def store(at, z):
            zb = z.astype(BF16)
            z_ref[pl.ds(at, 32), :] = zb
            ztbl[0, pl.ds(at, 32), :] = zb.astype(F32)
        gather_sum(ids, w_ref, tbl, 1, masks, j, store)
    start, run = each_block(src_any, wt_ref, ring, wts, sem, block)
    start()
    rows, halo = own_ref.shape[0], halo_ref.shape[0]
    masks = row_masks()

    def load_own(o):
        tbl[0, pl.ds(o, 256), :] = own_ref[pl.ds(o, 256), :].astype(F32)

    def load_halo(o):
        tbl[0, pl.ds(o + rows, 256), :] = halo_ref[pl.ds(o, 256), :].astype(F32)
    chunked(rows, 256, load_own)
    chunked(halo, 256, load_halo)
    run()
    send_rows(list_ref, ztbl, out_ref, masks)


def hidden(z, w1):
    return jnp.maximum(dot(z, w1, ((1,), (0,))), 0.0).astype(BF16)


def layer_two_kernel(src_any, total_ref, wt_ref, z_own_ref, z_halo_ref, w1_ref, w2t_ref, lab_ref, mask_ref,
                     g2_ref, gw2t_ref, loss_ref, tbl, wts, z2, w2s, lg, g2ts, sem, *ring):
    def block(j, ids, w_ref):
        def store(at, z):
            z2[pl.ds(at, 32), :] = z.astype(BF16)
        gather_sum(ids, w_ref, tbl, 2, masks, j, store)
    start, run = each_block(src_any, wt_ref, ring, wts, sem, block)
    start()
    classes = w2t_ref.shape[0]
    rows, halo = z_own_ref.shape[0], z_halo_ref.shape[0]
    masks = row_masks()
    w1 = w1_ref[...].astype(BF16)

    def load(ref, base):
        def fn(o):
            h = hidden(ref[pl.ds(o, 1024), :], w1).astype(F32)
            tbl[0, pl.ds(o + base, 1024), :] = h[:, :LANES]
            tbl[1, pl.ds(o + base, 1024), :] = h[:, LANES:]
        return fn
    chunked(rows, 1024, load(z_own_ref, 0))
    chunked(halo, 1024, load(z_halo_ref, rows))
    run()

    total = total_ref[0]
    w2s[...] = jnp.zeros_like(w2s)
    w2s[pl.ds(0, classes), :] = w2t_ref[...].astype(BF16)
    w2t = w2s[...]
    pad_cls = w2t.shape[0]
    loss_ref[...] = jnp.zeros_like(loss_ref)
    cls = lax.broadcasted_iota(jnp.int32, (pad_cls, 256), 0)

    def project(o):
        lg[:, pl.ds(o, 1024)] = dot(w2t, z2[pl.ds(o, 1024), :], ((1,), (1,)))
    chunked(rows, 1024, project)

    def chunk(i, _):
        o = pl.multiple_of(i * 256, 256)
        logits = lg[:, pl.ds(o, 256)]
        live = cls < classes
        lab = jnp.concatenate([lab_ref[pl.ds(2 * i + t, 1), :] for t in range(2)], 1)
        mf = jnp.concatenate([mask_ref[pl.ds(2 * i + t, 1), :] for t in range(2)], 1).astype(F32)
        top = jnp.max(jnp.where(live, logits, -jnp.inf), axis=0, keepdims=True)
        shifted = logits - top
        ex = jnp.where(live, jnp.exp(shifted), 0.0)
        norm = jnp.sum(ex, axis=0, keepdims=True)
        logp = shifted - jnp.log(norm)
        hot = cls == lab
        loss_ref[...] += mf * jnp.sum(jnp.where(hot, logp, 0.0), axis=0, keepdims=True)
        g2t = ((ex * (1.0 / norm) - hot.astype(F32)) * (mf / total)).astype(BF16)
        g2ts[:, pl.ds(o, 256)] = g2t
        g2 = jnp.concatenate([g2t.astype(F32), jnp.zeros((2 * LANES - pad_cls, 256), F32)], 0).T
        g2_ref[pl.ds(o, 256), :] = g2.astype(BF16)
        return 0
    lax.fori_loop(0, rows // 256, chunk, 0)
    gw2t_ref[...] = dot(g2ts[...], z2[...], ((1,), (0,)))


PACKED = 88


def in_span(at, rows, width):
    lane = lax.broadcasted_iota(jnp.int32, (rows, LANES), 1)
    return (lane >= at) & (lane < at + width)


def scatter_kernel(in_deg, src_any, wt_ref, g2_ref, own_ref, halo_ref, sem, wts, *more):
    bufs, ring = more[:SUMS], more[SUMS:]

    def block(j, ids, w_ref):
        for c in range(LANES // 32):
            at = pl.multiple_of(j * LANES, LANES) + 32 * c
            gg = g2_ref[pl.ds(at, 32), :].astype(F32)
            for h in range(4):
                w8 = w_ref[32 * c + 8 * h:32 * c + 8 * h + 8, :]
                gs = [gg[8 * h:8 * h + 8, t * LANES:(t + 1) * LANES] for t in range(2)]
                terms = []
                for k in range(in_deg):
                    wk = jnp.broadcast_to(w8[:, k:k + 1], (8, LANES))
                    terms.append([wk * x for x in gs])
                for r in range(8):
                    for k in range(in_deg):
                        i = ids[k, 32 * c + 8 * h + r]
                        for t in range(2):
                            row = jnp.broadcast_to(bufs[((h * 8 + r) * in_deg + k) % SUMS][t, pl.ds(i, 1), :], (8, LANES)) + terms[k][t]
                            bufs[((h * 8 + r) * in_deg + k) % SUMS][t, pl.ds(i, 1), :] = row[r:r + 1, :]
    start, run = each_block(src_any, wt_ref, ring, wts, sem, block)
    start()
    rows, nodes = own_ref.shape[1], halo_ref.shape[0]

    def zero(i, _):
        for b in bufs:
            for t in range(2):
                b[t, pl.ds(pl.multiple_of(i * 64, 64), 64), :] = jnp.zeros((64, LANES), F32)
        return 0
    lax.fori_loop(0, bufs[0].shape[1] // 64, zero, 0)
    run()

    def total(t, o, n):
        s = pl.ds(o, n)
        a = bufs[0][t, s, :]
        for b in bufs[1:]:
            a = a + b[t, s, :]
        return a

    def red_own(o):
        for t in range(2):
            own_ref[t, pl.ds(o, 64), :] = total(t, o, 64)
    chunked(rows, 64, red_own)

    def red_halo(q, _):
        o = pl.multiple_of(rows + q * 64, 64)
        halo_ref[q, pl.ds(0, 64), :] = total(0, o, 64)
        hi = total(1, o, 64)
        packed = hi[:16]
        for g in range(1, 4):
            packed = jnp.where(in_span(32 * g, 16, 32), pltpu.roll(hi[16 * g:16 * g + 16], 32 * g, 1), packed)
        halo_ref[q, pl.ds(64, 16), :] = packed
        packed = pltpu.roll(hi[:8], LANES - 32, 1)
        for g in range(1, 8):
            packed = jnp.where(in_span(16 * g, 8, 16), pltpu.roll(hi[8 * g:8 * g + 8], (16 * g - 32) % LANES, 1), packed)
        halo_ref[q, pl.ds(80, 8), :] = packed
        return 0
    lax.fori_loop(0, nodes, red_halo, 0)


def combine_kernel(list_ref, own_ref, back_ref, z_ref, w1_ref, w2t_ref, gw1_ref, w2p, g1s, *bufs):
    nb = len(bufs)
    rows = own_ref.shape[1]

    def init(o):
        for t in range(2):
            bufs[0][t, pl.ds(o, 256), :] = own_ref[t, pl.ds(o, 256), :]
            for b in bufs[1:]:
                b[t, pl.ds(o, 256), :] = jnp.zeros((256, LANES), F32)
    chunked(rows, 256, init)
    first, second = in_span(0, 8, 32), in_span(32, 8, 16)

    def body(q, _):
        last = back_ref[q, pl.ds(80, 8), :]
        for g in range(8):
            lo = back_ref[q, pl.ds(8 * g, 8), :]
            mid = back_ref[q, pl.ds(64 + 8 * (g % 2), 8), :]
            mid = mid if g < 2 else pltpu.roll(mid, LANES - 32 * (g // 2), 1)
            tail = pltpu.roll(last, (32 - 16 * g) % LANES, 1) if g != 2 else last
            hi = jnp.where(first, mid, jnp.where(second, tail, 0.0))
            for r in range(8):
                b = bufs[r % nb]
                i = list_ref[q, 8 * g + r]
                for t, x in ((0, lo), (1, hi)):
                    row = jnp.broadcast_to(b[t, pl.ds(i, 1), :], (8, LANES)) + x
                    b[t, pl.ds(i, 1), :] = row[r:r + 1, :]
        return 0
    lax.fori_loop(0, back_ref.shape[0], body, 0)

    w1 = w1_ref[...].astype(BF16)
    w2p[...] = jnp.zeros_like(w2p)
    w2p[pl.ds(0, w2t_ref.shape[0]), :] = w2t_ref[...].astype(BF16)

    def finish(o):
        n = 512
        z = z_ref[pl.ds(o, n), :]
        h = hidden(z, w1)
        halves = []
        for t in range(2):
            a = bufs[0][t, pl.ds(o, n), :]
            for b in bufs[1:]:
                a = a + b[t, pl.ds(o, n), :]
            halves.append(a)
        x = jnp.concatenate(halves, 1)
        x1 = x.astype(BF16)
        rest = x - x1.astype(F32)
        x2 = rest.astype(BF16)
        x3 = (rest - x2.astype(F32)).astype(BF16)
        w2 = w2p[...]
        dh = dot(x3, w2, ((1,), (0,))) + dot(x2, w2, ((1,), (0,))) + dot(x1, w2, ((1,), (0,)))
        g1s[pl.ds(o, n), :] = jnp.where(h.astype(F32) > 0, dh, 0.0).astype(BF16)
    chunked(rows, 512, finish)
    gw1_ref[...] = dot(z_ref[...], g1s[...], ((0,), (0,)))


def solution(mesh):
    dev_count = mesh.shape["graph"]

    def device_step(feats, w_one, w_two, send_idx, send_count, edge_src, edge_wt, labels, label_mask):
        rows, feat_in = feats.shape
        hid, classes = w_two.shape
        halo_rows = send_idx.shape[1]
        in_deg = edge_src.shape[1]
        halo = dev_count * halo_rows
        ext = rows + halo + 16
        blocks = rows // LANES
        pad_cls = -(-classes // 16) * 16
        src = edge_src.T.reshape(in_deg, blocks, LANES).transpose(1, 0, 2)
        wt, w2t = edge_wt.T, w_two.T
        edge_ids = [pltpu.SMEM((in_deg, LANES), jnp.int32)] * RING
        edge_w = pltpu.VMEM((RING, LANES, 8), F32)
        edge_sem = pltpu.SemaphoreType.DMA((RING,))

        def comm(limit_mib, cid):
            return pltpu.CompilerParams(vmem_limit_bytes=limit_mib * 2**20,
                                        collective_id=cid, has_side_effects=True)

        def exchange(x, cid):
            return pl.pallas_call(
                functools.partial(exchange_kernel, dev_count), out_shape=jax.ShapeDtypeStruct(x.shape, x.dtype),
                in_specs=[VMEM], out_specs=VMEM, scratch_shapes=[pltpu.SemaphoreType.DMA((2, dev_count))],
                compiler_params=comm(8, cid), name="exchange",
            )(x)

        halo0, total = pl.pallas_call(
            functools.partial(first_kernel, dev_count),
            out_shape=[jax.ShapeDtypeStruct((dev_count, halo_rows, feat_in), BF16), jax.ShapeDtypeStruct((1,), F32)],
            in_specs=[SMEM, VMEM, VMEM], out_specs=[VMEM, SMEM],
            scratch_shapes=[pltpu.VMEM((1, rows, feat_in), F32), pltpu.VMEM((dev_count, halo_rows, feat_in), BF16),
                            pltpu.VMEM((dev_count, 1, LANES), F32), pltpu.VMEM((dev_count, 1, LANES), F32),
                            pltpu.SemaphoreType.DMA((4, dev_count))],
            compiler_params=comm(16, 0), name="first",
        )(send_idx, feats, label_mask.reshape(blocks, LANES))
        z1, out1 = pl.pallas_call(
            layer_one_kernel,
            out_shape=[jax.ShapeDtypeStruct((rows, feat_in), BF16), jax.ShapeDtypeStruct((dev_count, halo_rows, feat_in), BF16)],
            in_specs=[ANY, SMEM, VMEM, VMEM, VMEM], out_specs=[VMEM, VMEM],
            scratch_shapes=[pltpu.VMEM((1, ext, feat_in), F32), edge_w, pltpu.VMEM((1, rows, feat_in), F32), edge_sem] + edge_ids,
            compiler_params=params(16), name="layer_one",
        )(src, send_idx, wt, feats, halo0.reshape(halo, feat_in))
        zh = exchange(out1, 1).reshape(halo, feat_in)
        g2, gw2t, loss_part = pl.pallas_call(
            layer_two_kernel,
            out_shape=[jax.ShapeDtypeStruct((rows, 2 * LANES), BF16), jax.ShapeDtypeStruct((pad_cls, hid), F32), jax.ShapeDtypeStruct((1, 256), F32)],
            in_specs=[ANY, SMEM, VMEM, VMEM, VMEM, VMEM, VMEM, VMEM, VMEM], out_specs=[VMEM, VMEM, VMEM],
            scratch_shapes=[pltpu.VMEM((2, ext, LANES), F32), edge_w, pltpu.VMEM((rows, hid), BF16),
                            pltpu.VMEM((pad_cls, hid), BF16), pltpu.VMEM((pad_cls, rows), F32), pltpu.VMEM((pad_cls, rows), BF16), edge_sem] + edge_ids,
            compiler_params=params(28), name="layer_two",
        )(src, total, wt, z1, zh, w_one, w2t, labels.reshape(blocks, LANES), label_mask.reshape(blocks, LANES))
        own, halo_g = pl.pallas_call(
            functools.partial(scatter_kernel, in_deg),
            out_shape=[jax.ShapeDtypeStruct((2, rows, LANES), F32), jax.ShapeDtypeStruct((dev_count, PACKED, LANES), F32)],
            in_specs=[ANY, VMEM, VMEM], out_specs=[VMEM, VMEM],
            scratch_shapes=[edge_sem, edge_w] + [pltpu.VMEM((2, ext, LANES), F32)] * SUMS + edge_ids,
            compiler_params=params(39), name="scatter",
        )(src, wt, g2)
        back = exchange(halo_g, 2)
        gw1 = pl.pallas_call(
            combine_kernel, out_shape=jax.ShapeDtypeStruct((feat_in, hid), F32),
            in_specs=[SMEM, VMEM, VMEM, VMEM, VMEM, VMEM], out_specs=VMEM,
            scratch_shapes=[pltpu.VMEM((2 * LANES, hid), BF16), pltpu.VMEM((rows, hid), BF16)] + [pltpu.VMEM((2, rows + 16, LANES), F32)] * 4,
            compiler_params=params(32), name="combine",
        )(send_idx, own, back, z1, w_one, w2t)
        chips = dev_count // 2
        gw1, gw2t, loss = pl.pallas_call(
            functools.partial(reduce_kernel, dev_count, classes),
            out_shape=[jax.ShapeDtypeStruct((feat_in, hid), F32), jax.ShapeDtypeStruct((classes, hid), F32), jax.ShapeDtypeStruct((1,), F32)],
            in_specs=[VMEM, VMEM, VMEM, SMEM], out_specs=[VMEM, VMEM, SMEM],
            scratch_shapes=[pltpu.VMEM((2, chips, 3, 8, LANES), F32), pltpu.VMEM((chips, 3, 8, LANES), F32), pltpu.VMEM((chips, 3, 8, LANES), F32),
                            pltpu.VMEM((chips, 3, 8, LANES), F32), pltpu.VMEM((2, chips, 3, 8, LANES), F32), pltpu.SemaphoreType.DMA((6, dev_count))],
            compiler_params=comm(8, 3), name="reduce",
        )(gw1, gw2t, loss_part, total)
        return loss[0], gw1, gw2t.T

    row_spec = P("graph", None)
    vec_spec = P("graph")
    return jax.shard_map(device_step, mesh=mesh, in_specs=(row_spec, P(), P(), row_spec, vec_spec, row_spec, row_spec, vec_spec, vec_spec), out_specs=(P(), P(), P()), check_vma=False)
```

```python
import functools

import jax
import jax.numpy as jnp
from jax import lax
from jax.experimental import pallas as pl
from jax.experimental.pallas import tpu as pltpu
from jax.sharding import PartitionSpec as P

LANES = 128
F32, BF16 = jnp.float32, jnp.bfloat16
VMEM = pl.BlockSpec(memory_space=pltpu.VMEM)
SMEM = pl.BlockSpec(memory_space=pltpu.SMEM)
ANY = pl.BlockSpec(memory_space=pl.ANY)
MESH = pl.DeviceIdType.MESH


def params(limit_mib):
    return pltpu.CompilerParams(vmem_limit_bytes=limit_mib * 2**20)


def row_masks():
    sub = lax.broadcasted_iota(jnp.int32, (8, LANES), 0)
    return [sub == r for r in range(8)]


def dot(a, b, dims):
    return lax.dot_general(a, b, (dims, ((), ())), preferred_element_type=F32)


SUMS = 6
RING = 4


def each_block(src_any, wt_ref, ring, wts, sem, fn):
    blocks = src_any.shape[0]
    deg = wt_ref.shape[0]

    def copy(j, b):
        return pltpu.make_async_copy(src_any.at[j], ring[b], sem.at[b])

    def turn(j, b):
        cols = wt_ref[:, pl.ds(pl.multiple_of(j * LANES, LANES), LANES)]
        wts[b] = jnp.concatenate([cols, jnp.zeros((8 - deg, LANES), F32)], 0).T

    def start():
        for b in range(RING):
            copy(b, b).start()
        turn(0, 0)

    def run():
        def body(i, _):
            for b in range(RING):
                j = i * RING + b
                copy(j, b).wait()
                turn(jnp.minimum(j + 1, blocks - 1), (b + 1) % RING)
                fn(j, ring[b], wts.at[b])

                @pl.when(j + RING < blocks)
                def _():
                    copy(j + RING, b).start()
            return 0
        lax.fori_loop(0, blocks // RING, body, 0)
    return start, run


def pick_rows(tbl, parts, ids, masks):
    outs = []
    for t in range(parts):
        v = None
        for r in range(8):
            row = jnp.broadcast_to(tbl[t, pl.ds(ids[r], 1), :], (8, LANES))
            v = row if v is None else jnp.where(masks[r], row, v)
        outs.append(v)
    return outs


def gather_sum(ids, w_ref, tbl, parts, masks, j, store):
    for c in range(LANES // 32):
        out = []
        at = pl.multiple_of(j * LANES, LANES) + 32 * c
        for h in range(4):
            w8 = w_ref[32 * c + 8 * h:32 * c + 8 * h + 8, :]
            acc = None
            for k in range(ids.shape[0]):
                wk = jnp.broadcast_to(w8[:, k:k + 1], (8, LANES))
                vs = pick_rows(tbl, parts, [ids[k, 32 * c + 8 * h + r] for r in range(8)], masks)
                vs = [v * wk for v in vs]
                acc = vs if acc is None else [a + v for a, v in zip(acc, vs)]
            out.append(jnp.concatenate(acc, 1))
        store(at, jnp.concatenate(out, 0))


def send_rows(list_ref, tbl, out_ref, masks):
    blocks, size = out_ref.shape[:2]

    def body(q, _):
        for g in range(size // 32):
            blk = list_ref.at[q, pl.ds(32 * g, 32)]
            parts = [pick_rows(tbl, 1, [blk[8 * h + r] for r in range(8)], masks)[0] for h in range(4)]
            out_ref[q, pl.ds(32 * g, 32), :] = jnp.concatenate(parts, 0).astype(BF16)
        return 0
    lax.fori_loop(0, blocks, body, 0)


def chunked(total, chunk, fn):
    def body(i, _):
        fn(pl.multiple_of(i * chunk, chunk))
        return 0
    lax.fori_loop(0, total // chunk, body, 0)


def enter(n, me):
    barrier = pltpu.get_barrier_semaphore()
    for i in range(1, n):
        pl.semaphore_signal(barrier, inc=1, device_id=((me + i) % n,), device_id_type=MESH)
    return lambda: pl.semaphore_wait(barrier, n - 1)


def far_first(me, n, plane):
    z, r = me // plane, me % plane
    if n // plane == 4:
        up = z // 2
        zs = [3 - 3 * up, 2 - up, z + 1 - 2 * (z % 2)]
    else:
        zs = [(z + i) % (n // plane) for i in range(1, n // plane)]
    peers = [to * plane + (r + i) % plane for to in zs for i in range(plane)]
    return peers + [z * plane + (r + i) % plane for i in range(1, plane)]


def send_all(peers, me, src_of, dst, send_sem, recv_sem, device_of=lambda p: p):
    made = []
    for i, p in enumerate(peers):
        made.append(pltpu.make_async_remote_copy(
            src_ref=src_of(p), dst_ref=dst, send_sem=send_sem.at[i], recv_sem=recv_sem.at[me],
            device_id=(device_of(p),), device_id_type=MESH))
    for c in made:
        c.start()

    def wait(dst_of):
        for p in peers:
            pltpu.make_async_remote_copy(
                src_ref=dst_of(p), dst_ref=dst_of(p), send_sem=send_sem.at[0], recv_sem=recv_sem.at[p],
                device_id=(device_of(p),), device_id_type=MESH).wait_recv()
        for c in made:
            c.wait_send()
    return wait


def all_to_all(n, me, src, dst, send_sem, recv_sem):
    wait = send_all(far_first(me, n, 8), me, lambda p: src.at[p], dst.at[me], send_sem, recv_sem)
    return lambda: wait(lambda p: dst.at[p])


def first_kernel(n, list_ref, own_ref, mask_ref, halo_ref, total_ref, tbl, out, cnt, cnts, sems):
    me = lax.axis_index("graph")
    ready = enter(n, me)
    rows = own_ref.shape[0]
    mine = jnp.sum(mask_ref[...].astype(F32), axis=0, keepdims=True)
    for p in range(n):
        cnt[p] = mine

    def load_own(o):
        tbl[0, pl.ds(o, 256), :] = own_ref[pl.ds(o, 256), :].astype(F32)
    chunked(rows, 256, load_own)
    send_rows(list_ref, tbl, out, row_masks())
    ready()
    big = all_to_all(n, me, out, halo_ref, sems.at[2], sems.at[3])
    small = all_to_all(n, me, cnt, cnts, sems.at[0], sems.at[1])
    halo_ref[pl.ds(me, 1)] = out[pl.ds(me, 1)]
    cnts[pl.ds(me, 1)] = cnt[pl.ds(me, 1)]
    small()
    total_ref[0] = jnp.sum(jnp.sum(cnts[...], axis=0))
    big()


def exchange_kernel(n, x_ref, o_ref, sems):
    me = lax.axis_index("graph")
    enter(n, me)()
    arrived = all_to_all(n, me, x_ref, o_ref, sems.at[0], sems.at[1])
    o_ref[pl.ds(me, 1)] = x_ref[pl.ds(me, 1)]
    arrived()


def reduce_kernel(n, classes, gw1_ref, gw2t_ref, loss_ref, total_ref, o1_ref, o2_ref, ol_ref, full, pair, acc, ring, half, sems):
    chips = n // 2
    me = lax.axis_index("graph")
    chip, core = me // 2, me % 2
    ready = enter(n, me)
    full[...] = jnp.zeros_like(full)

    def tiles(rows):
        return [(i, t) for i in range(rows // 8) for t in range(2)]
    where_ = {}
    at = 0
    for name, ref, rows in (("a", gw1_ref, gw1_ref.shape[0]), ("b", gw2t_ref, gw2t_ref.shape[0])):
        for i, t in tiles(rows):
            where_[name, i, t] = (at // (3 * chips), at // 3 % chips, at % 3)
            full[where_[name, i, t]] = ref[8 * i:8 * i + 8, t * LANES:(t + 1) * LANES]
            at += 1
    last = (at // (3 * chips), at // 3 % chips, at % 3)
    full[last[0], last[1], last[2], 0:1] = loss_ref[:, :LANES] + loss_ref[:, LANES:]
    ready()
    partner = me + 1 - 2 * core
    swap = pltpu.make_async_remote_copy(src_ref=full.at[1 - core], dst_ref=pair, send_sem=sems.at[0, 0], recv_sem=sems.at[1, 0],
                                        device_id=(partner,), device_id_type=MESH)
    swap.start()
    swap.wait()
    acc[...] = pair[...] + full[core]

    peers = far_first(chip, chips, 4)

    def others(src_of, dst, s):
        return send_all(peers, chip, src_of, dst, sems.at[s], sems.at[s + 1], lambda p: 2 * p + core)
    first = others(lambda other: acc.at[other], ring.at[chip], 2)
    ring[pl.ds(chip, 1)] = acc[pl.ds(chip, 1)]
    first(lambda other: ring.at[other])
    half[pl.ds(core, 1), pl.ds(chip, 1)] = jnp.sum(ring[...], axis=0)[None, None]
    second = others(lambda other: half.at[core, chip], half.at[core, chip], 4)
    second(lambda other: half.at[core, other])
    back = pltpu.make_async_remote_copy(src_ref=half.at[core], dst_ref=half.at[core], send_sem=sems.at[0, 1], recv_sem=sems.at[1, 1],
                                        device_id=(partner,), device_id_type=MESH)
    back.start()
    back.wait()
    for name, ref, rows in (("a", o1_ref, o1_ref.shape[0]), ("b", o2_ref, gw2t_ref.shape[0])):
        for i, t in tiles(rows):
            n_rows = min(8, ref.shape[0] - 8 * i)
            ref[8 * i:8 * i + n_rows, t * LANES:(t + 1) * LANES] = half[where_[name, i, t]][:n_rows]
    ol_ref[0] = -jnp.sum(half[last]) / total_ref[0]


def layer_one_kernel(src_any, list_ref, wt_ref, own_ref, halo_ref, z_ref, out_ref, tbl, wts, ztbl, sem, *ring):
    def block(j, ids, w_ref):
        def store(at, z):
            zb = z.astype(BF16)
            z_ref[pl.ds(at, 32), :] = zb
            ztbl[0, pl.ds(at, 32), :] = zb.astype(F32)
        gather_sum(ids, w_ref, tbl, 1, masks, j, store)
    start, run = each_block(src_any, wt_ref, ring, wts, sem, block)
    start()
    rows, halo = own_ref.shape[0], halo_ref.shape[0]
    masks = row_masks()

    def load_own(o):
        tbl[0, pl.ds(o, 256), :] = own_ref[pl.ds(o, 256), :].astype(F32)

    def load_halo(o):
        tbl[0, pl.ds(o + rows, 256), :] = halo_ref[pl.ds(o, 256), :].astype(F32)
    chunked(rows, 256, load_own)
    chunked(halo, 256, load_halo)
    run()
    send_rows(list_ref, ztbl, out_ref, masks)


def hidden(z, w1):
    return jnp.maximum(dot(z, w1, ((1,), (0,))), 0.0).astype(BF16)


def layer_two_kernel(src_any, total_ref, wt_ref, z_own_ref, z_halo_ref, w1_ref, w2t_ref, lab_ref, mask_ref,
                     g2_ref, gw2t_ref, loss_ref, tbl, wts, z2, w2s, lg, g2ts, sem, *ring):
    def block(j, ids, w_ref):
        def store(at, z):
            z2[pl.ds(at, 32), :] = z.astype(BF16)
        gather_sum(ids, w_ref, tbl, 2, masks, j, store)
    start, run = each_block(src_any, wt_ref, ring, wts, sem, block)
    start()
    classes = w2t_ref.shape[0]
    rows, halo = z_own_ref.shape[0], z_halo_ref.shape[0]
    masks = row_masks()
    w1 = w1_ref[...].astype(BF16)

    def load(ref, base):
        def fn(o):
            h = hidden(ref[pl.ds(o, 1024), :], w1).astype(F32)
            tbl[0, pl.ds(o + base, 1024), :] = h[:, :LANES]
            tbl[1, pl.ds(o + base, 1024), :] = h[:, LANES:]
        return fn
    chunked(rows, 1024, load(z_own_ref, 0))
    chunked(halo, 1024, load(z_halo_ref, rows))
    run()

    total = total_ref[0]
    w2s[...] = jnp.zeros_like(w2s)
    w2s[pl.ds(0, classes), :] = w2t_ref[...].astype(BF16)
    w2t = w2s[...]
    pad_cls = w2t.shape[0]
    loss_ref[...] = jnp.zeros_like(loss_ref)
    cls = lax.broadcasted_iota(jnp.int32, (pad_cls, 256), 0)

    def project(o):
        lg[:, pl.ds(o, 1024)] = dot(w2t, z2[pl.ds(o, 1024), :], ((1,), (1,)))
    chunked(rows, 1024, project)

    def chunk(i, _):
        o = pl.multiple_of(i * 256, 256)
        logits = lg[:, pl.ds(o, 256)]
        live = cls < classes
        lab = jnp.concatenate([lab_ref[pl.ds(2 * i + t, 1), :] for t in range(2)], 1)
        mf = jnp.concatenate([mask_ref[pl.ds(2 * i + t, 1), :] for t in range(2)], 1).astype(F32)
        top = jnp.max(jnp.where(live, logits, -jnp.inf), axis=0, keepdims=True)
        shifted = logits - top
        ex = jnp.where(live, jnp.exp(shifted), 0.0)
        norm = jnp.sum(ex, axis=0, keepdims=True)
        logp = shifted - jnp.log(norm)
        hot = cls == lab
        loss_ref[...] += mf * jnp.sum(jnp.where(hot, logp, 0.0), axis=0, keepdims=True)
        g2t = ((ex * (1.0 / norm) - hot.astype(F32)) * (mf / total)).astype(BF16)
        g2ts[:, pl.ds(o, 256)] = g2t
        g2 = jnp.concatenate([g2t.astype(F32), jnp.zeros((2 * LANES - pad_cls, 256), F32)], 0).T
        g2_ref[pl.ds(o, 256), :] = g2.astype(BF16)
        return 0
    lax.fori_loop(0, rows // 256, chunk, 0)
    gw2t_ref[...] = dot(g2ts[...], z2[...], ((1,), (0,)))


PACKED = 88


def in_span(at, rows, width):
    lane = lax.broadcasted_iota(jnp.int32, (rows, LANES), 1)
    return (lane >= at) & (lane < at + width)


def scatter_kernel(in_deg, src_any, wt_ref, g2_ref, own_ref, halo_ref, sem, wts, *more):
    bufs, ring = more[:SUMS], more[SUMS:]

    def block(j, ids, w_ref):
        for c in range(LANES // 32):
            at = pl.multiple_of(j * LANES, LANES) + 32 * c
            gg = g2_ref[pl.ds(at, 32), :].astype(F32)
            for h in range(4):
                w8 = w_ref[32 * c + 8 * h:32 * c + 8 * h + 8, :]
                gs = [gg[8 * h:8 * h + 8, t * LANES:(t + 1) * LANES] for t in range(2)]
                terms = []
                for k in range(in_deg):
                    wk = jnp.broadcast_to(w8[:, k:k + 1], (8, LANES))
                    terms.append([wk * x for x in gs])
                for r in range(8):
                    for k in range(in_deg):
                        i = ids[k, 32 * c + 8 * h + r]
                        for t in range(2):
                            row = jnp.broadcast_to(bufs[((h * 8 + r) * in_deg + k) % SUMS][t, pl.ds(i, 1), :], (8, LANES)) + terms[k][t]
                            bufs[((h * 8 + r) * in_deg + k) % SUMS][t, pl.ds(i, 1), :] = row[r:r + 1, :]
    start, run = each_block(src_any, wt_ref, ring, wts, sem, block)
    start()
    rows, nodes = own_ref.shape[1], halo_ref.shape[0]

    def zero(i, _):
        for b in bufs:
            for t in range(2):
                b[t, pl.ds(pl.multiple_of(i * 64, 64), 64), :] = jnp.zeros((64, LANES), F32)
        return 0
    lax.fori_loop(0, bufs[0].shape[1] // 64, zero, 0)
    run()

    def total(t, o, n):
        s = pl.ds(o, n)
        a = bufs[0][t, s, :]
        for b in bufs[1:]:
            a = a + b[t, s, :]
        return a

    def red_own(o):
        for t in range(2):
            own_ref[t, pl.ds(o, 64), :] = total(t, o, 64)
    chunked(rows, 64, red_own)

    def red_halo(q, _):
        o = pl.multiple_of(rows + q * 64, 64)
        halo_ref[q, pl.ds(0, 64), :] = total(0, o, 64)
        hi = total(1, o, 64)
        packed = hi[:16]
        for g in range(1, 4):
            packed = jnp.where(in_span(32 * g, 16, 32), pltpu.roll(hi[16 * g:16 * g + 16], 32 * g, 1), packed)
        halo_ref[q, pl.ds(64, 16), :] = packed
        packed = pltpu.roll(hi[:8], LANES - 32, 1)
        for g in range(1, 8):
            packed = jnp.where(in_span(16 * g, 8, 16), pltpu.roll(hi[8 * g:8 * g + 8], (16 * g - 32) % LANES, 1), packed)
        halo_ref[q, pl.ds(80, 8), :] = packed
        return 0
    lax.fori_loop(0, nodes, red_halo, 0)


def combine_kernel(list_ref, own_ref, back_ref, z_ref, w1_ref, w2t_ref, gw1_ref, w2p, g1s, *bufs):
    nb = len(bufs)
    rows = own_ref.shape[1]

    def init(o):
        for t in range(2):
            bufs[0][t, pl.ds(o, 256), :] = own_ref[t, pl.ds(o, 256), :]
            for b in bufs[1:]:
                b[t, pl.ds(o, 256), :] = jnp.zeros((256, LANES), F32)
    chunked(rows, 256, init)
    first, second = in_span(0, 8, 32), in_span(32, 8, 16)

    def body(q, _):
        last = back_ref[q, pl.ds(80, 8), :]
        for g in range(8):
            lo = back_ref[q, pl.ds(8 * g, 8), :]
            mid = back_ref[q, pl.ds(64 + 8 * (g % 2), 8), :]
            mid = mid if g < 2 else pltpu.roll(mid, LANES - 32 * (g // 2), 1)
            tail = pltpu.roll(last, (32 - 16 * g) % LANES, 1) if g != 2 else last
            hi = jnp.where(first, mid, jnp.where(second, tail, 0.0))
            for r in range(8):
                b = bufs[r % nb]
                i = list_ref[q, 8 * g + r]
                for t, x in ((0, lo), (1, hi)):
                    row = jnp.broadcast_to(b[t, pl.ds(i, 1), :], (8, LANES)) + x
                    b[t, pl.ds(i, 1), :] = row[r:r + 1, :]
        return 0
    lax.fori_loop(0, back_ref.shape[0], body, 0)

    w1 = w1_ref[...].astype(BF16)
    w2p[...] = jnp.zeros_like(w2p)
    w2p[pl.ds(0, w2t_ref.shape[0]), :] = w2t_ref[...].astype(BF16)

    def finish(o):
        n = 512
        z = z_ref[pl.ds(o, n), :]
        h = hidden(z, w1)
        halves = []
        for t in range(2):
            a = bufs[0][t, pl.ds(o, n), :]
            for b in bufs[1:]:
                a = a + b[t, pl.ds(o, n), :]
            halves.append(a)
        x = jnp.concatenate(halves, 1)
        x1 = x.astype(BF16)
        rest = x - x1.astype(F32)
        x2 = rest.astype(BF16)
        x3 = (rest - x2.astype(F32)).astype(BF16)
        w2 = w2p[...]
        dh = dot(x3, w2, ((1,), (0,))) + dot(x2, w2, ((1,), (0,))) + dot(x1, w2, ((1,), (0,)))
        g1s[pl.ds(o, n), :] = jnp.where(h.astype(F32) > 0, dh, 0.0).astype(BF16)
    chunked(rows, 512, finish)
    gw1_ref[...] = dot(z_ref[...], g1s[...], ((0,), (0,)))


def solution(mesh):
    dev_count = mesh.shape["graph"]

    def device_step(feats, w_one, w_two, send_idx, send_count, edge_src, edge_wt, labels, label_mask):
        rows, feat_in = feats.shape
        hid, classes = w_two.shape
        halo_rows = send_idx.shape[1]
        in_deg = edge_src.shape[1]
        halo = dev_count * halo_rows
        ext = rows + halo + 16
        blocks = rows // LANES
        pad_cls = -(-classes // 16) * 16
        src = edge_src.T.reshape(in_deg, blocks, LANES).transpose(1, 0, 2)
        wt, w2t = edge_wt.T, w_two.T
        edge_ids = [pltpu.SMEM((in_deg, LANES), jnp.int32)] * RING
        edge_w = pltpu.VMEM((RING, LANES, 8), F32)
        edge_sem = pltpu.SemaphoreType.DMA((RING,))

        def comm(limit_mib, cid):
            return pltpu.CompilerParams(vmem_limit_bytes=limit_mib * 2**20,
                                        collective_id=cid, has_side_effects=True)

        def exchange(x, cid):
            return pl.pallas_call(
                functools.partial(exchange_kernel, dev_count), out_shape=jax.ShapeDtypeStruct(x.shape, x.dtype),
                in_specs=[VMEM], out_specs=VMEM, scratch_shapes=[pltpu.SemaphoreType.DMA((2, dev_count))],
                compiler_params=comm(8, cid), name="exchange",
            )(x)

        halo0, total = pl.pallas_call(
            functools.partial(first_kernel, dev_count),
            out_shape=[jax.ShapeDtypeStruct((dev_count, halo_rows, feat_in), BF16), jax.ShapeDtypeStruct((1,), F32)],
            in_specs=[SMEM, VMEM, VMEM], out_specs=[VMEM, SMEM],
            scratch_shapes=[pltpu.VMEM((1, rows, feat_in), F32), pltpu.VMEM((dev_count, halo_rows, feat_in), BF16),
                            pltpu.VMEM((dev_count, 1, LANES), F32), pltpu.VMEM((dev_count, 1, LANES), F32),
                            pltpu.SemaphoreType.DMA((4, dev_count))],
            compiler_params=comm(16, 0), name="first",
        )(send_idx, feats, label_mask.reshape(blocks, LANES))
        z1, out1 = pl.pallas_call(
            layer_one_kernel,
            out_shape=[jax.ShapeDtypeStruct((rows, feat_in), BF16), jax.ShapeDtypeStruct((dev_count, halo_rows, feat_in), BF16)],
            in_specs=[ANY, SMEM, VMEM, VMEM, VMEM], out_specs=[VMEM, VMEM],
            scratch_shapes=[pltpu.VMEM((1, ext, feat_in), F32), edge_w, pltpu.VMEM((1, rows, feat_in), F32), edge_sem] + edge_ids,
            compiler_params=params(16), name="layer_one",
        )(src, send_idx, wt, feats, halo0.reshape(halo, feat_in))
        zh = exchange(out1, 1).reshape(halo, feat_in)
        g2, gw2t, loss_part = pl.pallas_call(
            layer_two_kernel,
            out_shape=[jax.ShapeDtypeStruct((rows, 2 * LANES), BF16), jax.ShapeDtypeStruct((pad_cls, hid), F32), jax.ShapeDtypeStruct((1, 256), F32)],
            in_specs=[ANY, SMEM, VMEM, VMEM, VMEM, VMEM, VMEM, VMEM, VMEM], out_specs=[VMEM, VMEM, VMEM],
            scratch_shapes=[pltpu.VMEM((2, ext, LANES), F32), edge_w, pltpu.VMEM((rows, hid), BF16),
                            pltpu.VMEM((pad_cls, hid), BF16), pltpu.VMEM((pad_cls, rows), F32), pltpu.VMEM((pad_cls, rows), BF16), edge_sem] + edge_ids,
            compiler_params=params(28), name="layer_two",
        )(src, total, wt, z1, zh, w_one, w2t, labels.reshape(blocks, LANES), label_mask.reshape(blocks, LANES))
        own, halo_g = pl.pallas_call(
            functools.partial(scatter_kernel, in_deg),
            out_shape=[jax.ShapeDtypeStruct((2, rows, LANES), F32), jax.ShapeDtypeStruct((dev_count, PACKED, LANES), F32)],
            in_specs=[ANY, VMEM, VMEM], out_specs=[VMEM, VMEM],
            scratch_shapes=[edge_sem, edge_w] + [pltpu.VMEM((2, ext, LANES), F32)] * SUMS + edge_ids,
            compiler_params=params(39), name="scatter",
        )(src, wt, g2)
        back = exchange(halo_g, 2)
        gw1 = pl.pallas_call(
            combine_kernel, out_shape=jax.ShapeDtypeStruct((feat_in, hid), F32),
            in_specs=[SMEM, VMEM, VMEM, VMEM, VMEM, VMEM], out_specs=VMEM,
            scratch_shapes=[pltpu.VMEM((2 * LANES, hid), BF16), pltpu.VMEM((rows, hid), BF16)] + [pltpu.VMEM((2, rows + 16, LANES), F32)] * 4,
            compiler_params=params(32), name="combine",
        )(send_idx, own, back, z1, w_one, w2t)
        chips = dev_count // 2
        gw1, gw2t, loss = pl.pallas_call(
            functools.partial(reduce_kernel, dev_count, classes),
            out_shape=[jax.ShapeDtypeStruct((feat_in, hid), F32), jax.ShapeDtypeStruct((classes, hid), F32), jax.ShapeDtypeStruct((1,), F32)],
            in_specs=[VMEM, VMEM, VMEM, SMEM], out_specs=[VMEM, VMEM, SMEM],
            scratch_shapes=[pltpu.VMEM((2, chips, 3, 8, LANES), F32), pltpu.VMEM((chips, 3, 8, LANES), F32), pltpu.VMEM((chips, 3, 8, LANES), F32),
                            pltpu.VMEM((chips, 3, 8, LANES), F32), pltpu.VMEM((2, chips, 3, 8, LANES), F32), pltpu.SemaphoreType.DMA((6, dev_count))],
            compiler_params=comm(8, 3), name="reduce",
        )(gw1, gw2t, loss_part, total)
        return loss[0], gw1, gw2t.T

    row_spec = P("graph", None)
    vec_spec = P("graph")
    return jax.shard_map(device_step, mesh=mesh, in_specs=(row_spec, P(), P(), row_spec, vec_spec, row_spec, row_spec, vec_spec, vec_spec), out_specs=(P(), P(), P()), check_vma=False)
```

```python
import functools

import jax
import jax.numpy as jnp
from jax import lax
from jax.experimental import pallas as pl
from jax.experimental.pallas import tpu as pltpu
from jax.sharding import PartitionSpec as P

LANES = 128
F32, BF16 = jnp.float32, jnp.bfloat16
VMEM = pl.BlockSpec(memory_space=pltpu.VMEM)
SMEM = pl.BlockSpec(memory_space=pltpu.SMEM)
ANY = pl.BlockSpec(memory_space=pl.ANY)
MESH = pl.DeviceIdType.MESH


def params(limit_mib):
    return pltpu.CompilerParams(vmem_limit_bytes=limit_mib * 2**20)


def row_masks():
    sub = lax.broadcasted_iota(jnp.int32, (8, LANES), 0)
    return [sub == r for r in range(8)]


def dot(a, b, dims):
    return lax.dot_general(a, b, (dims, ((), ())), preferred_element_type=F32)


SUMS = 6
WORK = 4_000_000
RING = 4


def each_block(src_any, wt_ref, ring, wts, sem, fn):
    blocks = src_any.shape[0]
    deg = wt_ref.shape[0]

    def copy(j, b):
        return pltpu.make_async_copy(src_any.at[j], ring[b], sem.at[b])

    def turn(j, b):
        cols = wt_ref[:, pl.ds(pl.multiple_of(j * LANES, LANES), LANES)]
        wts[b] = jnp.concatenate([cols, jnp.zeros((8 - deg, LANES), F32)], 0).T

    def start():
        for b in range(RING):
            copy(b, b).start()
        turn(0, 0)

    def run():
        def body(i, _):
            for b in range(RING):
                j = i * RING + b
                copy(j, b).wait()
                turn((j + 1) % blocks, (b + 1) % RING)
                fn(j, ring[b], wts.at[b])
                copy((j + RING) % blocks, b).start()
            return 0
        lax.fori_loop(0, blocks // RING, body, 0)
        for b in range(RING):
            copy(b, b).wait()
    return start, run


def pick_rows(tbl, parts, ids, masks):
    outs = []
    for t in range(parts):
        v = None
        for r in range(8):
            row = jnp.broadcast_to(tbl[t, pl.ds(ids[r], 1), :], (8, LANES))
            v = row if v is None else jnp.where(masks[r], row, v)
        outs.append(v)
    return outs


def gather_sum(ids, w_ref, tbl, parts, masks, j, store):
    for c in range(LANES // 32):
        out = []
        at = pl.multiple_of(j * LANES, LANES) + 32 * c
        for h in range(4):
            w8 = w_ref[32 * c + 8 * h:32 * c + 8 * h + 8, :]
            acc = None
            for k in range(ids.shape[0]):
                wk = jnp.broadcast_to(w8[:, k:k + 1], (8, LANES))
                vs = pick_rows(tbl, parts, [ids[k, 32 * c + 8 * h + r] for r in range(8)], masks)
                vs = [v * wk for v in vs]
                acc = vs if acc is None else [a + v for a, v in zip(acc, vs)]
            out.append(jnp.concatenate(acc, 1))
        store(at, jnp.concatenate(out, 0))


def send_rows(list_ref, tbl, out_ref, masks):
    blocks, size = out_ref.shape[:2]

    def body(q, _):
        for g in range(size // 32):
            blk = list_ref.at[q, pl.ds(32 * g, 32)]
            parts = [pick_rows(tbl, 1, [blk[8 * h + r] for r in range(8)], masks)[0] for h in range(4)]
            out_ref[q, pl.ds(32 * g, 32), :] = jnp.concatenate(parts, 0).astype(BF16)
        return 0
    lax.fori_loop(0, blocks, body, 0)


def chunked(total, chunk, fn):
    def body(i, _):
        fn(pl.multiple_of(i * chunk, chunk))
        return 0
    lax.fori_loop(0, total // chunk, body, 0)


def enter(n, me):
    barrier = pltpu.get_barrier_semaphore()
    for i in range(1, n):
        pl.semaphore_signal(barrier, inc=1, device_id=((me + i) % n,), device_id_type=MESH)
    return lambda: pl.semaphore_wait(barrier, n - 1)


def far_first(me, n, plane):
    z, r = me // plane, me % plane
    if n // plane == 4:
        up = z // 2
        zs = [3 - 3 * up, 2 - up, z + 1 - 2 * (z % 2)]
    else:
        zs = [(z + i) % (n // plane) for i in range(1, n // plane)]
    peers = [to * plane + (r + i) % plane for to in zs for i in range(plane)]
    return peers + [z * plane + (r + i) % plane for i in range(1, plane)]


def send_all(peers, me, src_of, dst, send_sem, recv_sem, device_of=lambda p: p):
    made = []
    for i, p in enumerate(peers):
        made.append(pltpu.make_async_remote_copy(
            src_ref=src_of(p), dst_ref=dst, send_sem=send_sem.at[i], recv_sem=recv_sem.at[me],
            device_id=(device_of(p),), device_id_type=MESH))
    for c in made:
        c.start()

    def wait(dst_of):
        for p in peers:
            pltpu.make_async_remote_copy(
                src_ref=dst_of(p), dst_ref=dst_of(p), send_sem=send_sem.at[0], recv_sem=recv_sem.at[p],
                device_id=(device_of(p),), device_id_type=MESH).wait_recv()
        for c in made:
            c.wait_send()
    return wait


def all_to_all(n, me, src, dst, send_sem, recv_sem):
    wait = send_all(far_first(me, n, 8), me, lambda p: src.at[p], dst.at[me], send_sem, recv_sem)
    return lambda: wait(lambda p: dst.at[p])


def first_kernel(n, list_ref, own_ref, mask_ref, halo_ref, total_ref, tbl, out, cnt, cnts, sems):
    me = lax.axis_index("graph")
    ready = enter(n, me)
    rows = own_ref.shape[0]
    mine = jnp.sum(mask_ref[...].astype(F32), axis=0, keepdims=True)
    for p in range(n):
        cnt[p] = mine

    def load_own(o):
        tbl[0, pl.ds(o, 256), :] = own_ref[pl.ds(o, 256), :].astype(F32)
    chunked(rows, 256, load_own)
    send_rows(list_ref, tbl, out, row_masks())
    ready()
    small = all_to_all(n, me, cnt, cnts, sems.at[0], sems.at[1])
    big = all_to_all(n, me, out, halo_ref, sems.at[2], sems.at[3])
    halo_ref[pl.ds(me, 1)] = out[pl.ds(me, 1)]
    cnts[pl.ds(me, 1)] = cnt[pl.ds(me, 1)]
    small()
    total_ref[0] = jnp.sum(jnp.sum(cnts[...], axis=0))
    big()


def exchange_kernel(n, x_ref, o_ref, sems):
    me = lax.axis_index("graph")
    enter(n, me)()
    arrived = all_to_all(n, me, x_ref, o_ref, sems.at[0], sems.at[1])
    o_ref[pl.ds(me, 1)] = x_ref[pl.ds(me, 1)]
    arrived()


def reduce_kernel(n, classes, gw1_ref, gw2t_ref, loss_ref, total_ref, o1_ref, o2_ref, ol_ref, full, pair, acc, ring, half, sems):
    chips = n // 2
    me = lax.axis_index("graph")
    chip, core = me // 2, me % 2
    ready = enter(n, me)
    full[...] = jnp.zeros_like(full)

    def tiles(rows):
        return [(i, t) for i in range(rows // 8) for t in range(2)]
    where_ = {}
    at = 0
    for name, ref, rows in (("a", gw1_ref, gw1_ref.shape[0]), ("b", gw2t_ref, gw2t_ref.shape[0])):
        for i, t in tiles(rows):
            where_[name, i, t] = (at // (3 * chips), at // 3 % chips, at % 3)
            full[where_[name, i, t]] = ref[8 * i:8 * i + 8, t * LANES:(t + 1) * LANES]
            at += 1
    last = (at // (3 * chips), at // 3 % chips, at % 3)
    full[last[0], last[1], last[2], 0:1] = loss_ref[:, :LANES] + loss_ref[:, LANES:]
    ready()
    partner = me + 1 - 2 * core
    swap = pltpu.make_async_remote_copy(src_ref=full.at[1 - core], dst_ref=pair, send_sem=sems.at[0, 0], recv_sem=sems.at[1, 0],
                                        device_id=(partner,), device_id_type=MESH)
    swap.start()
    swap.wait()
    acc[...] = pair[...] + full[core]

    peers = far_first(chip, chips, 4)

    def others(src_of, dst, s):
        return send_all(peers, chip, src_of, dst, sems.at[s], sems.at[s + 1], lambda p: 2 * p + core)
    first = others(lambda other: acc.at[other], ring.at[chip], 2)
    ring[pl.ds(chip, 1)] = acc[pl.ds(chip, 1)]
    first(lambda other: ring.at[other])
    half[pl.ds(core, 1), pl.ds(chip, 1)] = jnp.sum(ring[...], axis=0)[None, None]
    second = others(lambda other: half.at[core, chip], half.at[core, chip], 4)
    second(lambda other: half.at[core, other])
    back = pltpu.make_async_remote_copy(src_ref=half.at[core], dst_ref=half.at[core], send_sem=sems.at[0, 1], recv_sem=sems.at[1, 1],
                                        device_id=(partner,), device_id_type=MESH)
    back.start()
    back.wait()
    for name, ref, rows in (("a", o1_ref, o1_ref.shape[0]), ("b", o2_ref, gw2t_ref.shape[0])):
        for i, t in tiles(rows):
            n_rows = min(8, ref.shape[0] - 8 * i)
            ref[8 * i:8 * i + n_rows, t * LANES:(t + 1) * LANES] = half[where_[name, i, t]][:n_rows]
    ol_ref[0] = -jnp.sum(half[last]) / total_ref[0]


def layer_one_kernel(src_any, list_ref, wt_ref, own_ref, halo_ref, z_ref, out_ref, tbl, wts, ztbl, sem, *ring):
    def block(j, ids, w_ref):
        def store(at, z):
            zb = z.astype(BF16)
            z_ref[pl.ds(at, 32), :] = zb
            ztbl[0, pl.ds(at, 32), :] = zb.astype(F32)
        gather_sum(ids, w_ref, tbl, 1, masks, j, store)
    start, run = each_block(src_any, wt_ref, ring, wts, sem, block)
    start()
    rows, halo = own_ref.shape[0], halo_ref.shape[0]
    masks = row_masks()

    def load_own(o):
        tbl[0, pl.ds(o, 256), :] = own_ref[pl.ds(o, 256), :].astype(F32)

    def load_halo(o):
        tbl[0, pl.ds(o + rows, 256), :] = halo_ref[pl.ds(o, 256), :].astype(F32)
    chunked(rows, 256, load_own)
    chunked(halo, 256, load_halo)
    run()
    send_rows(list_ref, ztbl, out_ref, masks)


def hidden(z, w1):
    return jnp.maximum(dot(z, w1, ((1,), (0,))), 0.0).astype(BF16)


def layer_two_kernel(src_any, total_ref, wt_ref, z_own_ref, z_halo_ref, w1_ref, w2t_ref, lab_ref, mask_ref,
                     g2_ref, gw2t_ref, loss_ref, tbl, wts, z2, w2s, lg, g2ts, sem, *ring):
    def block(j, ids, w_ref):
        def store(at, z):
            z2[pl.ds(at, 32), :] = z.astype(BF16)
        gather_sum(ids, w_ref, tbl, 2, masks, j, store)
    start, run = each_block(src_any, wt_ref, ring, wts, sem, block)
    start()
    classes = w2t_ref.shape[0]
    rows, halo = z_own_ref.shape[0], z_halo_ref.shape[0]
    masks = row_masks()
    w1 = w1_ref[...].astype(BF16)

    def load(ref, base):
        def fn(o):
            h = hidden(ref[pl.ds(o, 1024), :], w1).astype(F32)
            tbl[0, pl.ds(o + base, 1024), :] = h[:, :LANES]
            tbl[1, pl.ds(o + base, 1024), :] = h[:, LANES:]
        return fn
    chunked(rows, 1024, load(z_own_ref, 0))
    chunked(halo, 1024, load(z_halo_ref, rows))
    run()

    total = total_ref[0]
    w2s[...] = jnp.zeros_like(w2s)
    w2s[pl.ds(0, classes), :] = w2t_ref[...].astype(BF16)
    w2t = w2s[...]
    pad_cls = w2t.shape[0]
    loss_ref[...] = jnp.zeros_like(loss_ref)
    cls = lax.broadcasted_iota(jnp.int32, (pad_cls, 256), 0)

    def project(o):
        lg[:, pl.ds(o, 1024)] = dot(w2t, z2[pl.ds(o, 1024), :], ((1,), (1,)))
    chunked(rows, 1024, project)

    def chunk(i, _):
        o = pl.multiple_of(i * 256, 256)
        logits = lg[:, pl.ds(o, 256)]
        live = cls < classes
        lab = jnp.concatenate([lab_ref[pl.ds(2 * i + t, 1), :] for t in range(2)], 1)
        mf = jnp.concatenate([mask_ref[pl.ds(2 * i + t, 1), :] for t in range(2)], 1).astype(F32)
        top = jnp.max(jnp.where(live, logits, -jnp.inf), axis=0, keepdims=True)
        shifted = logits - top
        ex = jnp.where(live, jnp.exp(shifted), 0.0)
        norm = jnp.sum(ex, axis=0, keepdims=True)
        logp = shifted - jnp.log(norm)
        hot = cls == lab
        loss_ref[...] += mf * jnp.sum(jnp.where(hot, logp, 0.0), axis=0, keepdims=True)
        g2t = ((ex * (1.0 / norm) - hot.astype(F32)) * (mf / total)).astype(BF16)
        g2ts[:, pl.ds(o, 256)] = g2t
        g2 = jnp.concatenate([g2t.astype(F32), jnp.zeros((2 * LANES - pad_cls, 256), F32)], 0).T
        g2_ref[pl.ds(o, 256), :] = g2.astype(BF16)
        return 0
    lax.fori_loop(0, rows // 256, chunk, 0)
    gw2t_ref[...] = dot(g2ts[...], z2[...], ((1,), (0,)))


PACKED = 88


def in_span(at, rows, width):
    lane = lax.broadcasted_iota(jnp.int32, (rows, LANES), 1)
    return (lane >= at) & (lane < at + width)


def scatter_kernel(in_deg, src_any, wt_ref, g2_ref, own_ref, halo_ref, sem, wts, *more):
    bufs, ring = more[:SUMS], more[SUMS:]

    def block(j, ids, w_ref):
        for c in range(LANES // 32):
            at = pl.multiple_of(j * LANES, LANES) + 32 * c
            gg = g2_ref[pl.ds(at, 32), :].astype(F32)
            for h in range(4):
                w8 = w_ref[32 * c + 8 * h:32 * c + 8 * h + 8, :]
                gs = [gg[8 * h:8 * h + 8, t * LANES:(t + 1) * LANES] for t in range(2)]
                terms = []
                for k in range(in_deg):
                    wk = jnp.broadcast_to(w8[:, k:k + 1], (8, LANES))
                    terms.append([wk * x for x in gs])
                for r in range(8):
                    for k in range(in_deg):
                        i = ids[k, 32 * c + 8 * h + r]
                        for t in range(2):
                            row = jnp.broadcast_to(bufs[((h * 8 + r) * in_deg + k) % SUMS][t, pl.ds(i, 1), :], (8, LANES)) + terms[k][t]
                            bufs[((h * 8 + r) * in_deg + k) % SUMS][t, pl.ds(i, 1), :] = row[r:r + 1, :]
    start, run = each_block(src_any, wt_ref, ring, wts, sem, block)
    start()
    rows, nodes = own_ref.shape[1], halo_ref.shape[0]

    def zero(i, _):
        for b in bufs:
            for t in range(2):
                b[t, pl.ds(pl.multiple_of(i * 64, 64), 64), :] = jnp.zeros((64, LANES), F32)
        return 0
    lax.fori_loop(0, bufs[0].shape[1] // 64, zero, 0)
    run()

    def total(t, o, n):
        s = pl.ds(o, n)
        a = bufs[0][t, s, :]
        for b in bufs[1:]:
            a = a + b[t, s, :]
        return a

    def red_own(o):
        for t in range(2):
            own_ref[t, pl.ds(o, 64), :] = total(t, o, 64)
    chunked(rows, 64, red_own)

    def red_halo(q, _):
        o = pl.multiple_of(rows + q * 64, 64)
        halo_ref[q, pl.ds(0, 64), :] = total(0, o, 64)
        hi = total(1, o, 64)
        packed = hi[:16]
        for g in range(1, 4):
            packed = jnp.where(in_span(32 * g, 16, 32), pltpu.roll(hi[16 * g:16 * g + 16], 32 * g, 1), packed)
        halo_ref[q, pl.ds(64, 16), :] = packed
        packed = pltpu.roll(hi[:8], LANES - 32, 1)
        for g in range(1, 8):
            packed = jnp.where(in_span(16 * g, 8, 16), pltpu.roll(hi[8 * g:8 * g + 8], (16 * g - 32) % LANES, 1), packed)
        halo_ref[q, pl.ds(80, 8), :] = packed
        return 0
    lax.fori_loop(0, nodes, red_halo, 0)


def combine_kernel(list_ref, own_ref, back_ref, z_ref, w1_ref, w2t_ref, gw1_ref, w2p, g1s, *bufs):
    nb = len(bufs)
    rows = own_ref.shape[1]

    def init(o):
        for t in range(2):
            bufs[0][t, pl.ds(o, 256), :] = own_ref[t, pl.ds(o, 256), :]
            for b in bufs[1:]:
                b[t, pl.ds(o, 256), :] = jnp.zeros((256, LANES), F32)
    chunked(rows, 256, init)
    first, second = in_span(0, 8, 32), in_span(32, 8, 16)

    def body(q, _):
        last = back_ref[q, pl.ds(80, 8), :]
        for g in range(8):
            lo = back_ref[q, pl.ds(8 * g, 8), :]
            mid = back_ref[q, pl.ds(64 + 8 * (g % 2), 8), :]
            mid = mid if g < 2 else pltpu.roll(mid, LANES - 32 * (g // 2), 1)
            tail = pltpu.roll(last, (32 - 16 * g) % LANES, 1) if g != 2 else last
            hi = jnp.where(first, mid, jnp.where(second, tail, 0.0))
            for r in range(8):
                b = bufs[r % nb]
                i = list_ref[q, 8 * g + r]
                for t, x in ((0, lo), (1, hi)):
                    row = jnp.broadcast_to(b[t, pl.ds(i, 1), :], (8, LANES)) + x
                    b[t, pl.ds(i, 1), :] = row[r:r + 1, :]
        return 0
    lax.fori_loop(0, back_ref.shape[0], body, 0)

    w1 = w1_ref[...].astype(BF16)
    w2p[...] = jnp.zeros_like(w2p)
    w2p[pl.ds(0, w2t_ref.shape[0]), :] = w2t_ref[...].astype(BF16)

    def finish(o):
        n = 512
        z = z_ref[pl.ds(o, n), :]
        h = hidden(z, w1)
        halves = []
        for t in range(2):
            a = bufs[0][t, pl.ds(o, n), :]
            for b in bufs[1:]:
                a = a + b[t, pl.ds(o, n), :]
            halves.append(a)
        x = jnp.concatenate(halves, 1)
        x1 = x.astype(BF16)
        rest = x - x1.astype(F32)
        x2 = rest.astype(BF16)
        x3 = (rest - x2.astype(F32)).astype(BF16)
        w2 = w2p[...]
        dh = dot(x3, w2, ((1,), (0,))) + dot(x2, w2, ((1,), (0,))) + dot(x1, w2, ((1,), (0,)))
        g1s[pl.ds(o, n), :] = jnp.where(h.astype(F32) > 0, dh, 0.0).astype(BF16)
    chunked(rows, 512, finish)
    gw1_ref[...] = dot(z_ref[...], g1s[...], ((0,), (0,)))


def solution(mesh):
    dev_count = mesh.shape["graph"]

    def device_step(feats, w_one, w_two, send_idx, send_count, edge_src, edge_wt, labels, label_mask):
        rows, feat_in = feats.shape
        hid, classes = w_two.shape
        halo_rows = send_idx.shape[1]
        in_deg = edge_src.shape[1]
        halo = dev_count * halo_rows
        ext = rows + halo + 16
        blocks = rows // LANES
        pad_cls = -(-classes // 16) * 16
        src = edge_src.T.reshape(in_deg, blocks, LANES).transpose(1, 0, 2)
        wt, w2t = edge_wt.T, w_two.T
        edge_ids = [pltpu.SMEM((in_deg, LANES), jnp.int32)] * RING
        edge_w = pltpu.VMEM((RING, LANES, 8), F32)
        edge_sem = pltpu.SemaphoreType.DMA((RING,))

        def comm(limit_mib, cid):
            return pltpu.CompilerParams(vmem_limit_bytes=limit_mib * 2**20,
                                        collective_id=cid, has_side_effects=True)

        def exchange(x, cid):
            return pl.pallas_call(
                functools.partial(exchange_kernel, dev_count), out_shape=jax.ShapeDtypeStruct(x.shape, x.dtype),
                in_specs=[VMEM], out_specs=VMEM, scratch_shapes=[pltpu.SemaphoreType.DMA((2, dev_count))],
                compiler_params=comm(8, cid), name="exchange", cost_estimate=pl.CostEstimate(flops=16 * WORK, bytes_accessed=0, transcendentals=0),
            )(x)

        halo0, total = pl.pallas_call(
            functools.partial(first_kernel, dev_count),
            out_shape=[jax.ShapeDtypeStruct((dev_count, halo_rows, feat_in), BF16), jax.ShapeDtypeStruct((1,), F32)],
            in_specs=[SMEM, VMEM, VMEM], out_specs=[VMEM, SMEM],
            scratch_shapes=[pltpu.VMEM((1, rows, feat_in), F32), pltpu.VMEM((dev_count, halo_rows, feat_in), BF16),
                            pltpu.VMEM((dev_count, 1, LANES), F32), pltpu.VMEM((dev_count, 1, LANES), F32),
                            pltpu.SemaphoreType.DMA((4, dev_count))],
            compiler_params=comm(16, 0), name="first", cost_estimate=pl.CostEstimate(flops=20 * WORK, bytes_accessed=0, transcendentals=0),
        )(send_idx, feats, label_mask.reshape(blocks, LANES))
        z1, out1 = pl.pallas_call(
            layer_one_kernel,
            out_shape=[jax.ShapeDtypeStruct((rows, feat_in), BF16), jax.ShapeDtypeStruct((dev_count, halo_rows, feat_in), BF16)],
            in_specs=[ANY, SMEM, VMEM, VMEM, VMEM], out_specs=[VMEM, VMEM],
            scratch_shapes=[pltpu.VMEM((1, ext, feat_in), F32), edge_w, pltpu.VMEM((1, rows, feat_in), F32), edge_sem] + edge_ids,
            compiler_params=params(16), name="layer_one", cost_estimate=pl.CostEstimate(flops=19 * WORK, bytes_accessed=0, transcendentals=0),
        )(src, send_idx, wt, feats, halo0.reshape(halo, feat_in))
        zh = exchange(out1, 1).reshape(halo, feat_in)
        g2, gw2t, loss_part = pl.pallas_call(
            layer_two_kernel,
            out_shape=[jax.ShapeDtypeStruct((rows, 2 * LANES), BF16), jax.ShapeDtypeStruct((pad_cls, hid), F32), jax.ShapeDtypeStruct((1, 256), F32)],
            in_specs=[ANY, SMEM, VMEM, VMEM, VMEM, VMEM, VMEM, VMEM, VMEM], out_specs=[VMEM, VMEM, VMEM],
            scratch_shapes=[pltpu.VMEM((2, ext, LANES), F32), edge_w, pltpu.VMEM((rows, hid), BF16),
                            pltpu.VMEM((pad_cls, hid), BF16), pltpu.VMEM((pad_cls, rows), F32), pltpu.VMEM((pad_cls, rows), BF16), edge_sem] + edge_ids,
            compiler_params=params(28), name="layer_two", cost_estimate=pl.CostEstimate(flops=28 * WORK, bytes_accessed=0, transcendentals=0),
        )(src, total, wt, z1, zh, w_one, w2t, labels.reshape(blocks, LANES), label_mask.reshape(blocks, LANES))
        own, halo_g = pl.pallas_call(
            functools.partial(scatter_kernel, in_deg),
            out_shape=[jax.ShapeDtypeStruct((2, rows, LANES), F32), jax.ShapeDtypeStruct((dev_count, PACKED, LANES), F32)],
            in_specs=[ANY, VMEM, VMEM], out_specs=[VMEM, VMEM],
            scratch_shapes=[edge_sem, edge_w] + [pltpu.VMEM((2, ext, LANES), F32)] * SUMS + edge_ids,
            compiler_params=params(39), name="scatter", cost_estimate=pl.CostEstimate(flops=33 * WORK, bytes_accessed=0, transcendentals=0),
        )(src, wt, g2)
        back = exchange(halo_g, 2)
        gw1 = pl.pallas_call(
            combine_kernel, out_shape=jax.ShapeDtypeStruct((feat_in, hid), F32),
            in_specs=[SMEM, VMEM, VMEM, VMEM, VMEM, VMEM], out_specs=VMEM,
            scratch_shapes=[pltpu.VMEM((2 * LANES, hid), BF16), pltpu.VMEM((rows, hid), BF16)] + [pltpu.VMEM((2, rows + 16, LANES), F32)] * 4,
            compiler_params=params(32), name="combine", cost_estimate=pl.CostEstimate(flops=11 * WORK, bytes_accessed=0, transcendentals=0),
        )(send_idx, own, back, z1, w_one, w2t)
        chips = dev_count // 2
        gw1, gw2t, loss = pl.pallas_call(
            functools.partial(reduce_kernel, dev_count, classes),
            out_shape=[jax.ShapeDtypeStruct((feat_in, hid), F32), jax.ShapeDtypeStruct((classes, hid), F32), jax.ShapeDtypeStruct((1,), F32)],
            in_specs=[VMEM, VMEM, VMEM, SMEM], out_specs=[VMEM, VMEM, SMEM],
            scratch_shapes=[pltpu.VMEM((2, chips, 3, 8, LANES), F32), pltpu.VMEM((chips, 3, 8, LANES), F32), pltpu.VMEM((chips, 3, 8, LANES), F32),
                            pltpu.VMEM((chips, 3, 8, LANES), F32), pltpu.VMEM((2, chips, 3, 8, LANES), F32), pltpu.SemaphoreType.DMA((6, dev_count))],
            compiler_params=comm(8, 3), name="reduce", cost_estimate=pl.CostEstimate(flops=20 * WORK, bytes_accessed=0, transcendentals=0),
        )(gw1, gw2t, loss_part, total)
        return loss[0], gw1, gw2t.T

    row_spec = P("graph", None)
    vec_spec = P("graph")
    return jax.shard_map(device_step, mesh=mesh, in_specs=(row_spec, P(), P(), row_spec, vec_spec, row_spec, row_spec, vec_spec, vec_spec), out_specs=(P(), P(), P()), check_vma=False)
```

```python
import functools

import jax
import jax.numpy as jnp
from jax import lax
from jax.experimental import pallas as pl
from jax.experimental.pallas import tpu as pltpu
from jax.sharding import PartitionSpec as P

LANES = 128
F32, BF16 = jnp.float32, jnp.bfloat16
VMEM = pl.BlockSpec(memory_space=pltpu.VMEM)
SMEM = pl.BlockSpec(memory_space=pltpu.SMEM)
ANY = pl.BlockSpec(memory_space=pl.ANY)
MESH = pl.DeviceIdType.MESH


def params(limit_mib):
    return pltpu.CompilerParams(vmem_limit_bytes=limit_mib * 2**20)


def row_masks():
    sub = lax.broadcasted_iota(jnp.int32, (8, LANES), 0)
    return [sub == r for r in range(8)]


def dot(a, b, dims):
    return lax.dot_general(a, b, (dims, ((), ())), preferred_element_type=F32)


SUMS = 6
RING = 4


def each_block(src_any, wt_ref, ring, wts, sem, fn):
    blocks = src_any.shape[0]
    deg = wt_ref.shape[0]

    def copy(j, b):
        return pltpu.make_async_copy(src_any.at[j], ring[b], sem.at[b])

    def turn(j, b):
        cols = wt_ref[:, pl.ds(pl.multiple_of(j * LANES, LANES), LANES)]
        wts[b] = jnp.concatenate([cols, jnp.zeros((8 - deg, LANES), F32)], 0).T

    def start():
        for b in range(RING):
            copy(b, b).start()
        turn(0, 0)

    def run():
        def body(i, _):
            for b in range(RING):
                j = i * RING + b
                copy(j, b).wait()
                turn(jnp.minimum(j + 1, blocks - 1), (b + 1) % RING)
                fn(j, ring[b], wts.at[b])

                @pl.when(j + RING < blocks)
                def _():
                    copy(j + RING, b).start()
            return 0
        lax.fori_loop(0, blocks // RING, body, 0)
    return start, run


def pick_rows(tbl, parts, ids, masks):
    outs = []
    for t in range(parts):
        v = None
        for r in range(8):
            row = jnp.broadcast_to(tbl[t, pl.ds(ids[r], 1), :], (8, LANES))
            v = row if v is None else jnp.where(masks[r], row, v)
        outs.append(v)
    return outs


def gather_sum(ids, w_ref, tbl, parts, masks, j, store):
    for c in range(LANES // 32):
        out = []
        at = pl.multiple_of(j * LANES, LANES) + 32 * c
        for h in range(4):
            w8 = w_ref[32 * c + 8 * h:32 * c + 8 * h + 8, :]
            acc = None
            for k in range(ids.shape[0]):
                wk = jnp.broadcast_to(w8[:, k:k + 1], (8, LANES))
                vs = pick_rows(tbl, parts, [ids[k, 32 * c + 8 * h + r] for r in range(8)], masks)
                vs = [v * wk for v in vs]
                acc = vs if acc is None else [a + v for a, v in zip(acc, vs)]
            out.append(jnp.concatenate(acc, 1))
        store(at, jnp.concatenate(out, 0))


def send_rows(list_ref, tbl, out_ref, masks):
    blocks, size = out_ref.shape[:2]

    def body(q, _):
        for g in range(size // 32):
            blk = list_ref.at[q, pl.ds(32 * g, 32)]
            parts = [pick_rows(tbl, 1, [blk[8 * h + r] for r in range(8)], masks)[0] for h in range(4)]
            out_ref[q, pl.ds(32 * g, 32), :] = jnp.concatenate(parts, 0).astype(BF16)
        return 0
    lax.fori_loop(0, blocks, body, 0)


def chunked(total, chunk, fn):
    def body(i, _):
        fn(pl.multiple_of(i * chunk, chunk))
        return 0
    lax.fori_loop(0, total // chunk, body, 0)


def enter(n, me):
    barrier = pltpu.get_barrier_semaphore()
    for i in range(1, n):
        pl.semaphore_signal(barrier, inc=1, device_id=((me + i) % n,), device_id_type=MESH)
    return lambda: pl.semaphore_wait(barrier, n - 1)


def far_first(me, n, plane):
    z, r = me // plane, me % plane
    if n // plane == 4:
        up = z // 2
        zs = [3 - 3 * up, 2 - up, z + 1 - 2 * (z % 2)]
    else:
        zs = [(z + i) % (n // plane) for i in range(1, n // plane)]
    peers = [to * plane + (r + i) % plane for to in zs for i in range(plane)]
    return peers + [z * plane + (r + i) % plane for i in range(1, plane)]


def send_all(peers, me, src_of, dst, send_sem, recv_sem, device_of=lambda p: p):
    made = []
    for i, p in enumerate(peers):
        made.append(pltpu.make_async_remote_copy(
            src_ref=src_of(p), dst_ref=dst, send_sem=send_sem.at[i], recv_sem=recv_sem.at[me],
            device_id=(device_of(p),), device_id_type=MESH))
    for c in made:
        c.start()

    def wait(dst_of):
        for p in peers:
            pltpu.make_async_remote_copy(
                src_ref=dst_of(p), dst_ref=dst_of(p), send_sem=send_sem.at[0], recv_sem=recv_sem.at[p],
                device_id=(device_of(p),), device_id_type=MESH).wait_recv()
        for c in made:
            c.wait_send()
    return wait


def all_to_all(n, me, src, dst, send_sem, recv_sem):
    wait = send_all(far_first(me, n, 8), me, lambda p: src.at[p], dst.at[me], send_sem, recv_sem)
    return lambda: wait(lambda p: dst.at[p])


def first_kernel(n, list_ref, own_ref, mask_ref, halo_ref, total_ref, tbl, out, cnt, cnts, sems):
    me = lax.axis_index("graph")
    ready = enter(n, me)
    rows = own_ref.shape[0]
    mine = jnp.sum(mask_ref[...].astype(F32), axis=0, keepdims=True)
    for p in range(n):
        cnt[p] = mine

    def load_own(o):
        tbl[0, pl.ds(o, 256), :] = own_ref[pl.ds(o, 256), :].astype(F32)
    chunked(rows, 256, load_own)
    send_rows(list_ref, tbl, out, row_masks())
    ready()
    big = all_to_all(n, me, out, halo_ref, sems.at[2], sems.at[3])
    small = all_to_all(n, me, cnt, cnts, sems.at[0], sems.at[1])
    halo_ref[pl.ds(me, 1)] = out[pl.ds(me, 1)]
    cnts[pl.ds(me, 1)] = cnt[pl.ds(me, 1)]
    small()
    total_ref[0] = jnp.sum(jnp.sum(cnts[...], axis=0))
    big()


def exchange_kernel(n, x_ref, o_ref, sems):
    me = lax.axis_index("graph")
    enter(n, me)()
    arrived = all_to_all(n, me, x_ref, o_ref, sems.at[0], sems.at[1])
    o_ref[pl.ds(me, 1)] = x_ref[pl.ds(me, 1)]
    arrived()


def reduce_kernel(n, classes, gw1_ref, gw2t_ref, loss_ref, total_ref, o1_ref, o2_ref, ol_ref, full, pair, acc, ring, half, sems):
    chips = n // 2
    me = lax.axis_index("graph")
    chip, core = me // 2, me % 2
    ready = enter(n, me)
    full[...] = jnp.zeros_like(full)
    per = full.shape[2]

    def tiles(rows):
        return [(i, t) for i in range(rows // 4) for t in range(2)]

    def place(at):
        return at // (per * chips), at // per % chips, at % per
    where_ = {}
    for name, ref, rows in (("a", gw1_ref, gw1_ref.shape[0]), ("b", gw2t_ref, classes)):
        for i, t in tiles(rows):
            where_[name, i, t] = place(len(where_))
            full[where_[name, i, t]] = ref[4 * i:4 * i + 4, t * LANES:(t + 1) * LANES]
    last = place(len(where_))
    full[last[0], last[1], last[2], 0:1] = loss_ref[:, :LANES] + loss_ref[:, LANES:]
    ready()
    partner = me + 1 - 2 * core
    swap = pltpu.make_async_remote_copy(src_ref=full.at[1 - core], dst_ref=pair, send_sem=sems.at[0, 0], recv_sem=sems.at[1, 0],
                                        device_id=(partner,), device_id_type=MESH)
    swap.start()
    swap.wait()
    acc[...] = pair[...] + full[core]

    peers = far_first(chip, chips, 4)

    def others(src_of, dst, s):
        return send_all(peers, chip, src_of, dst, sems.at[s], sems.at[s + 1], lambda p: 2 * p + core)
    first = others(lambda other: acc.at[other], ring.at[chip], 2)
    ring[pl.ds(chip, 1)] = acc[pl.ds(chip, 1)]
    first(lambda other: ring.at[other])
    half[pl.ds(core, 1), pl.ds(chip, 1)] = jnp.sum(ring[...], axis=0)[None, None]
    second = others(lambda other: half.at[core, chip], half.at[core, chip], 4)
    second(lambda other: half.at[core, other])
    back = pltpu.make_async_remote_copy(src_ref=half.at[core], dst_ref=half.at[core], send_sem=sems.at[0, 1], recv_sem=sems.at[1, 1],
                                        device_id=(partner,), device_id_type=MESH)
    back.start()
    back.wait()
    for name, ref in (("a", o1_ref), ("b", o2_ref)):
        for i, t in tiles(ref.shape[0]):
            ref[4 * i:4 * i + 4, t * LANES:(t + 1) * LANES] = half[where_[name, i, t]]
    ol_ref[0] = -jnp.sum(half[last]) / total_ref[0]


def layer_one_kernel(src_any, list_ref, wt_ref, own_ref, halo_ref, z_ref, out_ref, tbl, wts, ztbl, sem, *ring):
    def block(j, ids, w_ref):
        def store(at, z):
            zb = z.astype(BF16)
            z_ref[pl.ds(at, 32), :] = zb
            ztbl[0, pl.ds(at, 32), :] = zb.astype(F32)
        gather_sum(ids, w_ref, tbl, 1, masks, j, store)
    start, run = each_block(src_any, wt_ref, ring, wts, sem, block)
    start()
    rows, halo = own_ref.shape[0], halo_ref.shape[0]
    masks = row_masks()

    def load_own(o):
        tbl[0, pl.ds(o, 256), :] = own_ref[pl.ds(o, 256), :].astype(F32)

    def load_halo(o):
        tbl[0, pl.ds(o + rows, 256), :] = halo_ref[pl.ds(o, 256), :].astype(F32)
    chunked(rows, 256, load_own)
    chunked(halo, 256, load_halo)
    run()
    send_rows(list_ref, ztbl, out_ref, masks)


def hidden(z, w1):
    return jnp.maximum(dot(z, w1, ((1,), (0,))), 0.0).astype(BF16)


def layer_two_kernel(src_any, total_ref, wt_ref, z_own_ref, z_halo_ref, w1_ref, w2t_ref, lab_ref, mask_ref,
                     g2_ref, gw2t_ref, loss_ref, tbl, wts, z2, w2s, lg, g2ts, sem, *ring):
    def block(j, ids, w_ref):
        def store(at, z):
            z2[pl.ds(at, 32), :] = z.astype(BF16)
        gather_sum(ids, w_ref, tbl, 2, masks, j, store)
    start, run = each_block(src_any, wt_ref, ring, wts, sem, block)
    start()
    classes = w2t_ref.shape[0]
    rows, halo = z_own_ref.shape[0], z_halo_ref.shape[0]
    masks = row_masks()
    w1 = w1_ref[...].astype(BF16)

    def load(ref, base):
        def fn(o):
            h = hidden(ref[pl.ds(o, 1024), :], w1).astype(F32)
            tbl[0, pl.ds(o + base, 1024), :] = h[:, :LANES]
            tbl[1, pl.ds(o + base, 1024), :] = h[:, LANES:]
        return fn
    chunked(rows, 1024, load(z_own_ref, 0))
    chunked(halo, 1024, load(z_halo_ref, rows))
    run()

    total = total_ref[0]
    w2s[...] = jnp.zeros_like(w2s)
    w2s[pl.ds(0, classes), :] = w2t_ref[...].astype(BF16)
    w2t = w2s[...]
    pad_cls = w2t.shape[0]
    loss_ref[...] = jnp.zeros_like(loss_ref)
    cls = lax.broadcasted_iota(jnp.int32, (pad_cls, 256), 0)

    def project(o):
        lg[:, pl.ds(o, 1024)] = dot(w2t, z2[pl.ds(o, 1024), :], ((1,), (1,)))
    chunked(rows, 1024, project)

    def chunk(i, _):
        o = pl.multiple_of(i * 256, 256)
        logits = lg[:, pl.ds(o, 256)]
        live = cls < classes
        lab = jnp.concatenate([lab_ref[pl.ds(2 * i + t, 1), :] for t in range(2)], 1)
        mf = jnp.concatenate([mask_ref[pl.ds(2 * i + t, 1), :] for t in range(2)], 1).astype(F32)
        top = jnp.max(jnp.where(live, logits, -jnp.inf), axis=0, keepdims=True)
        shifted = logits - top
        ex = jnp.where(live, jnp.exp(shifted), 0.0)
        norm = jnp.sum(ex, axis=0, keepdims=True)
        logp = shifted - jnp.log(norm)
        hot = cls == lab
        loss_ref[...] += mf * jnp.sum(jnp.where(hot, logp, 0.0), axis=0, keepdims=True)
        g2t = ((ex * (1.0 / norm) - hot.astype(F32)) * (mf / total)).astype(BF16)
        g2ts[:, pl.ds(o, 256)] = g2t
        g2 = jnp.concatenate([g2t.astype(F32), jnp.zeros((2 * LANES - pad_cls, 256), F32)], 0).T
        g2_ref[pl.ds(o, 256), :] = g2.astype(BF16)
        return 0
    lax.fori_loop(0, rows // 256, chunk, 0)
    gw2t_ref[...] = dot(g2ts[...], z2[...], ((1,), (0,)))


PACKED = 88


def in_span(at, rows, width):
    lane = lax.broadcasted_iota(jnp.int32, (rows, LANES), 1)
    return (lane >= at) & (lane < at + width)


def scatter_kernel(in_deg, src_any, wt_ref, g2_ref, own_ref, halo_ref, sem, wts, *more):
    bufs, ring = more[:SUMS], more[SUMS:]

    def block(j, ids, w_ref):
        for c in range(LANES // 32):
            at = pl.multiple_of(j * LANES, LANES) + 32 * c
            gg = g2_ref[pl.ds(at, 32), :].astype(F32)
            for h in range(4):
                w8 = w_ref[32 * c + 8 * h:32 * c + 8 * h + 8, :]
                gs = [gg[8 * h:8 * h + 8, t * LANES:(t + 1) * LANES] for t in range(2)]
                terms = []
                for k in range(in_deg):
                    wk = jnp.broadcast_to(w8[:, k:k + 1], (8, LANES))
                    terms.append([wk * x for x in gs])
                for r in range(8):
                    for k in range(in_deg):
                        i = ids[k, 32 * c + 8 * h + r]
                        for t in range(2):
                            row = jnp.broadcast_to(bufs[((h * 8 + r) * in_deg + k) % SUMS][t, pl.ds(i, 1), :], (8, LANES)) + terms[k][t]
                            bufs[((h * 8 + r) * in_deg + k) % SUMS][t, pl.ds(i, 1), :] = row[r:r + 1, :]
    start, run = each_block(src_any, wt_ref, ring, wts, sem, block)
    start()
    rows, nodes = own_ref.shape[1], halo_ref.shape[0]

    def zero(i, _):
        for b in bufs:
            for t in range(2):
                b[t, pl.ds(pl.multiple_of(i * 64, 64), 64), :] = jnp.zeros((64, LANES), F32)
        return 0
    lax.fori_loop(0, bufs[0].shape[1] // 64, zero, 0)
    run()

    def total(t, o, n):
        s = pl.ds(o, n)
        a = bufs[0][t, s, :]
        for b in bufs[1:]:
            a = a + b[t, s, :]
        return a

    def red_own(o):
        for t in range(2):
            own_ref[t, pl.ds(o, 64), :] = total(t, o, 64)
    chunked(rows, 64, red_own)

    def red_halo(q, _):
        o = pl.multiple_of(rows + q * 64, 64)
        halo_ref[q, pl.ds(0, 64), :] = total(0, o, 64)
        hi = total(1, o, 64)
        packed = hi[:16]
        for g in range(1, 4):
            packed = jnp.where(in_span(32 * g, 16, 32), pltpu.roll(hi[16 * g:16 * g + 16], 32 * g, 1), packed)
        halo_ref[q, pl.ds(64, 16), :] = packed
        packed = pltpu.roll(hi[:8], LANES - 32, 1)
        for g in range(1, 8):
            packed = jnp.where(in_span(16 * g, 8, 16), pltpu.roll(hi[8 * g:8 * g + 8], (16 * g - 32) % LANES, 1), packed)
        halo_ref[q, pl.ds(80, 8), :] = packed
        return 0
    lax.fori_loop(0, nodes, red_halo, 0)


def combine_kernel(list_ref, own_ref, back_ref, z_ref, w1_ref, w2t_ref, gw1_ref, w2p, g1s, *bufs):
    nb = len(bufs)
    rows = own_ref.shape[1]

    def init(o):
        for t in range(2):
            bufs[0][t, pl.ds(o, 256), :] = own_ref[t, pl.ds(o, 256), :]
            for b in bufs[1:]:
                b[t, pl.ds(o, 256), :] = jnp.zeros((256, LANES), F32)
    chunked(rows, 256, init)
    first, second = in_span(0, 8, 32), in_span(32, 8, 16)

    def body(q, _):
        last = back_ref[q, pl.ds(80, 8), :]
        for g in range(8):
            lo = back_ref[q, pl.ds(8 * g, 8), :]
            mid = back_ref[q, pl.ds(64 + 8 * (g % 2), 8), :]
            mid = mid if g < 2 else pltpu.roll(mid, LANES - 32 * (g // 2), 1)
            tail = pltpu.roll(last, (32 - 16 * g) % LANES, 1) if g != 2 else last
            hi = jnp.where(first, mid, jnp.where(second, tail, 0.0))
            for r in range(8):
                b = bufs[r % nb]
                i = list_ref[q, 8 * g + r]
                for t, x in ((0, lo), (1, hi)):
                    row = jnp.broadcast_to(b[t, pl.ds(i, 1), :], (8, LANES)) + x
                    b[t, pl.ds(i, 1), :] = row[r:r + 1, :]
        return 0
    lax.fori_loop(0, back_ref.shape[0], body, 0)

    w1 = w1_ref[...].astype(BF16)
    w2p[...] = jnp.zeros_like(w2p)
    w2p[pl.ds(0, w2t_ref.shape[0]), :] = w2t_ref[...].astype(BF16)

    def finish(o):
        n = 512
        z = z_ref[pl.ds(o, n), :]
        h = hidden(z, w1)
        halves = []
        for t in range(2):
            a = bufs[0][t, pl.ds(o, n), :]
            for b in bufs[1:]:
                a = a + b[t, pl.ds(o, n), :]
            halves.append(a)
        x = jnp.concatenate(halves, 1)
        x1 = x.astype(BF16)
        rest = x - x1.astype(F32)
        x2 = rest.astype(BF16)
        x3 = (rest - x2.astype(F32)).astype(BF16)
        w2 = w2p[...]
        dh = dot(x3, w2, ((1,), (0,))) + dot(x2, w2, ((1,), (0,))) + dot(x1, w2, ((1,), (0,)))
        g1s[pl.ds(o, n), :] = jnp.where(h.astype(F32) > 0, dh, 0.0).astype(BF16)
    chunked(rows, 512, finish)
    gw1_ref[...] = dot(z_ref[...], g1s[...], ((0,), (0,)))


def solution(mesh):
    dev_count = mesh.shape["graph"]

    def device_step(feats, w_one, w_two, send_idx, send_count, edge_src, edge_wt, labels, label_mask):
        rows, feat_in = feats.shape
        hid, classes = w_two.shape
        halo_rows = send_idx.shape[1]
        in_deg = edge_src.shape[1]
        halo = dev_count * halo_rows
        ext = rows + halo + 16
        blocks = rows // LANES
        pad_cls = -(-classes // 16) * 16
        src = edge_src.T.reshape(in_deg, blocks, LANES).transpose(1, 0, 2)
        wt, w2t = edge_wt.T, w_two.T
        edge_ids = [pltpu.SMEM((in_deg, LANES), jnp.int32)] * RING
        edge_w = pltpu.VMEM((RING, LANES, 8), F32)
        edge_sem = pltpu.SemaphoreType.DMA((RING,))

        def comm(limit_mib, cid):
            return pltpu.CompilerParams(vmem_limit_bytes=limit_mib * 2**20,
                                        collective_id=cid, has_side_effects=True)

        def exchange(x, cid):
            return pl.pallas_call(
                functools.partial(exchange_kernel, dev_count), out_shape=jax.ShapeDtypeStruct(x.shape, x.dtype),
                in_specs=[VMEM], out_specs=VMEM, scratch_shapes=[pltpu.SemaphoreType.DMA((2, dev_count))],
                compiler_params=comm(8, cid), name="exchange",
            )(x)

        halo0, total = pl.pallas_call(
            functools.partial(first_kernel, dev_count),
            out_shape=[jax.ShapeDtypeStruct((dev_count, halo_rows, feat_in), BF16), jax.ShapeDtypeStruct((1,), F32)],
            in_specs=[SMEM, VMEM, VMEM], out_specs=[VMEM, SMEM],
            scratch_shapes=[pltpu.VMEM((1, rows, feat_in), F32), pltpu.VMEM((dev_count, halo_rows, feat_in), BF16),
                            pltpu.VMEM((dev_count, 1, LANES), F32), pltpu.VMEM((dev_count, 1, LANES), F32),
                            pltpu.SemaphoreType.DMA((4, dev_count))],
            compiler_params=comm(16, 0), name="first",
        )(send_idx, feats, label_mask.reshape(blocks, LANES))
        z1, out1 = pl.pallas_call(
            layer_one_kernel,
            out_shape=[jax.ShapeDtypeStruct((rows, feat_in), BF16), jax.ShapeDtypeStruct((dev_count, halo_rows, feat_in), BF16)],
            in_specs=[ANY, SMEM, VMEM, VMEM, VMEM], out_specs=[VMEM, VMEM],
            scratch_shapes=[pltpu.VMEM((1, ext, feat_in), F32), edge_w, pltpu.VMEM((1, rows, feat_in), F32), edge_sem] + edge_ids,
            compiler_params=params(16), name="layer_one",
        )(src, send_idx, wt, feats, halo0.reshape(halo, feat_in))
        zh = exchange(out1, 1).reshape(halo, feat_in)
        g2, gw2t, loss_part = pl.pallas_call(
            layer_two_kernel,
            out_shape=[jax.ShapeDtypeStruct((rows, 2 * LANES), BF16), jax.ShapeDtypeStruct((pad_cls, hid), F32), jax.ShapeDtypeStruct((1, 256), F32)],
            in_specs=[ANY, SMEM, VMEM, VMEM, VMEM, VMEM, VMEM, VMEM, VMEM], out_specs=[VMEM, VMEM, VMEM],
            scratch_shapes=[pltpu.VMEM((2, ext, LANES), F32), edge_w, pltpu.VMEM((rows, hid), BF16),
                            pltpu.VMEM((pad_cls, hid), BF16), pltpu.VMEM((pad_cls, rows), F32), pltpu.VMEM((pad_cls, rows), BF16), edge_sem] + edge_ids,
            compiler_params=params(28), name="layer_two",
        )(src, total, wt, z1, zh, w_one, w2t, labels.reshape(blocks, LANES), label_mask.reshape(blocks, LANES))
        own, halo_g = pl.pallas_call(
            functools.partial(scatter_kernel, in_deg),
            out_shape=[jax.ShapeDtypeStruct((2, rows, LANES), F32), jax.ShapeDtypeStruct((dev_count, PACKED, LANES), F32)],
            in_specs=[ANY, VMEM, VMEM], out_specs=[VMEM, VMEM],
            scratch_shapes=[edge_sem, edge_w] + [pltpu.VMEM((2, ext, LANES), F32)] * SUMS + edge_ids,
            compiler_params=params(39), name="scatter",
        )(src, wt, g2)
        back = exchange(halo_g, 2)
        gw1 = pl.pallas_call(
            combine_kernel, out_shape=jax.ShapeDtypeStruct((feat_in, hid), F32),
            in_specs=[SMEM, VMEM, VMEM, VMEM, VMEM, VMEM], out_specs=VMEM,
            scratch_shapes=[pltpu.VMEM((2 * LANES, hid), BF16), pltpu.VMEM((rows, hid), BF16)] + [pltpu.VMEM((2, rows + 16, LANES), F32)] * 4,
            compiler_params=params(32), name="combine",
        )(send_idx, own, back, z1, w_one, w2t)
        chips = dev_count // 2
        per = -(-(2 * (feat_in + classes) // 4 + 1) // (2 * chips))
        gw1, gw2t, loss = pl.pallas_call(
            functools.partial(reduce_kernel, dev_count, classes),
            out_shape=[jax.ShapeDtypeStruct((feat_in, hid), F32), jax.ShapeDtypeStruct((classes, hid), F32), jax.ShapeDtypeStruct((1,), F32)],
            in_specs=[VMEM, VMEM, VMEM, SMEM], out_specs=[VMEM, VMEM, SMEM],
            scratch_shapes=[pltpu.VMEM((2, chips, per, 4, LANES), F32), pltpu.VMEM((chips, per, 4, LANES), F32), pltpu.VMEM((chips, per, 4, LANES), F32),
                            pltpu.VMEM((chips, per, 4, LANES), F32), pltpu.VMEM((2, chips, per, 4, LANES), F32), pltpu.SemaphoreType.DMA((6, dev_count))],
            compiler_params=comm(8, 3), name="reduce",
        )(gw1, gw2t, loss_part, total)
        return loss[0], gw1, gw2t.T

    row_spec = P("graph", None)
    vec_spec = P("graph")
    return jax.shard_map(device_step, mesh=mesh, in_specs=(row_spec, P(), P(), row_spec, vec_spec, row_spec, row_spec, vec_spec, vec_spec), out_specs=(P(), P(), P()), check_vma=False)
```

```python
import functools

import jax
import jax.numpy as jnp
from jax import lax
from jax.experimental import pallas as pl
from jax.experimental.pallas import tpu as pltpu
from jax.sharding import PartitionSpec as P

LANES = 128
F32, BF16 = jnp.float32, jnp.bfloat16
VMEM = pl.BlockSpec(memory_space=pltpu.VMEM)
SMEM = pl.BlockSpec(memory_space=pltpu.SMEM)
ANY = pl.BlockSpec(memory_space=pl.ANY)
MESH = pl.DeviceIdType.MESH


def params(limit_mib):
    return pltpu.CompilerParams(vmem_limit_bytes=limit_mib * 2**20)


def row_masks():
    sub = lax.broadcasted_iota(jnp.int32, (8, LANES), 0)
    return [sub == r for r in range(8)]


def dot(a, b, dims):
    return lax.dot_general(a, b, (dims, ((), ())), preferred_element_type=F32)


SUMS = 7
RING = 4


def each_block(src_any, wt_ref, ring, wts, sem, fn):
    blocks = src_any.shape[0]
    deg = wt_ref.shape[0]

    def copy(j, b):
        return pltpu.make_async_copy(src_any.at[j], ring[b], sem.at[b])

    def turn(j, b):
        cols = wt_ref[:, pl.ds(pl.multiple_of(j * LANES, LANES), LANES)]
        wts[b] = jnp.concatenate([cols, jnp.zeros((8 - deg, LANES), F32)], 0).T

    def start():
        for b in range(RING):
            copy(b, b).start()
        turn(0, 0)

    def run():
        def body(i, _):
            for b in range(RING):
                j = i * RING + b
                copy(j, b).wait()
                turn(jnp.minimum(j + 1, blocks - 1), (b + 1) % RING)
                fn(j, ring[b], wts.at[b])

                @pl.when(j + RING < blocks)
                def _():
                    copy(j + RING, b).start()
            return 0
        lax.fori_loop(0, blocks // RING, body, 0)
    return start, run


def pick_rows(tbl, parts, ids, masks):
    outs = []
    for t in range(parts):
        v = None
        for r in range(8):
            row = jnp.broadcast_to(tbl[t, pl.ds(ids[r], 1), :], (8, LANES))
            v = row if v is None else jnp.where(masks[r], row, v)
        outs.append(v)
    return outs


def gather_sum(ids, w_ref, tbl, parts, masks, j, store):
    for c in range(LANES // 32):
        out = []
        at = pl.multiple_of(j * LANES, LANES) + 32 * c
        for h in range(4):
            w8 = w_ref[32 * c + 8 * h:32 * c + 8 * h + 8, :]
            acc = None
            for k in range(ids.shape[0]):
                wk = jnp.broadcast_to(w8[:, k:k + 1], (8, LANES))
                vs = pick_rows(tbl, parts, [ids[k, 32 * c + 8 * h + r] for r in range(8)], masks)
                vs = [v * wk for v in vs]
                acc = vs if acc is None else [a + v for a, v in zip(acc, vs)]
            out.append(jnp.concatenate(acc, 1))
        store(at, jnp.concatenate(out, 0))


def send_rows(list_ref, tbl, out_ref, masks):
    blocks, size = out_ref.shape[:2]

    def body(q, _):
        for g in range(size // 32):
            blk = list_ref.at[q, pl.ds(32 * g, 32)]
            parts = [pick_rows(tbl, 1, [blk[8 * h + r] for r in range(8)], masks)[0] for h in range(4)]
            out_ref[q, pl.ds(32 * g, 32), :] = jnp.concatenate(parts, 0).astype(BF16)
        return 0
    lax.fori_loop(0, blocks, body, 0)


def chunked(total, chunk, fn):
    def body(i, _):
        fn(pl.multiple_of(i * chunk, chunk))
        return 0
    lax.fori_loop(0, total // chunk, body, 0)


def enter(n, me):
    barrier = pltpu.get_barrier_semaphore()
    for i in range(1, n):
        pl.semaphore_signal(barrier, inc=1, device_id=((me + i) % n,), device_id_type=MESH)
    return lambda: pl.semaphore_wait(barrier, n - 1)


def far_first(me, n, plane):
    z, r = me // plane, me % plane
    if n // plane == 4:
        up = z // 2
        zs = [3 - 3 * up, 2 - up, z + 1 - 2 * (z % 2)]
    else:
        zs = [(z + i) % (n // plane) for i in range(1, n // plane)]
    peers = [to * plane + (r + i) % plane for to in zs for i in range(plane)]
    return peers + [z * plane + (r + i) % plane for i in range(1, plane)]


def send_all(peers, me, src_of, dst, send_sem, recv_sem, device_of=lambda p: p):
    made = []
    for i, p in enumerate(peers):
        made.append(pltpu.make_async_remote_copy(
            src_ref=src_of(p), dst_ref=dst, send_sem=send_sem.at[i], recv_sem=recv_sem.at[me],
            device_id=(device_of(p),), device_id_type=MESH))
    for c in made:
        c.start()

    def wait(dst_of):
        for p in peers:
            pltpu.make_async_remote_copy(
                src_ref=dst_of(p), dst_ref=dst_of(p), send_sem=send_sem.at[0], recv_sem=recv_sem.at[p],
                device_id=(device_of(p),), device_id_type=MESH).wait_recv()
        for c in made:
            c.wait_send()
    return wait


def all_to_all(n, me, src, dst, send_sem, recv_sem):
    wait = send_all(far_first(me, n, 8), me, lambda p: src.at[p], dst.at[me], send_sem, recv_sem)
    return lambda: wait(lambda p: dst.at[p])


def first_kernel(n, list_ref, own_ref, mask_ref, halo_ref, total_ref, tbl, out, cnt, cnts, sems):
    me = lax.axis_index("graph")
    ready = enter(n, me)
    rows = own_ref.shape[0]
    mine = jnp.sum(mask_ref[...].astype(F32), axis=0, keepdims=True)
    for p in range(n):
        cnt[p] = mine

    def load_own(o):
        tbl[0, pl.ds(o, 256), :] = own_ref[pl.ds(o, 256), :].astype(F32)
    chunked(rows, 256, load_own)
    send_rows(list_ref, tbl, out, row_masks())
    ready()
    big = all_to_all(n, me, out, halo_ref, sems.at[2], sems.at[3])
    small = all_to_all(n, me, cnt, cnts, sems.at[0], sems.at[1])
    halo_ref[pl.ds(me, 1)] = out[pl.ds(me, 1)]
    cnts[pl.ds(me, 1)] = cnt[pl.ds(me, 1)]
    small()
    total_ref[0] = jnp.sum(jnp.sum(cnts[...], axis=0))
    big()


def exchange_kernel(n, x_ref, o_ref, sems):
    me = lax.axis_index("graph")
    enter(n, me)()
    arrived = all_to_all(n, me, x_ref, o_ref, sems.at[0], sems.at[1])
    o_ref[pl.ds(me, 1)] = x_ref[pl.ds(me, 1)]
    arrived()


def reduce_kernel(n, classes, gw1_ref, gw2t_ref, loss_ref, total_ref, o1_ref, o2_ref, ol_ref, full, pair, acc, ring, half, sems):
    chips = n // 2
    me = lax.axis_index("graph")
    chip, core = me // 2, me % 2
    ready = enter(n, me)
    full[...] = jnp.zeros_like(full)
    per = full.shape[2]

    def tiles(rows):
        return [(i, t) for i in range(rows // 4) for t in range(2)]

    def place(at):
        return at // (per * chips), at // per % chips, at % per
    where_ = {}
    for name, ref, rows in (("a", gw1_ref, gw1_ref.shape[0]), ("b", gw2t_ref, classes)):
        for i, t in tiles(rows):
            where_[name, i, t] = place(len(where_))
            full[where_[name, i, t]] = ref[4 * i:4 * i + 4, t * LANES:(t + 1) * LANES]
    last = place(len(where_))
    full[last[0], last[1], last[2], 0:1] = loss_ref[:, :LANES] + loss_ref[:, LANES:]
    ready()
    partner = me + 1 - 2 * core
    swap = pltpu.make_async_remote_copy(src_ref=full.at[1 - core], dst_ref=pair, send_sem=sems.at[0, 0], recv_sem=sems.at[1, 0],
                                        device_id=(partner,), device_id_type=MESH)
    swap.start()
    swap.wait()
    acc[...] = pair[...] + full[core]

    peers = far_first(chip, chips, 4)

    def others(src_of, dst, s):
        return send_all(peers, chip, src_of, dst, sems.at[s], sems.at[s + 1], lambda p: 2 * p + core)
    first = others(lambda other: acc.at[other], ring.at[chip], 2)
    ring[pl.ds(chip, 1)] = acc[pl.ds(chip, 1)]
    first(lambda other: ring.at[other])
    half[pl.ds(core, 1), pl.ds(chip, 1)] = jnp.sum(ring[...], axis=0)[None, None]
    second = others(lambda other: half.at[core, chip], half.at[core, chip], 4)
    second(lambda other: half.at[core, other])
    back = pltpu.make_async_remote_copy(src_ref=half.at[core], dst_ref=half.at[core], send_sem=sems.at[0, 1], recv_sem=sems.at[1, 1],
                                        device_id=(partner,), device_id_type=MESH)
    back.start()
    back.wait()
    for name, ref in (("a", o1_ref), ("b", o2_ref)):
        for i, t in tiles(ref.shape[0]):
            ref[4 * i:4 * i + 4, t * LANES:(t + 1) * LANES] = half[where_[name, i, t]]
    ol_ref[0] = -jnp.sum(half[last]) / total_ref[0]


def layer_one_kernel(src_any, list_ref, wt_ref, own_ref, halo_ref, z_ref, out_ref, tbl, wts, ztbl, sem, *ring):
    def block(j, ids, w_ref):
        def store(at, z):
            zb = z.astype(BF16)
            z_ref[pl.ds(at, 32), :] = zb
            ztbl[0, pl.ds(at, 32), :] = zb.astype(F32)
        gather_sum(ids, w_ref, tbl, 1, masks, j, store)
    start, run = each_block(src_any, wt_ref, ring, wts, sem, block)
    start()
    rows, halo = own_ref.shape[0], halo_ref.shape[0]
    masks = row_masks()

    def load_own(o):
        tbl[0, pl.ds(o, 256), :] = own_ref[pl.ds(o, 256), :].astype(F32)

    def load_halo(o):
        tbl[0, pl.ds(o + rows, 256), :] = halo_ref[pl.ds(o, 256), :].astype(F32)
    chunked(rows, 256, load_own)
    chunked(halo, 256, load_halo)
    run()
    send_rows(list_ref, ztbl, out_ref, masks)


def hidden(z, w1):
    return jnp.maximum(dot(z, w1, ((1,), (0,))), 0.0).astype(BF16)


def layer_two_kernel(src_any, total_ref, wt_ref, z_own_ref, z_halo_ref, w1_ref, w2t_ref, lab_ref, mask_ref,
                     g2_ref, gw2t_ref, loss_ref, tbl, wts, z2, w2s, lg, g2ts, sem, *ring):
    def block(j, ids, w_ref):
        def store(at, z):
            z2[pl.ds(at, 32), :] = z.astype(BF16)
        gather_sum(ids, w_ref, tbl, 2, masks, j, store)
    start, run = each_block(src_any, wt_ref, ring, wts, sem, block)
    start()
    classes = w2t_ref.shape[0]
    rows, halo = z_own_ref.shape[0], z_halo_ref.shape[0]
    masks = row_masks()
    w1 = w1_ref[...].astype(BF16)

    def load(ref, base):
        def fn(o):
            h = hidden(ref[pl.ds(o, 1024), :], w1).astype(F32)
            tbl[0, pl.ds(o + base, 1024), :] = h[:, :LANES]
            tbl[1, pl.ds(o + base, 1024), :] = h[:, LANES:]
        return fn
    chunked(rows, 1024, load(z_own_ref, 0))
    chunked(halo, 1024, load(z_halo_ref, rows))
    run()

    total = total_ref[0]
    w2s[...] = jnp.zeros_like(w2s)
    w2s[pl.ds(0, classes), :] = w2t_ref[...].astype(BF16)
    w2t = w2s[...]
    pad_cls = w2t.shape[0]
    loss_ref[...] = jnp.zeros_like(loss_ref)
    cls = lax.broadcasted_iota(jnp.int32, (pad_cls, 256), 0)

    def project(o):
        lg[:, pl.ds(o, 1024)] = dot(w2t, z2[pl.ds(o, 1024), :], ((1,), (1,)))
    chunked(rows, 1024, project)

    def chunk(i, _):
        o = pl.multiple_of(i * 256, 256)
        logits = lg[:, pl.ds(o, 256)]
        live = cls < classes
        lab = jnp.concatenate([lab_ref[pl.ds(2 * i + t, 1), :] for t in range(2)], 1)
        mf = jnp.concatenate([mask_ref[pl.ds(2 * i + t, 1), :] for t in range(2)], 1).astype(F32)
        top = jnp.max(jnp.where(live, logits, -jnp.inf), axis=0, keepdims=True)
        shifted = logits - top
        ex = jnp.where(live, jnp.exp(shifted), 0.0)
        norm = jnp.sum(ex, axis=0, keepdims=True)
        logp = shifted - jnp.log(norm)
        hot = cls == lab
        loss_ref[...] += mf * jnp.sum(jnp.where(hot, logp, 0.0), axis=0, keepdims=True)
        g2t = ((ex * (1.0 / norm) - hot.astype(F32)) * (mf / total)).astype(BF16)
        g2ts[:, pl.ds(o, 256)] = g2t
        g2 = jnp.concatenate([g2t.astype(F32), jnp.zeros((2 * LANES - pad_cls, 256), F32)], 0).T
        g2_ref[pl.ds(o, 256), :] = g2.astype(BF16)
        return 0
    lax.fori_loop(0, rows // 256, chunk, 0)
    gw2t_ref[...] = dot(g2ts[...], z2[...], ((1,), (0,)))


PACKED = 88


def in_span(at, rows, width):
    lane = lax.broadcasted_iota(jnp.int32, (rows, LANES), 1)
    return (lane >= at) & (lane < at + width)


def scatter_kernel(in_deg, src_any, wt_ref, g2_ref, own_ref, halo_ref, sem, wts, *more):
    bufs, ring = more[:SUMS], more[SUMS:]

    def block(j, ids, w_ref):
        for c in range(LANES // 32):
            at = pl.multiple_of(j * LANES, LANES) + 32 * c
            gg = g2_ref[pl.ds(at, 32), :].astype(F32)
            for h in range(4):
                w8 = w_ref[32 * c + 8 * h:32 * c + 8 * h + 8, :]
                gs = [gg[8 * h:8 * h + 8, t * LANES:(t + 1) * LANES] for t in range(2)]
                terms = []
                for k in range(in_deg):
                    wk = jnp.broadcast_to(w8[:, k:k + 1], (8, LANES))
                    terms.append([wk * x for x in gs])
                for r in range(8):
                    for k in range(in_deg):
                        i = ids[k, 32 * c + 8 * h + r]
                        for t in range(2):
                            row = jnp.broadcast_to(bufs[((h * 8 + r) * in_deg + k) % SUMS][t, pl.ds(i, 1), :], (8, LANES)) + terms[k][t]
                            bufs[((h * 8 + r) * in_deg + k) % SUMS][t, pl.ds(i, 1), :] = row[r:r + 1, :]
    start, run = each_block(src_any, wt_ref, ring, wts, sem, block)
    start()
    rows, nodes = own_ref.shape[1], halo_ref.shape[0]

    def zero(i, _):
        for b in bufs:
            for t in range(2):
                b[t, pl.ds(pl.multiple_of(i * 64, 64), 64), :] = jnp.zeros((64, LANES), F32)
        return 0
    lax.fori_loop(0, bufs[0].shape[1] // 64, zero, 0)
    run()

    def total(t, o, n):
        s = pl.ds(o, n)
        a = bufs[0][t, s, :]
        for b in bufs[1:]:
            a = a + b[t, s, :]
        return a

    def red_own(o):
        for t in range(2):
            own_ref[t, pl.ds(o, 64), :] = total(t, o, 64)
    chunked(rows, 64, red_own)

    def red_halo(q, _):
        o = pl.multiple_of(rows + q * 64, 64)
        halo_ref[q, pl.ds(0, 64), :] = total(0, o, 64)
        hi = total(1, o, 64)
        packed = hi[:16]
        for g in range(1, 4):
            packed = jnp.where(in_span(32 * g, 16, 32), pltpu.roll(hi[16 * g:16 * g + 16], 32 * g, 1), packed)
        halo_ref[q, pl.ds(64, 16), :] = packed
        packed = pltpu.roll(hi[:8], LANES - 32, 1)
        for g in range(1, 8):
            packed = jnp.where(in_span(16 * g, 8, 16), pltpu.roll(hi[8 * g:8 * g + 8], (16 * g - 32) % LANES, 1), packed)
        halo_ref[q, pl.ds(80, 8), :] = packed
        return 0
    lax.fori_loop(0, nodes, red_halo, 0)


def combine_kernel(list_ref, own_ref, back_ref, z_ref, w1_ref, w2t_ref, gw1_ref, w2p, g1s, *bufs):
    nb = len(bufs)
    rows = own_ref.shape[1]

    def init(o):
        for t in range(2):
            bufs[0][t, pl.ds(o, 256), :] = own_ref[t, pl.ds(o, 256), :]
            for b in bufs[1:]:
                b[t, pl.ds(o, 256), :] = jnp.zeros((256, LANES), F32)
    chunked(rows, 256, init)
    first, second = in_span(0, 8, 32), in_span(32, 8, 16)

    def body(q, _):
        last = back_ref[q, pl.ds(80, 8), :]
        for g in range(8):
            lo = back_ref[q, pl.ds(8 * g, 8), :]
            mid = back_ref[q, pl.ds(64 + 8 * (g % 2), 8), :]
            mid = mid if g < 2 else pltpu.roll(mid, LANES - 32 * (g // 2), 1)
            tail = pltpu.roll(last, (32 - 16 * g) % LANES, 1) if g != 2 else last
            hi = jnp.where(first, mid, jnp.where(second, tail, 0.0))
            for r in range(8):
                b = bufs[r % nb]
                i = list_ref[q, 8 * g + r]
                for t, x in ((0, lo), (1, hi)):
                    row = jnp.broadcast_to(b[t, pl.ds(i, 1), :], (8, LANES)) + x
                    b[t, pl.ds(i, 1), :] = row[r:r + 1, :]
        return 0
    lax.fori_loop(0, back_ref.shape[0], body, 0)

    w1 = w1_ref[...].astype(BF16)
    w2p[...] = jnp.zeros_like(w2p)
    w2p[pl.ds(0, w2t_ref.shape[0]), :] = w2t_ref[...].astype(BF16)

    def finish(o):
        n = 512
        z = z_ref[pl.ds(o, n), :]
        h = hidden(z, w1)
        halves = []
        for t in range(2):
            a = bufs[0][t, pl.ds(o, n), :]
            for b in bufs[1:]:
                a = a + b[t, pl.ds(o, n), :]
            halves.append(a)
        x = jnp.concatenate(halves, 1)
        x1 = x.astype(BF16)
        rest = x - x1.astype(F32)
        x2 = rest.astype(BF16)
        x3 = (rest - x2.astype(F32)).astype(BF16)
        w2 = w2p[...]
        dh = dot(x3, w2, ((1,), (0,))) + dot(x2, w2, ((1,), (0,))) + dot(x1, w2, ((1,), (0,)))
        g1s[pl.ds(o, n), :] = jnp.where(h.astype(F32) > 0, dh, 0.0).astype(BF16)
    chunked(rows, 512, finish)
    gw1_ref[...] = dot(z_ref[...], g1s[...], ((0,), (0,)))


def solution(mesh):
    dev_count = mesh.shape["graph"]

    def device_step(feats, w_one, w_two, send_idx, send_count, edge_src, edge_wt, labels, label_mask):
        rows, feat_in = feats.shape
        hid, classes = w_two.shape
        halo_rows = send_idx.shape[1]
        in_deg = edge_src.shape[1]
        halo = dev_count * halo_rows
        ext = rows + halo + 16
        blocks = rows // LANES
        pad_cls = -(-classes // 16) * 16
        src = edge_src.T.reshape(in_deg, blocks, LANES).transpose(1, 0, 2)
        wt, w2t = edge_wt.T, w_two.T
        edge_ids = [pltpu.SMEM((in_deg, LANES), jnp.int32)] * RING
        edge_w = pltpu.VMEM((RING, LANES, 8), F32)
        edge_sem = pltpu.SemaphoreType.DMA((RING,))

        def comm(limit_mib, cid):
            return pltpu.CompilerParams(vmem_limit_bytes=limit_mib * 2**20,
                                        collective_id=cid, has_side_effects=True)

        def exchange(x, cid):
            return pl.pallas_call(
                functools.partial(exchange_kernel, dev_count), out_shape=jax.ShapeDtypeStruct(x.shape, x.dtype),
                in_specs=[VMEM], out_specs=VMEM, scratch_shapes=[pltpu.SemaphoreType.DMA((2, dev_count))],
                compiler_params=comm(8, cid), name="exchange",
            )(x)

        halo0, total = pl.pallas_call(
            functools.partial(first_kernel, dev_count),
            out_shape=[jax.ShapeDtypeStruct((dev_count, halo_rows, feat_in), BF16), jax.ShapeDtypeStruct((1,), F32)],
            in_specs=[SMEM, VMEM, VMEM], out_specs=[VMEM, SMEM],
            scratch_shapes=[pltpu.VMEM((1, rows, feat_in), F32), pltpu.VMEM((dev_count, halo_rows, feat_in), BF16),
                            pltpu.VMEM((dev_count, 1, LANES), F32), pltpu.VMEM((dev_count, 1, LANES), F32),
                            pltpu.SemaphoreType.DMA((4, dev_count))],
            compiler_params=comm(16, 0), name="first",
        )(send_idx, feats, label_mask.reshape(blocks, LANES))
        z1, out1 = pl.pallas_call(
            layer_one_kernel,
            out_shape=[jax.ShapeDtypeStruct((rows, feat_in), BF16), jax.ShapeDtypeStruct((dev_count, halo_rows, feat_in), BF16)],
            in_specs=[ANY, SMEM, VMEM, VMEM, VMEM], out_specs=[VMEM, VMEM],
            scratch_shapes=[pltpu.VMEM((1, ext, feat_in), F32), edge_w, pltpu.VMEM((1, rows, feat_in), F32), edge_sem] + edge_ids,
            compiler_params=params(16), name="layer_one",
        )(src, send_idx, wt, feats, halo0.reshape(halo, feat_in))
        zh = exchange(out1, 1).reshape(halo, feat_in)
        g2, gw2t, loss_part = pl.pallas_call(
            layer_two_kernel,
            out_shape=[jax.ShapeDtypeStruct((rows, 2 * LANES), BF16), jax.ShapeDtypeStruct((pad_cls, hid), F32), jax.ShapeDtypeStruct((1, 256), F32)],
            in_specs=[ANY, SMEM, VMEM, VMEM, VMEM, VMEM, VMEM, VMEM, VMEM], out_specs=[VMEM, VMEM, VMEM],
            scratch_shapes=[pltpu.VMEM((2, ext, LANES), F32), edge_w, pltpu.VMEM((rows, hid), BF16),
                            pltpu.VMEM((pad_cls, hid), BF16), pltpu.VMEM((pad_cls, rows), F32), pltpu.VMEM((pad_cls, rows), BF16), edge_sem] + edge_ids,
            compiler_params=params(28), name="layer_two",
        )(src, total, wt, z1, zh, w_one, w2t, labels.reshape(blocks, LANES), label_mask.reshape(blocks, LANES))
        own, halo_g = pl.pallas_call(
            functools.partial(scatter_kernel, in_deg),
            out_shape=[jax.ShapeDtypeStruct((2, rows, LANES), F32), jax.ShapeDtypeStruct((dev_count, PACKED, LANES), F32)],
            in_specs=[ANY, VMEM, VMEM], out_specs=[VMEM, VMEM],
            scratch_shapes=[edge_sem, edge_w] + [pltpu.VMEM((2, ext, LANES), F32)] * SUMS + edge_ids,
            compiler_params=params(43), name="scatter",
        )(src, wt, g2)
        back = exchange(halo_g, 2)
        gw1 = pl.pallas_call(
            combine_kernel, out_shape=jax.ShapeDtypeStruct((feat_in, hid), F32),
            in_specs=[SMEM, VMEM, VMEM, VMEM, VMEM, VMEM], out_specs=VMEM,
            scratch_shapes=[pltpu.VMEM((2 * LANES, hid), BF16), pltpu.VMEM((rows, hid), BF16)] + [pltpu.VMEM((2, rows + 16, LANES), F32)] * 4,
            compiler_params=params(32), name="combine",
        )(send_idx, own, back, z1, w_one, w2t)
        chips = dev_count // 2
        per = -(-(2 * (feat_in + classes) // 4 + 1) // (2 * chips))
        gw1, gw2t, loss = pl.pallas_call(
            functools.partial(reduce_kernel, dev_count, classes),
            out_shape=[jax.ShapeDtypeStruct((feat_in, hid), F32), jax.ShapeDtypeStruct((classes, hid), F32), jax.ShapeDtypeStruct((1,), F32)],
            in_specs=[VMEM, VMEM, VMEM, SMEM], out_specs=[VMEM, VMEM, SMEM],
            scratch_shapes=[pltpu.VMEM((2, chips, per, 4, LANES), F32), pltpu.VMEM((chips, per, 4, LANES), F32), pltpu.VMEM((chips, per, 4, LANES), F32),
                            pltpu.VMEM((chips, per, 4, LANES), F32), pltpu.VMEM((2, chips, per, 4, LANES), F32), pltpu.SemaphoreType.DMA((6, dev_count))],
            compiler_params=comm(8, 3), name="reduce",
        )(gw1, gw2t, loss_part, total)
        return loss[0], gw1, gw2t.T

    row_spec = P("graph", None)
    vec_spec = P("graph")
    return jax.shard_map(device_step, mesh=mesh, in_specs=(row_spec, P(), P(), row_spec, vec_spec, row_spec, row_spec, vec_spec, vec_spec), out_specs=(P(), P(), P()), check_vma=False)
```
